16 devices in a mesh: fsdp: 16 (over z, y, x, core).
Axes of the slice: x: 2, y: 2, z: 2, core: 2. Of those that a mesh axis runs over, the one named last changes fastest.
Arguments:
- grad_mat: bfloat16 [16, 19660800], P('fsdp')
- grad_vec: bfloat16 [16, 8192], P('fsdp')
- master_mat: float32 [19660800], P('fsdp')
- moment_mat: float32 [19660800], P('fsdp')
- second_mat: float32 [19660800], P('fsdp')
- master_vec: float32 [8192], P('fsdp')
- moment_vec: float32 [8192], P('fsdp')
- second_vec: float32 [8192], P('fsdp')
Outputs:
- output 1: float32 [19660800], P('fsdp')
- output 2: float32 [19660800], P('fsdp')
- output 3: float32 [19660800], P('fsdp')
- output 4: float32 [8192], P('fsdp')
- output 5: float32 [8192], P('fsdp')
- output 6: float32 [8192], P('fsdp')
- output 7: bfloat16 [19660800], replicated
- output 8: bfloat16 [8192], replicated
All inputs are finite; a program needn't handle non-finite values.
Results may differ from the reference program's by a relative error of at most 0.001.
Values are sent between devices in bfloat16 or wider.
A program may use at most 1 GiB of HBM per device.

```python
import jax
import jax.numpy as jnp
from jax import lax

D = 960
HEADS = 15
KV_HEADS = 5
HEAD = 64
FF = 2560
LAYERS = 2
GROUP = 16
NM_PAD = 19660800
NV_PAD = 8192
STEP = 4

Q_OUT = HEADS * HEAD
KV_OUT = KV_HEADS * HEAD
MAT_COUNT = LAYERS * (2 * D * Q_OUT + 2 * D * KV_OUT + 3 * D * FF)
VEC_COUNT = LAYERS * (Q_OUT + 2 * KV_OUT + 2 * D)
GRAD_UNIT = (MAT_COUNT + VEC_COUNT) ** -0.5
TARGET_NORM = 3.0
LEARN_RATE = 1e-3
BETA_ONE = 0.9
BETA_TWO = 0.999
ADAM_EPS = 1e-8
DECAY = 0.01
NORM_EPS = 1e-6
FIX_ONE = 1.0 - BETA_ONE ** STEP
FIX_TWO = 1.0 - BETA_TWO ** STEP


def pad_flat(flat, total):
    return jnp.pad(flat, (0, total - flat.shape[0]))


def layer_draw(key, pieces):
    sub_keys = jax.random.split(key, len(pieces))
    drawn = [jax.random.normal(sub_key, (LAYERS, length), jnp.float32) * scale + offset
             for sub_key, (length, scale, offset) in zip(sub_keys, pieces)]
    return jnp.concatenate(drawn, axis=1).reshape(-1)


def grad_rows(key, total, valid):
    keep = jnp.arange(total) < valid
    scale = TARGET_NORM * GRAD_UNIT * GROUP ** -0.5

    def one_row(row):
        noise = jax.random.normal(jax.random.fold_in(key, row), (total,), jnp.float32)
        return jnp.where(keep, noise * scale, 0.0).astype(jnp.bfloat16)

    return lax.map(one_row, jnp.arange(GROUP))


def moment_draw(key, total, valid):
    keep = jnp.arange(total) < valid
    noise = jax.random.normal(key, (total,), jnp.float32)
    return jnp.where(keep, 0.1 * GRAD_UNIT * noise, 0.0)


def second_draw(key, total, valid):
    keep = jnp.arange(total) < valid
    noise = jax.random.normal(key, (total,), jnp.float32)
    return jnp.where(keep, 0.003 * GRAD_UNIT ** 2 * (noise * noise + 0.5), 0.0)


def setup_inputs(seed: int = 0) -> dict:
    keys = jax.random.split(jax.random.key(seed), 8)
    mat_pieces = [(D * Q_OUT, D ** -0.5, 0.0), (D * KV_OUT, D ** -0.5, 0.0), (D * KV_OUT, D ** -0.5, 0.0),
                  (Q_OUT * D, Q_OUT ** -0.5, 0.0), (D * FF, D ** -0.5, 0.0), (D * FF, D ** -0.5, 0.0),
                  (FF * D, FF ** -0.5, 0.0)]
    vec_pieces = [(Q_OUT, 0.5, 0.0), (KV_OUT, 0.5, 0.0), (KV_OUT, 0.5, 0.0), (D, 0.2, 1.0), (D, 0.2, 1.0)]
    return {
        'grad_mat': grad_rows(keys[0], NM_PAD, MAT_COUNT),
        'grad_vec': grad_rows(keys[1], NV_PAD, VEC_COUNT),
        'master_mat': pad_flat(layer_draw(keys[2], mat_pieces), NM_PAD),
        'moment_mat': moment_draw(keys[3], NM_PAD, MAT_COUNT),
        'second_mat': second_draw(keys[4], NM_PAD, MAT_COUNT),
        'master_vec': pad_flat(layer_draw(keys[5], vec_pieces), NV_PAD),
        'moment_vec': moment_draw(keys[6], NV_PAD, VEC_COUNT),
        'second_vec': second_draw(keys[7], NV_PAD, VEC_COUNT),
    }


def row_total(grad_block):
    def add_row(running, row_vals):
        return running + row_vals.astype(jnp.float32), None

    total, _ = lax.scan(add_row, jnp.zeros(grad_block.shape[1:], jnp.float32), grad_block)
    return total


def adam_update(grad_sum, clip_coef, master, moment, second, decay):
    clip_grad = clip_coef * grad_sum
    new_moment = BETA_ONE * moment + (1.0 - BETA_ONE) * clip_grad
    new_second = BETA_TWO * second + (1.0 - BETA_TWO) * clip_grad * clip_grad
    step_dir = (new_moment / FIX_ONE) / (jnp.sqrt(new_second / FIX_TWO) + ADAM_EPS)
    new_master = master - LEARN_RATE * (step_dir + decay * master)
    return new_master, new_moment, new_second


def reference(grad_mat, grad_vec, master_mat, moment_mat, second_mat, master_vec, moment_vec, second_vec):
    sum_mat = row_total(grad_mat)
    sum_vec = row_total(grad_vec)
    total_norm = jnp.sqrt(jnp.sum(sum_mat * sum_mat) + jnp.sum(sum_vec * sum_vec))
    clip_coef = jnp.minimum(1.0, 1.0 / (total_norm + NORM_EPS))
    mat_out = adam_update(sum_mat, clip_coef, master_mat, moment_mat, second_mat, DECAY)
    vec_out = adam_update(sum_vec, clip_coef, master_vec, moment_vec, second_vec, 0.0)
    return (mat_out[0], mat_out[1], mat_out[2], vec_out[0], vec_out[1], vec_out[2],
            mat_out[0].astype(jnp.bfloat16), vec_out[0].astype(jnp.bfloat16))
```

```python
import functools

import jax
import jax.numpy as jnp
from jax import lax
from jax.experimental import pallas as pl
from jax.experimental.pallas import tpu as pltpu
from jax.sharding import PartitionSpec as P

STEP = 4
LEARN_RATE = 1e-3
BETA_ONE = 0.9
BETA_TWO = 0.999
ADAM_EPS = 1e-8
DECAY = 0.01
NORM_EPS = 1e-6
FIX_ONE = 1.0 - BETA_ONE ** STEP
FIX_TWO = 1.0 - BETA_TWO ** STEP

AXIS = 'fsdp'
MESH = pl.DeviceIdType.MESH
GROUP = 16
LANES = 128
ORDERS = ((2, 4, 8), (4, 8, 2), (8, 2, 4))
COLORS = len(ORDERS)
CHUNKS = 4
SUB_ROWS = 160


def adam_update(grad_sum, clip_coef, master, moment, second, decay):
    clip_grad = clip_coef * grad_sum
    new_moment = BETA_ONE * moment + (1.0 - BETA_ONE) * clip_grad
    new_second = BETA_TWO * second + (1.0 - BETA_TWO) * clip_grad * clip_grad
    step_dir = (new_moment / FIX_ONE) / (jnp.sqrt(new_second / FIX_TWO) + ADAM_EPS)
    new_master = master - LEARN_RATE * (step_dir + decay * master)
    return new_master, new_moment, new_second


def flip_of(me, bit):
    return bit * (1 - 2 * ((me // bit) % 2))


def reduce_kernel(rows, share, vec_share, grad_ref, vec_ref,
                  sum_ref, vec_sum_ref, square_ref, land_ref,
                  raw_in, raw_out, part_in, own_in, s4_out, keep0, keep1, recv2, recv3,
                  vec_land, square_land, square_acc,
                  in_sem, send1_sem, part_sem, own_sem, recv1_sem, recv2_sem, recv3_sem,
                  send2_sem, send3_sem, out_sem, small_sem):
    me = lax.axis_index(AXIS)
    core = me % 2
    block = rows * LANES
    color_len = share // COLORS
    flips = [[flip_of(me, bit) for bit in order] for order in ORDERS]

    def vec_copy(dist):
        other = (me + dist) % GROUP
        return pltpu.make_async_remote_copy(
            vec_ref.at[:, pl.ds(pl.multiple_of(other * vec_share, vec_share), vec_share)], vec_land.at[me],
            small_sem.at[0], small_sem.at[1], device_id=(other,), device_id_type=MESH)

    def vec_start(dist, carry):
        vec_copy(dist).start()
        return carry

    lax.fori_loop(1, GROUP, vec_start, 0)
    vec_own = pltpu.make_async_copy(
        vec_ref.at[:, pl.ds(pl.multiple_of(me * vec_share, vec_share), vec_share)], vec_land.at[me], small_sem.at[2])
    vec_own.start()

    def piece_at(owner, color, chunk):
        start = pl.multiple_of(owner * share + color * color_len + chunk * block, block)
        return grad_ref.at[:, pl.ds(start, block)]

    def route(item, color):
        place, kind = item // 3, (item + 1) % 3
        flip1, flip2, flip3 = flips[color]
        local = (2 - kind) // 2
        target_core = local * (1 - core) + (1 - local) * (kind - 1)
        target = me - core + (1 - local) * flip1 + target_core
        owner = target + (1 - place // 2) * flip2 + (1 - place % 2) * flip3
        source = (1 - local) * (1 + core)
        return owner, target, source, place

    def in_copy(chunk, item, color):
        owner = route(item, color)[0]
        return pltpu.make_async_copy(piece_at(owner, color, chunk), raw_in.at[item % 2, color], in_sem.at[item % 2, color])

    def pack_and_send(chunk):
        slot = chunk % 2
        for color in range(COLORS):
            in_copy(chunk, 0, color).start()

        def one_item(item, carry):
            @pl.when(item + 1 < 12)
            def _():
                for color in range(COLORS):
                    in_copy(chunk, item + 1, color).start()

            for color in range(COLORS):
                in_copy(chunk, item, color).wait()

                def pack(sub, inner):
                    off = pl.multiple_of(sub * SUB_ROWS * LANES, SUB_ROWS * LANES)
                    vals = raw_in[item % 2, color, :, pl.ds(off, SUB_ROWS * LANES)].astype(jnp.float32)
                    to = pl.multiple_of(sub * SUB_ROWS, SUB_ROWS)
                    raw_out[slot, color, item, pl.ds(to, SUB_ROWS), :] = (
                        vals.reshape(SUB_ROWS, LANES).astype(jnp.bfloat16))
                    return inner

                lax.fori_loop(0, rows // SUB_ROWS, pack, 0)
            for color in range(COLORS):
                owner, target, source, place = route(item, color)
                pltpu.make_async_remote_copy(
                    raw_out.at[slot, color, item], land_ref.at[color, chunk, place, source],
                    send1_sem.at[slot], recv1_sem.at[color, chunk], device_id=(target,), device_id_type=MESH).start()
            return carry

        lax.fori_loop(0, 12, one_item, 0)

    def wait_bytes(ref, sem):
        pltpu.make_async_copy(ref, ref, sem).wait()

    def part_copies(chunk, place, color, slot):
        flip1, flip2, flip3 = flips[color]
        owner = me + (1 - place // 2) * flip2 + (1 - place % 2) * flip3
        return (pltpu.make_async_copy(land_ref.at[color, chunk, place], part_in.at[slot, color], part_sem.at[slot, color]),
                pltpu.make_async_copy(piece_at(owner, color, chunk), own_in.at[slot, color], own_sem.at[slot, color]))

    def first_sums(chunk):
        for color in range(COLORS):
            wait_bytes(land_ref.at[color, chunk], recv1_sem.at[color, chunk])
            for copy in part_copies(chunk, 0, color, 0):
                copy.start()
        for place in range(4):
            slot = place % 2
            for color in range(COLORS):
                if place < 3:
                    for copy in part_copies(chunk, place + 1, color, (place + 1) % 2):
                        copy.start()
                for copy in part_copies(chunk, place, color, slot):
                    copy.wait()
                total = (s4_out.at[chunk, color, place] if place < 2 else
                         (keep1 if place == 2 else keep0).at[chunk, color])

                def add(sub, inner):
                    off = pl.multiple_of(sub * SUB_ROWS * LANES, SUB_ROWS * LANES)
                    to = pl.ds(pl.multiple_of(sub * SUB_ROWS, SUB_ROWS), SUB_ROWS)
                    vals = own_in[slot, color, :, pl.ds(off, SUB_ROWS * LANES)].astype(jnp.float32)
                    vals = vals.reshape(SUB_ROWS, LANES)
                    for source in range(3):
                        vals = vals + part_in[slot, color, source, to, :].astype(jnp.float32)
                    total[to, :] = vals
                    return inner

                lax.fori_loop(0, rows // SUB_ROWS, add, 0)
                if place < 2:
                    pltpu.make_async_remote_copy(
                        total, recv2.at[chunk, color, place], send2_sem, recv2_sem.at[color, chunk],
                        device_id=(me + flips[color][1],), device_id_type=MESH).start()

    pack_and_send(0)
    pack_and_send(1)

    def first_stage(chunk, carry):
        first_sums(chunk)

        @pl.when(chunk + 2 < CHUNKS)
        def _():
            wait_bytes(raw_out.at[chunk % 2], send1_sem.at[chunk % 2])
            pack_and_send(chunk + 2)

        return carry

    lax.fori_loop(0, CHUNKS, first_stage, 0)

    def second_stage(chunk, carry):
        for color in range(COLORS):
            wait_bytes(recv2.at[chunk, color], recv2_sem.at[color, chunk])

            def add(sub, inner):
                to = pl.ds(pl.multiple_of(sub * SUB_ROWS, SUB_ROWS), SUB_ROWS)
                keep1[chunk, color, to, :] += recv2[chunk, color, 0, to, :]
                keep0[chunk, color, to, :] += recv2[chunk, color, 1, to, :]
                return inner

            lax.fori_loop(0, rows // SUB_ROWS, add, 0)
            pltpu.make_async_remote_copy(
                keep1.at[chunk, color], recv3.at[chunk, color], send3_sem, recv3_sem.at[color, chunk],
                device_id=(me + flips[color][2],), device_id_type=MESH).start()
        return carry

    lax.fori_loop(0, CHUNKS, second_stage, 0)

    vec_own.wait()
    wait_bytes(vec_land.at[pl.ds(0, GROUP - 1)], small_sem.at[1])
    vec_sum = jnp.sum(vec_land[...].astype(jnp.float32), axis=0)
    vec_sum_ref[...] = vec_sum
    square_acc[...] = jnp.zeros_like(square_acc)
    vec_square = sum(vec_sum[:, part * LANES:(part + 1) * LANES] ** 2 for part in range(vec_share // LANES))

    def third_stage(chunk, carry):
        for color in range(COLORS):
            wait_bytes(recv3.at[chunk, color], recv3_sem.at[color, chunk])

            def add(sub, inner):
                to = pl.ds(pl.multiple_of(sub * SUB_ROWS, SUB_ROWS), SUB_ROWS)
                vals = keep0[chunk, color, to, :] + recv3[chunk, color, to, :]
                keep0[chunk, color, to, :] = vals
                square_acc[...] += jnp.sum((vals * vals).reshape(SUB_ROWS // 8, 8, LANES), axis=0)
                return inner

            lax.fori_loop(0, rows // SUB_ROWS, add, 0)
            start = pl.multiple_of(color * (color_len // LANES) + chunk * rows, rows)
            pltpu.make_async_copy(keep0.at[chunk, color], sum_ref.at[pl.ds(start, rows)], out_sem).start()
        return carry

    lax.fori_loop(0, CHUNKS, third_stage, 0)

    square_land[me] = jnp.sum(square_acc[...], axis=0, keepdims=True) + vec_square

    def square_copy(dist, carry):
        pltpu.make_async_remote_copy(
            square_land.at[me], square_land.at[me], small_sem.at[3], small_sem.at[4],
            device_id=((me + dist) % GROUP,), device_id_type=MESH).start()
        return carry

    lax.fori_loop(1, GROUP, square_copy, 0)
    wait_bytes(square_land.at[pl.ds(0, GROUP - 1)], small_sem.at[4])
    lane_sum = jnp.sum(square_land[...], axis=0)
    square_ref[...] = jnp.broadcast_to(jnp.sum(lane_sum, axis=1, keepdims=True), square_ref.shape)

    wait_bytes(vec_land.at[pl.ds(0, GROUP - 1)], small_sem.at[0])
    for slot in range(2):
        wait_bytes(raw_out.at[slot], send1_sem.at[slot])
    wait_bytes(s4_out, send2_sem)
    wait_bytes(keep1, send3_sem)
    wait_bytes(keep0, out_sem)
    wait_bytes(square_land.at[pl.ds(0, GROUP - 1)], small_sem.at[3])


def reduce_call(grad_mat, grad_vec):
    share = grad_mat.shape[1] // GROUP
    vec_share = grad_vec.shape[1] // GROUP
    rows = share // COLORS // CHUNKS // LANES
    any_spec = pl.BlockSpec(memory_space=pltpu.HBM)
    vmem_spec = pl.BlockSpec(memory_space=pltpu.VMEM)
    f32, bf16 = jnp.float32, jnp.bfloat16
    dma = pltpu.SemaphoreType.DMA
    return pl.pallas_call(
        functools.partial(reduce_kernel, rows, share, vec_share),
        name='reduce_share',
        out_shape=(jax.ShapeDtypeStruct((share // LANES, LANES), f32),
                   jax.ShapeDtypeStruct((1, vec_share), f32),
                   jax.ShapeDtypeStruct((1, LANES), f32),
                   jax.ShapeDtypeStruct((COLORS, CHUNKS, 4, 3, rows, LANES), bf16)),
        in_specs=[any_spec, any_spec],
        out_specs=(any_spec, vmem_spec, vmem_spec, any_spec),
        scratch_shapes=[
            pltpu.VMEM((2, COLORS, 1, rows * LANES), bf16),
            pltpu.VMEM((2, COLORS, 12, rows, LANES), bf16),
            pltpu.VMEM((2, COLORS, 3, rows, LANES), bf16),
            pltpu.VMEM((2, COLORS, 1, rows * LANES), bf16),
            pltpu.VMEM((CHUNKS, COLORS, 2, rows, LANES), f32),
            pltpu.VMEM((CHUNKS, COLORS, rows, LANES), f32),
            pltpu.VMEM((CHUNKS, COLORS, rows, LANES), f32),
            pltpu.VMEM((CHUNKS, COLORS, 2, rows, LANES), f32),
            pltpu.VMEM((CHUNKS, COLORS, rows, LANES), f32),
            pltpu.VMEM((GROUP, 1, vec_share), bf16),
            pltpu.VMEM((GROUP, 1, LANES), f32),
            pltpu.VMEM((8, LANES), f32),
            dma((2, COLORS)), dma((2,)), dma((2, COLORS)), dma((2, COLORS)),
            dma((COLORS, CHUNKS)), dma((COLORS, CHUNKS)), dma((COLORS, CHUNKS)),
            dma, dma, dma, dma((5,)),
        ],
        compiler_params=pltpu.CompilerParams(has_side_effects=True, vmem_limit_bytes=66_000_000),
    )(grad_mat, grad_vec)


def solution(mesh):
    def local_step(grad_mat, grad_vec, master_mat, moment_mat, second_mat, master_vec, moment_vec, second_vec):
        sum_mat, sum_vec, square, _ = reduce_call(grad_mat, grad_vec)
        total_norm = jnp.sqrt(square[0, 0])
        clip_coef = jnp.minimum(1.0, 1.0 / (total_norm + NORM_EPS))
        new_mat = adam_update(sum_mat.reshape(-1), clip_coef, master_mat, moment_mat, second_mat, DECAY)
        new_vec = adam_update(sum_vec.reshape(-1), clip_coef, master_vec, moment_vec, second_vec, 0.0)
        weights_mat = lax.all_gather(new_mat[0].astype(jnp.bfloat16), AXIS, tiled=True)
        weights_vec = lax.all_gather(new_vec[0].astype(jnp.bfloat16), AXIS, tiled=True)
        return new_mat + new_vec + (weights_mat, weights_vec)

    row_spec = P(AXIS, None)
    flat_spec = P(AXIS)
    whole_spec = P()
    return jax.shard_map(local_step, mesh=mesh,
                         in_specs=(row_spec, row_spec) + (flat_spec,) * 6,
                         out_specs=(flat_spec,) * 6 + (whole_spec, whole_spec),
                         check_vma=False)
```

```python
import functools

import jax
import jax.numpy as jnp
from jax import lax
from jax.experimental import pallas as pl
from jax.experimental.pallas import tpu as pltpu
from jax.sharding import PartitionSpec as P

STEP = 4
LEARN_RATE = 1e-3
BETA_ONE = 0.9
BETA_TWO = 0.999
ADAM_EPS = 1e-8
DECAY = 0.01
NORM_EPS = 1e-6
FIX_ONE = 1.0 - BETA_ONE ** STEP
FIX_TWO = 1.0 - BETA_TWO ** STEP

AXIS = 'fsdp'
MESH = pl.DeviceIdType.MESH
GROUP = 16
LANES = 128
ORDERS = ((2, 4, 8), (4, 8, 2), (8, 2, 4))
COLORS = len(ORDERS)
CHUNKS = 4
SUB_ROWS = 160
UPDATE_ROWS = 80
GATHER_VMEM = 8_000_000
STORE_VMEM = GATHER_VMEM


def adam_update(grad_sum, clip_coef, master, moment, second, decay):
    clip_grad = clip_coef * grad_sum
    new_moment = BETA_ONE * moment + (1.0 - BETA_ONE) * clip_grad
    new_second = BETA_TWO * second + (1.0 - BETA_TWO) * clip_grad * clip_grad
    step_dir = (new_moment / FIX_ONE) / (jnp.sqrt(new_second / FIX_TWO) + ADAM_EPS)
    new_master = master - LEARN_RATE * (step_dir + decay * master)
    return new_master, new_moment, new_second


def flip_of(me, bit):
    return bit * (1 - 2 * ((me // bit) % 2))


def reduce_kernel(rows, share, vec_share, grad_ref, vec_ref,
                  sum_ref, vec_sum_ref, square_ref, land_ref,
                  raw_in, raw_out, part_in, own_in, s4_out, keep0, keep1, recv2, recv3,
                  vec_land, square_land, square_acc,
                  in_sem, send1_sem, part_sem, own_sem, recv1_sem, recv2_sem, recv3_sem,
                  send2_sem, send3_sem, out_sem, small_sem):
    me = lax.axis_index(AXIS)
    core = me % 2
    block = rows * LANES
    color_len = share // COLORS
    flips = [[flip_of(me, bit) for bit in order] for order in ORDERS]

    def vec_copy(dist):
        other = (me + dist) % GROUP
        return pltpu.make_async_remote_copy(
            vec_ref.at[:, pl.ds(pl.multiple_of(other * vec_share, vec_share), vec_share)], vec_land.at[me],
            small_sem.at[0], small_sem.at[1], device_id=(other,), device_id_type=MESH)

    def vec_start(dist, carry):
        vec_copy(dist).start()
        return carry

    lax.fori_loop(1, GROUP, vec_start, 0)
    vec_own = pltpu.make_async_copy(
        vec_ref.at[:, pl.ds(pl.multiple_of(me * vec_share, vec_share), vec_share)], vec_land.at[me], small_sem.at[2])
    vec_own.start()

    def piece_at(owner, color, chunk):
        start = pl.multiple_of(owner * share + color * color_len + chunk * block, block)
        return grad_ref.at[:, pl.ds(start, block)]

    def route(item, color):
        place, kind = item // 3, (item + 1) % 3
        flip1, flip2, flip3 = flips[color]
        local = (2 - kind) // 2
        target_core = local * (1 - core) + (1 - local) * (kind - 1)
        target = me - core + (1 - local) * flip1 + target_core
        owner = target + (1 - place // 2) * flip2 + (1 - place % 2) * flip3
        source = (1 - local) * (1 + core)
        return owner, target, source, place

    def in_copy(chunk, item, color):
        owner = route(item, color)[0]
        return pltpu.make_async_copy(piece_at(owner, color, chunk), raw_in.at[item % 2, color], in_sem.at[item % 2, color])

    def pack_and_send(chunk):
        slot = chunk % 2
        for color in range(COLORS):
            in_copy(chunk, 0, color).start()

        def one_item(item, carry):
            @pl.when(item + 1 < 12)
            def _():
                for color in range(COLORS):
                    in_copy(chunk, item + 1, color).start()

            for color in range(COLORS):
                in_copy(chunk, item, color).wait()

                def pack(sub, inner):
                    off = pl.multiple_of(sub * SUB_ROWS * LANES, SUB_ROWS * LANES)
                    vals = raw_in[item % 2, color, :, pl.ds(off, SUB_ROWS * LANES)].astype(jnp.float32)
                    to = pl.multiple_of(sub * SUB_ROWS, SUB_ROWS)
                    raw_out[slot, color, item, pl.ds(to, SUB_ROWS), :] = (
                        vals.reshape(SUB_ROWS, LANES).astype(jnp.bfloat16))
                    return inner

                lax.fori_loop(0, rows // SUB_ROWS, pack, 0)
            for color in range(COLORS):
                owner, target, source, place = route(item, color)
                pltpu.make_async_remote_copy(
                    raw_out.at[slot, color, item], land_ref.at[color, chunk, place, source],
                    send1_sem.at[slot], recv1_sem.at[color, chunk], device_id=(target,), device_id_type=MESH).start()
            return carry

        lax.fori_loop(0, 12, one_item, 0)

    def wait_bytes(ref, sem):
        pltpu.make_async_copy(ref, ref, sem).wait()

    def part_copies(chunk, place, color, slot):
        flip1, flip2, flip3 = flips[color]
        owner = me + (1 - place // 2) * flip2 + (1 - place % 2) * flip3
        return (pltpu.make_async_copy(land_ref.at[color, chunk, place], part_in.at[slot, color], part_sem.at[slot, color]),
                pltpu.make_async_copy(piece_at(owner, color, chunk), own_in.at[slot, color], own_sem.at[slot, color]))

    def first_sums(chunk):
        for color in range(COLORS):
            wait_bytes(land_ref.at[color, chunk], recv1_sem.at[color, chunk])
            for copy in part_copies(chunk, 0, color, 0):
                copy.start()
        for place in range(4):
            slot = place % 2
            for color in range(COLORS):
                if place < 3:
                    for copy in part_copies(chunk, place + 1, color, (place + 1) % 2):
                        copy.start()
                for copy in part_copies(chunk, place, color, slot):
                    copy.wait()
                total = (s4_out.at[chunk, color, place] if place < 2 else
                         (keep1 if place == 2 else keep0).at[chunk, color])

                def add(sub, inner):
                    off = pl.multiple_of(sub * SUB_ROWS * LANES, SUB_ROWS * LANES)
                    to = pl.ds(pl.multiple_of(sub * SUB_ROWS, SUB_ROWS), SUB_ROWS)
                    vals = own_in[slot, color, :, pl.ds(off, SUB_ROWS * LANES)].astype(jnp.float32)
                    vals = vals.reshape(SUB_ROWS, LANES)
                    for source in range(3):
                        vals = vals + part_in[slot, color, source, to, :].astype(jnp.float32)
                    total[to, :] = vals
                    return inner

                lax.fori_loop(0, rows // SUB_ROWS, add, 0)
                if place < 2:
                    pltpu.make_async_remote_copy(
                        total, recv2.at[chunk, color, place], send2_sem, recv2_sem.at[color, chunk],
                        device_id=(me + flips[color][1],), device_id_type=MESH).start()

    pack_and_send(0)
    pack_and_send(1)

    def first_stage(chunk, carry):
        first_sums(chunk)

        @pl.when(chunk + 2 < CHUNKS)
        def _():
            wait_bytes(raw_out.at[chunk % 2], send1_sem.at[chunk % 2])
            pack_and_send(chunk + 2)

        return carry

    lax.fori_loop(0, CHUNKS, first_stage, 0)

    def second_stage(chunk, carry):
        for color in range(COLORS):
            wait_bytes(recv2.at[chunk, color], recv2_sem.at[color, chunk])

            def add(sub, inner):
                to = pl.ds(pl.multiple_of(sub * SUB_ROWS, SUB_ROWS), SUB_ROWS)
                keep1[chunk, color, to, :] += recv2[chunk, color, 0, to, :]
                keep0[chunk, color, to, :] += recv2[chunk, color, 1, to, :]
                return inner

            lax.fori_loop(0, rows // SUB_ROWS, add, 0)
            pltpu.make_async_remote_copy(
                keep1.at[chunk, color], recv3.at[chunk, color], send3_sem, recv3_sem.at[color, chunk],
                device_id=(me + flips[color][2],), device_id_type=MESH).start()
        return carry

    lax.fori_loop(0, CHUNKS, second_stage, 0)

    vec_own.wait()
    wait_bytes(vec_land.at[pl.ds(0, GROUP - 1)], small_sem.at[1])
    vec_sum = jnp.sum(vec_land[...].astype(jnp.float32), axis=0)
    vec_sum_ref[...] = vec_sum
    square_acc[...] = jnp.zeros_like(square_acc)
    vec_square = sum(vec_sum[:, part * LANES:(part + 1) * LANES] ** 2 for part in range(vec_share // LANES))

    def third_stage(chunk, carry):
        for color in range(COLORS):
            wait_bytes(recv3.at[chunk, color], recv3_sem.at[color, chunk])

            def add(sub, inner):
                to = pl.ds(pl.multiple_of(sub * SUB_ROWS, SUB_ROWS), SUB_ROWS)
                vals = keep0[chunk, color, to, :] + recv3[chunk, color, to, :]
                keep0[chunk, color, to, :] = vals
                square_acc[...] += jnp.sum((vals * vals).reshape(SUB_ROWS // 8, 8, LANES), axis=0)
                return inner

            lax.fori_loop(0, rows // SUB_ROWS, add, 0)
            start = pl.multiple_of(color * (color_len // LANES) + chunk * rows, rows)
            pltpu.make_async_copy(keep0.at[chunk, color], sum_ref.at[pl.ds(start, rows)], out_sem).start()
        return carry

    lax.fori_loop(0, CHUNKS, third_stage, 0)

    square_land[me] = jnp.sum(square_acc[...], axis=0, keepdims=True) + vec_square

    def square_copy(dist, carry):
        pltpu.make_async_remote_copy(
            square_land.at[me], square_land.at[me], small_sem.at[3], small_sem.at[4],
            device_id=((me + dist) % GROUP,), device_id_type=MESH).start()
        return carry

    lax.fori_loop(1, GROUP, square_copy, 0)
    wait_bytes(square_land.at[pl.ds(0, GROUP - 1)], small_sem.at[4])
    lane_sum = jnp.sum(square_land[...], axis=0)
    square_ref[...] = jnp.broadcast_to(jnp.sum(lane_sum, axis=1, keepdims=True), square_ref.shape)

    wait_bytes(vec_land.at[pl.ds(0, GROUP - 1)], small_sem.at[0])
    for slot in range(2):
        wait_bytes(raw_out.at[slot], send1_sem.at[slot])
    wait_bytes(s4_out, send2_sem)
    wait_bytes(keep1, send3_sem)
    wait_bytes(keep0, out_sem)
    wait_bytes(square_land.at[pl.ds(0, GROUP - 1)], small_sem.at[3])


def reduce_call(grad_mat, grad_vec):
    share = grad_mat.shape[1] // GROUP
    vec_share = grad_vec.shape[1] // GROUP
    rows = share // COLORS // CHUNKS // LANES
    any_spec = pl.BlockSpec(memory_space=pltpu.HBM)
    vmem_spec = pl.BlockSpec(memory_space=pltpu.VMEM)
    f32, bf16 = jnp.float32, jnp.bfloat16
    dma = pltpu.SemaphoreType.DMA
    return pl.pallas_call(
        functools.partial(reduce_kernel, rows, share, vec_share),
        name='reduce_share',
        out_shape=(jax.ShapeDtypeStruct((share // LANES, LANES), f32),
                   jax.ShapeDtypeStruct((1, vec_share), f32),
                   jax.ShapeDtypeStruct((1, LANES), f32),
                   jax.ShapeDtypeStruct((COLORS, CHUNKS, 4, 3, rows, LANES), bf16)),
        in_specs=[any_spec, any_spec],
        out_specs=(any_spec, vmem_spec, vmem_spec, any_spec),
        scratch_shapes=[
            pltpu.VMEM((2, COLORS, 1, rows * LANES), bf16),
            pltpu.VMEM((2, COLORS, 12, rows, LANES), bf16),
            pltpu.VMEM((2, COLORS, 3, rows, LANES), bf16),
            pltpu.VMEM((2, COLORS, 1, rows * LANES), bf16),
            pltpu.VMEM((CHUNKS, COLORS, 2, rows, LANES), f32),
            pltpu.VMEM((CHUNKS, COLORS, rows, LANES), f32),
            pltpu.VMEM((CHUNKS, COLORS, rows, LANES), f32),
            pltpu.VMEM((CHUNKS, COLORS, 2, rows, LANES), f32),
            pltpu.VMEM((CHUNKS, COLORS, rows, LANES), f32),
            pltpu.VMEM((GROUP, 1, vec_share), bf16),
            pltpu.VMEM((GROUP, 1, LANES), f32),
            pltpu.VMEM((8, LANES), f32),
            dma((2, COLORS)), dma((2,)), dma((2, COLORS)), dma((2, COLORS)),
            dma((COLORS, CHUNKS)), dma((COLORS, CHUNKS)), dma((COLORS, CHUNKS)),
            dma, dma, dma, dma((5,)),
        ],
        compiler_params=pltpu.CompilerParams(has_side_effects=True, vmem_limit_bytes=66_000_000),
    )(grad_mat, grad_vec)


def gather_kernel(rows, share, vec_share, sum_ref, vec_sum_ref, square_ref, master_ref, moment_ref, second_ref,
                  vec_master_ref, vec_moment_ref, vec_second_ref,
                  new_master_ref, new_moment_ref, new_second_ref,
                  vec_new_master_ref, vec_new_moment_ref, vec_new_second_ref, land_ref, vec_land_ref,
                  state_in, state_sem, send_sem, recv_sem, core_send_sem, core_recv_sem, vec_sem):
    me = lax.axis_index(AXIS)
    partner = me + flip_of(me, 1)
    flips = [[flip_of(me, bit) for bit in order] for order in ORDERS]
    color_rows = share // COLORS // LANES

    def rows_at(color, chunk):
        return pl.ds(pl.multiple_of(color * color_rows + chunk * rows, rows), rows)

    def state_copies(chunk, color, slot):
        at = rows_at(color, chunk)
        return [pltpu.make_async_copy(ref.at[at], state_in.at[slot, index], state_sem.at[slot, index])
                for index, ref in enumerate((sum_ref, master_ref, moment_ref, second_ref))]

    def link_copy(stage, owner, color, chunk, hop):
        piece = land_ref.at[owner, rows_at(color, chunk)]
        return pltpu.make_async_remote_copy(
            piece, piece, send_sem.at[color], recv_sem.at[stage, color, chunk],
            device_id=(me + flips[color][hop],), device_id_type=MESH)

    def core_copy(owner, color, chunk):
        piece = land_ref.at[owner, rows_at(color, chunk)]
        return pltpu.make_async_remote_copy(
            piece, piece, core_send_sem.at[color], core_recv_sem.at[color],
            device_id=(partner,), device_id_type=MESH)

    for copy in state_copies(0, 0, 0):
        copy.start()
    norm = jnp.sqrt(square_ref[...][:, :1])
    clip_coef = jnp.minimum(1.0, 1.0 / (norm + NORM_EPS))

    def update_chunk(chunk, carry):
        for color in range(COLORS):
            item = chunk * COLORS + color
            slot = item % 2
            if color + 1 < COLORS:
                for copy in state_copies(chunk, color + 1, (item + 1) % 2):
                    copy.start()
            else:
                @pl.when(chunk + 1 < CHUNKS)
                def _():
                    for copy in state_copies(chunk + 1, 0, (item + 1) % 2):
                        copy.start()
            for copy in state_copies(chunk, color, slot):
                copy.wait()
            base = color * color_rows + chunk * rows

            def update(sub, inner):
                to = pl.ds(pl.multiple_of(sub * UPDATE_ROWS, UPDATE_ROWS), UPDATE_ROWS)
                out = pl.ds(pl.multiple_of(base + sub * UPDATE_ROWS, UPDATE_ROWS), UPDATE_ROWS)
                master, moment, second = adam_update(
                    state_in[slot, 0, to, :], clip_coef, state_in[slot, 1, to, :],
                    state_in[slot, 2, to, :], state_in[slot, 3, to, :], DECAY)
                new_master_ref[out, :] = master
                new_moment_ref[out, :] = moment
                new_second_ref[out, :] = second
                land_ref[me, out, :] = master.astype(jnp.bfloat16)
                return inner

            lax.fori_loop(0, rows // UPDATE_ROWS, update, 0)
            link_copy(0, me, color, chunk, 0).start()
        return carry

    lax.fori_loop(0, CHUNKS, update_chunk, 0)

    vec_new = adam_update(vec_sum_ref[...], clip_coef, vec_master_ref[...], vec_moment_ref[...], vec_second_ref[...], 0.0)
    vec_new_master_ref[...], vec_new_moment_ref[...], vec_new_second_ref[...] = vec_new
    vec_land_ref[me] = vec_new[0].reshape(vec_share // LANES, LANES)

    def own_sends(chunk, carry):
        for color in range(COLORS):
            link_copy(1, me, color, chunk, 1).start()
            core_copy(me, color, chunk).start()
        return carry

    lax.fori_loop(0, CHUNKS, own_sends, 0)

    def own_sends_last(chunk, carry):
        for color in range(COLORS):
            link_copy(3, me, color, chunk, 2).start()
        return carry

    lax.fori_loop(0, CHUNKS, own_sends_last, 0)

    def vec_send(dist, carry):
        pltpu.make_async_remote_copy(
            vec_land_ref.at[me], vec_land_ref.at[me], vec_sem.at[0], vec_sem.at[1],
            device_id=((me + dist) % GROUP,), device_id_type=MESH).start()
        return carry

    lax.fori_loop(1, GROUP, vec_send, 0)

    def arrivals(stage, hops, onward):
        def one_chunk(chunk, carry):
            for color in range(COLORS):
                owner = me + sum(flips[color][hop] for hop in hops)
                pltpu.make_async_copy(land_ref.at[owner, rows_at(color, chunk)], land_ref.at[owner, rows_at(color, chunk)],
                                      recv_sem.at[stage, color, chunk]).wait()
                for next_stage, hop in onward:
                    link_copy(next_stage, owner, color, chunk, hop).start()
                core_copy(owner, color, chunk).start()
            return carry

        lax.fori_loop(0, CHUNKS, one_chunk, 0)

    arrivals(0, (0,), ((2, 1), (4, 2)))
    arrivals(1, (1,), ((5, 2),))
    arrivals(3, (2,), ())
    arrivals(2, (0, 1), ((6, 2),))
    arrivals(4, (0, 2), ())
    arrivals(5, (1, 2), ())
    arrivals(6, (0, 1, 2), ())

    def wait_bytes(ref, sem):
        pltpu.make_async_copy(ref, ref, sem).wait()

    for color in range(COLORS):
        eight = land_ref.at[pl.ds(0, 8), pl.ds(color * color_rows, color_rows)]
        wait_bytes(land_ref.at[pl.ds(0, 7), pl.ds(color * color_rows, color_rows)], send_sem.at[color])
        wait_bytes(eight, core_send_sem.at[color])
        wait_bytes(eight, core_recv_sem.at[color])
    for index in range(2):
        wait_bytes(vec_land_ref.at[pl.ds(0, GROUP - 1)], vec_sem.at[index])


def gather_call(sums, states, vec_states):
    sum_mat, sum_vec, square = sums
    share, vec_share = sum_mat.size, sum_vec.size
    rows = share // COLORS // CHUNKS // LANES
    hbm_spec = pl.BlockSpec(memory_space=pltpu.HBM)
    vmem_spec = pl.BlockSpec(memory_space=pltpu.VMEM)
    f32, bf16 = jnp.float32, jnp.bfloat16
    dma = pltpu.SemaphoreType.DMA
    mat_out = pltpu.VMEM((share // LANES, LANES), f32)
    vec_out = pltpu.VMEM((1, vec_share), f32)
    return pl.pallas_call(
        functools.partial(gather_kernel, rows, share, vec_share),
        name='update_gather',
        out_shape=(mat_out,) * 3 + (vec_out,) * 3 + (
            pltpu.VMEM((GROUP, share // LANES, LANES), bf16), pltpu.VMEM((GROUP, vec_share // LANES, LANES), f32)),
        in_specs=[hbm_spec, vmem_spec, vmem_spec] + [hbm_spec] * 3 + [vmem_spec] * 3,
        out_specs=(vmem_spec,) * 8,
        scratch_shapes=[
            pltpu.VMEM((2, 4, rows, LANES), f32), dma((2, 4)),
            dma((COLORS,)), dma((7, COLORS, CHUNKS)), dma((COLORS,)), dma((COLORS,)), dma((2,)),
        ],
        compiler_params=pltpu.CompilerParams(has_side_effects=True, vmem_limit_bytes=GATHER_VMEM),
    )(sum_mat, sum_vec, square, *states, *vec_states)


def store_kernel(*refs):
    ins, outs, (vec_weights, sems) = refs[:8], refs[8:16], refs[16:]
    land, vec_land = ins[6:]
    copies = [pltpu.make_async_copy(source, target, sems.at[index])
              for index, (source, target) in enumerate(zip(ins[:6], outs[:6]))]
    for owner in range(GROUP):
        copies.append(pltpu.make_async_copy(land.at[owner], outs[6].at[owner], sems.at[6 + owner]))
    for copy in copies:
        copy.start()
    vec_rows = vec_land.shape[1]
    for owner in range(GROUP):
        vec_weights[owner * vec_rows:(owner + 1) * vec_rows, :] = vec_land[owner]
    outs[7][...] = vec_weights[...].astype(jnp.bfloat16)
    for copy in copies:
        copy.wait()


def store_call(results):
    vmem_spec = pl.BlockSpec(memory_space=pltpu.VMEM)
    hbm_spec = pl.BlockSpec(memory_space=pltpu.HBM)
    dma = pltpu.SemaphoreType.DMA
    vec_rows = results[7].size // LANES
    return pl.pallas_call(
        store_kernel,
        name='store_results',
        out_shape=tuple(jax.ShapeDtypeStruct(result.shape, result.dtype) for result in results[:7]) + (
            jax.ShapeDtypeStruct((vec_rows, LANES), jnp.bfloat16),),
        in_specs=[vmem_spec] * 8,
        out_specs=(hbm_spec,) * 7 + (vmem_spec,),
        scratch_shapes=[pltpu.VMEM((vec_rows, LANES), jnp.float32), dma((6 + GROUP,))],
        compiler_params=pltpu.CompilerParams(vmem_limit_bytes=STORE_VMEM),
    )(*[pltpu.with_memory_space_constraint(result, pltpu.VMEM) for result in results])


def solution(mesh):
    def local_step(grad_mat, grad_vec, master_mat, moment_mat, second_mat, master_vec, moment_vec, second_vec):
        sums = reduce_call(grad_mat, grad_vec)[:3]
        states = [state.reshape(-1, LANES) for state in (master_mat, moment_mat, second_mat)]
        vec_states = [state.reshape(1, -1) for state in (master_vec, moment_vec, second_vec)]
        results = store_call(gather_call(sums, states, vec_states))
        return tuple(result.reshape(-1) for result in results)

    row_spec = P(AXIS, None)
    flat_spec = P(AXIS)
    whole_spec = P()
    return jax.shard_map(local_step, mesh=mesh,
                         in_specs=(row_spec, row_spec) + (flat_spec,) * 6,
                         out_specs=(flat_spec,) * 6 + (whole_spec, whole_spec),
                         check_vma=False)
```

```python
import functools

import jax
import jax.numpy as jnp
from jax import lax
from jax.experimental import pallas as pl
from jax.experimental.pallas import tpu as pltpu
from jax.sharding import PartitionSpec as P

STEP = 4
LEARN_RATE = 1e-3
BETA_ONE = 0.9
BETA_TWO = 0.999
ADAM_EPS = 1e-8
DECAY = 0.01
NORM_EPS = 1e-6
FIX_ONE = 1.0 - BETA_ONE ** STEP
FIX_TWO = 1.0 - BETA_TWO ** STEP

AXIS = 'fsdp'
MESH = pl.DeviceIdType.MESH
GROUP = 16
LANES = 128
ORDERS = ((2, 4, 8), (4, 8, 2), (8, 2, 4))
COLORS = len(ORDERS)
CHUNKS = 8
AHEAD = 3
SUB_ROWS = 80
UPDATE_ROWS = 80
RING = 4
ITEMS = 12
SCRATCH_BYTES = 12_700_000


def adam_update(grad_sum, clip_coef, master, moment, second, decay):
    clip_grad = clip_coef * grad_sum
    new_moment = BETA_ONE * moment + (1.0 - BETA_ONE) * clip_grad
    new_second = BETA_TWO * second + (1.0 - BETA_TWO) * clip_grad * clip_grad
    step_dir = (new_moment / FIX_ONE) / (jnp.sqrt(new_second / FIX_TWO) + ADAM_EPS)
    new_master = master - LEARN_RATE * (step_dir + decay * master)
    return new_master, new_moment, new_second


def flip_of(me, bit):
    return bit * (1 - 2 * ((me // bit) % 2))


def step_kernel(rows, share, vec_share, grad_ref, vec_ref, master_ref, moment_ref, second_ref,
                vec_master_ref, vec_moment_ref, vec_second_ref,
                new_master_ref, new_moment_ref, new_second_ref,
                vec_new_master_ref, vec_new_moment_ref, vec_new_second_ref, weights_ref, vec_weights_ref,
                land_ref, recv2,
                pad_in, keep, recv2_in, recv3, vec_land, square_land, square_acc,
                pad_sem, part_sem, recv2_in_sem, state_sem,
                send1_sem, send2_sem, send3_sem, recv1_sem, recv2_sem, recv3_sem, small_sem,
                send_sem, recv_sem, core_send_sem, core_recv_sem):
    me = lax.axis_index(AXIS)
    core = me % 2
    partner = me + flip_of(me, 1)
    block = rows * LANES
    color_len = share // COLORS
    color_rows = color_len // LANES
    flips = [[flip_of(me, bit) for bit in order] for order in ORDERS]
    per_owner = share // LANES // rows

    def wait_bytes(ref, sem):
        pltpu.make_async_copy(ref, ref, sem).wait()

    def rows_at(color, chunk):
        return pl.ds(pl.multiple_of(color * color_rows + chunk * rows, rows), rows)

    def piece_at(owner, color, chunk):
        start = pl.multiple_of(owner * share + color * color_len + chunk * block, block)
        return grad_ref.at[:, pl.ds(start, block)]

    def packed_at(index):
        return index // per_owner, pl.multiple_of((index % per_owner) * rows, rows)

    def packed_index(color, chunk, item):
        return (chunk * COLORS + color) * ITEMS + item

    part_owner = COLORS * CHUNKS * ITEMS // per_owner
    part_rows = 3 * rows

    def part_at(slot, color):
        return (slot * COLORS + color) * part_rows

    def small_copy(dist):
        other = (me + dist) % GROUP
        return pltpu.make_async_remote_copy(
            vec_ref.at[:, pl.ds(pl.multiple_of(other * vec_share, vec_share), vec_share)], vec_land.at[me],
            small_sem.at[0], small_sem.at[1], device_id=(other,), device_id_type=MESH)

    def small_start(dist, carry):
        small_copy(dist).start()
        return carry

    def route(item, color):
        place, kind = item // 3, (item + 1) % 3
        flip1, flip2, flip3 = flips[color]
        local = (2 - kind) // 2
        target_core = local * (1 - core) + (1 - local) * (kind - 1)
        target = me - core + (1 - local) * flip1 + target_core
        owner = target + (1 - place // 2) * flip2 + (1 - place % 2) * flip3
        source = (1 - local) * (1 + core)
        return owner, target, source, place

    def in_copy(chunk, item, color):
        owner = route(item, color)[0]
        return pltpu.make_async_copy(piece_at(owner, color, chunk), pad_in.at[item % 2, color], pad_sem.at[item % 2, color])

    def pack_and_send(chunk):
        for color in range(COLORS):
            in_copy(chunk, 0, color).start()

        def one_item(item, carry):
            @pl.when(item + 1 < ITEMS)
            def _():
                for color in range(COLORS):
                    in_copy(chunk, item + 1, color).start()

            for color in range(COLORS):
                in_copy(chunk, item, color).wait()
                place_owner, place_row = packed_at(packed_index(color, chunk, item))

                def pack(sub, inner):
                    off = pl.multiple_of(sub * SUB_ROWS * LANES, SUB_ROWS * LANES)
                    vals = pad_in[item % 2, color, :, pl.ds(off, SUB_ROWS * LANES)].astype(jnp.float32)
                    to = pl.multiple_of(place_row + sub * SUB_ROWS, SUB_ROWS)
                    weights_ref[place_owner, pl.ds(to, SUB_ROWS), :] = (
                        vals.reshape(SUB_ROWS, LANES).astype(jnp.bfloat16))
                    return inner

                lax.fori_loop(0, rows // SUB_ROWS, pack, 0, unroll=True)
            for color in range(COLORS):
                owner, target, source, place = route(item, color)
                place_owner, place_row = packed_at(packed_index(color, chunk, item))
                pltpu.make_async_remote_copy(
                    weights_ref.at[place_owner, pl.ds(place_row, rows)],
                    land_ref.at[color, chunk, place, pl.ds(pl.multiple_of(source * rows, rows), rows)],
                    send1_sem.at[chunk], recv1_sem.at[color, chunk], device_id=(target,), device_id_type=MESH).start()
            return carry

        lax.fori_loop(0, ITEMS, one_item, 0)

    def part_copies(chunk, place, color, slot):
        flip1, flip2, flip3 = flips[color]
        owner = me + (1 - place // 2) * flip2 + (1 - place % 2) * flip3
        return (pltpu.make_async_copy(land_ref.at[color, chunk, place],
                                      weights_ref.at[part_owner, pl.ds(part_at(slot, color), part_rows)],
                                      part_sem.at[slot, color]),
                pltpu.make_async_copy(piece_at(owner, color, chunk), pad_in.at[slot, color], pad_sem.at[slot, color]))

    def first_sums(chunk):
        for color in range(COLORS):
            wait_bytes(land_ref.at[color, chunk], recv1_sem.at[color, chunk])
            for copy in part_copies(chunk, 0, color, 0):
                copy.start()
        for place in range(4):
            slot = place % 2
            for color in range(COLORS):
                if place < 3:
                    for copy in part_copies(chunk, place + 1, color, (place + 1) % 2):
                        copy.start()
                for copy in part_copies(chunk, place, color, slot):
                    copy.wait()
                at = rows_at(color, chunk)
                total = (new_moment_ref.at[at], new_second_ref.at[at], keep.at[chunk, color], new_master_ref.at[at])[place]

                def add(sub, inner):
                    off = pl.multiple_of(sub * SUB_ROWS * LANES, SUB_ROWS * LANES)
                    to = pl.ds(pl.multiple_of(sub * SUB_ROWS, SUB_ROWS), SUB_ROWS)
                    vals = pad_in[slot, color, :, pl.ds(off, SUB_ROWS * LANES)].astype(jnp.float32)
                    vals = vals.reshape(SUB_ROWS, LANES)
                    for source in range(3):
                        row = pl.multiple_of(part_at(slot, color) + source * rows + sub * SUB_ROWS, SUB_ROWS)
                        vals = vals + weights_ref[part_owner, pl.ds(row, SUB_ROWS), :].astype(jnp.float32)
                    total[to, :] = vals
                    return inner

                lax.fori_loop(0, rows // SUB_ROWS, add, 0, unroll=True)
                if place < 2:
                    pltpu.make_async_remote_copy(
                        total, recv2.at[chunk, color, place], send2_sem.at[place], recv2_sem.at[color, chunk],
                        device_id=(me + flips[color][1],), device_id_type=MESH).start()

    pack_and_send(0)
    lax.fori_loop(1, GROUP, small_start, 0)
    vec_own = pltpu.make_async_copy(
        vec_ref.at[:, pl.ds(pl.multiple_of(me * vec_share, vec_share), vec_share)], vec_land.at[me], small_sem.at[2])
    vec_own.start()

    def pack_ahead(chunk, carry):
        pack_and_send(chunk)
        return carry

    lax.fori_loop(1, AHEAD, pack_ahead, 0)

    def first_stage(chunk, carry):
        first_sums(chunk)

        @pl.when(chunk + AHEAD < CHUNKS)
        def _():
            pack_and_send(chunk + AHEAD)

        return carry

    lax.fori_loop(0, CHUNKS, first_stage, 0)

    def second_stage(chunk, carry):
        copies = [pltpu.make_async_copy(recv2.at[chunk, color], recv2_in.at[color], recv2_in_sem.at[color])
                  for color in range(COLORS)]
        for color in range(COLORS):
            wait_bytes(recv2.at[chunk, color], recv2_sem.at[color, chunk])
            copies[color].start()
        for color in range(COLORS):
            copies[color].wait()
            base = color * color_rows + chunk * rows

            def add(sub, inner):
                to = pl.ds(pl.multiple_of(sub * SUB_ROWS, SUB_ROWS), SUB_ROWS)
                out = pl.ds(pl.multiple_of(base + sub * SUB_ROWS, SUB_ROWS), SUB_ROWS)
                keep[chunk, color, to, :] += recv2_in[color, 0, to, :]
                new_master_ref[out, :] += recv2_in[color, 1, to, :]
                return inner

            lax.fori_loop(0, rows // SUB_ROWS, add, 0)
            pltpu.make_async_remote_copy(
                keep.at[chunk, color], recv3.at[chunk, color], send3_sem.at[chunk], recv3_sem.at[color, chunk],
                device_id=(me + flips[color][2],), device_id_type=MESH).start()
        return carry

    lax.fori_loop(0, CHUNKS, second_stage, 0)

    vec_own.wait()
    wait_bytes(vec_land.at[pl.ds(0, GROUP - 1)], small_sem.at[1])
    vec_sum = jnp.sum(vec_land[...].astype(jnp.float32), axis=0)
    square_acc[...] = jnp.zeros_like(square_acc)
    vec_square = sum(vec_sum[:, part * LANES:(part + 1) * LANES] ** 2 for part in range(vec_share // LANES))

    def third_stage(chunk, carry):
        for color in range(COLORS):
            wait_bytes(recv3.at[chunk, color], recv3_sem.at[color, chunk])
            base = color * color_rows + chunk * rows

            def add(sub, inner):
                to = pl.ds(pl.multiple_of(sub * SUB_ROWS, SUB_ROWS), SUB_ROWS)
                out = pl.ds(pl.multiple_of(base + sub * SUB_ROWS, SUB_ROWS), SUB_ROWS)
                vals = new_master_ref[out, :] + recv3[chunk, color, to, :]
                new_master_ref[out, :] = vals
                square_acc[...] += jnp.sum((vals * vals).reshape(SUB_ROWS // 8, 8, LANES), axis=0)
                return inner

            lax.fori_loop(0, rows // SUB_ROWS, add, 0)
        return carry

    def state_copies(chunk, color):
        slot = (chunk * COLORS + color) % RING
        at = rows_at(color, chunk)
        return [pltpu.make_async_copy(ref.at[at], keep.at[slot, index], state_sem.at[slot, index])
                for index, ref in enumerate((master_ref, moment_ref, second_ref))]

    lax.fori_loop(0, CHUNKS - 2, third_stage, 0)
    for chunk in range(RING):
        wait_bytes(keep.at[chunk], send3_sem.at[chunk])
    for item in range(RING):
        for copy in state_copies(item // COLORS, item % COLORS):
            copy.start()
    lax.fori_loop(CHUNKS - 2, CHUNKS, third_stage, 0)

    def wait_packed(chunk, carry):
        wait_bytes(weights_ref.at[pl.ds(0, COLORS), pl.ds(0, ITEMS * rows)], send1_sem.at[chunk])
        return carry

    lax.fori_loop(0, CHUNKS, wait_packed, 0)
    square_land[me] = jnp.sum(square_acc[...], axis=0, keepdims=True) + vec_square

    def square_copy(dist, carry):
        pltpu.make_async_remote_copy(
            square_land.at[me], square_land.at[me], small_sem.at[3], small_sem.at[4],
            device_id=((me + dist) % GROUP,), device_id_type=MESH).start()
        return carry

    lax.fori_loop(1, GROUP, square_copy, 0)
    wait_bytes(new_moment_ref, send2_sem.at[0])
    wait_bytes(new_second_ref, send2_sem.at[1])
    wait_bytes(square_land.at[pl.ds(0, GROUP - 1)], small_sem.at[4])
    norm = jnp.sqrt(jnp.sum(jnp.sum(square_land[...], axis=0), axis=1, keepdims=True))
    clip_coef = jnp.minimum(1.0, 1.0 / (norm + NORM_EPS))

    def link_copy(stage, owner, color, chunk, hop):
        piece = weights_ref.at[owner, rows_at(color, chunk)]
        return pltpu.make_async_remote_copy(
            piece, piece, send_sem.at[color], recv_sem.at[stage, color, chunk],
            device_id=(me + flips[color][hop],), device_id_type=MESH)

    def core_copy(owner, color, chunk):
        piece = weights_ref.at[owner, rows_at(color, chunk)]
        return pltpu.make_async_remote_copy(
            piece, piece, core_send_sem.at[color], core_recv_sem.at[color],
            device_id=(partner,), device_id_type=MESH)

    def update_chunk(chunk, carry):
        for color in range(COLORS):
            item = chunk * COLORS + color
            slot = item % RING
            for copy in state_copies(chunk, color):
                copy.wait()
            base = color * color_rows + chunk * rows

            def update(sub, inner):
                to = pl.ds(pl.multiple_of(sub * UPDATE_ROWS, UPDATE_ROWS), UPDATE_ROWS)
                out = pl.ds(pl.multiple_of(base + sub * UPDATE_ROWS, UPDATE_ROWS), UPDATE_ROWS)
                master, moment, second = adam_update(
                    new_master_ref[out, :], clip_coef, keep[slot, 0, to, :],
                    keep[slot, 1, to, :], keep[slot, 2, to, :], DECAY)
                new_master_ref[out, :] = master
                new_moment_ref[out, :] = moment
                new_second_ref[out, :] = second
                weights_ref[me, out, :] = master.astype(jnp.bfloat16)
                return inner

            lax.fori_loop(0, rows // UPDATE_ROWS, update, 0)
            link_copy(0, me, color, chunk, 0).start()

            @pl.when(item + RING < CHUNKS * COLORS)
            def _():
                for copy in state_copies((item + RING) // COLORS, (item + RING) % COLORS):
                    copy.start()
        return carry

    lax.fori_loop(0, CHUNKS, update_chunk, 0)

    vec_new = adam_update(vec_sum, clip_coef, vec_master_ref[...], vec_moment_ref[...], vec_second_ref[...], 0.0)
    vec_new_master_ref[...], vec_new_moment_ref[...], vec_new_second_ref[...] = vec_new
    vec_weights_ref[me] = vec_new[0].reshape(vec_share // LANES, LANES)

    def own_sends(chunk, carry):
        for color in range(COLORS):
            link_copy(1, me, color, chunk, 1).start()
            core_copy(me, color, chunk).start()
        return carry

    lax.fori_loop(0, CHUNKS, own_sends, 0)

    def own_sends_last(chunk, carry):
        for color in range(COLORS):
            link_copy(3, me, color, chunk, 2).start()
        return carry

    lax.fori_loop(0, CHUNKS, own_sends_last, 0)

    def vec_send(dist, carry):
        pltpu.make_async_remote_copy(
            vec_weights_ref.at[me], vec_weights_ref.at[me], small_sem.at[5], small_sem.at[6],
            device_id=((me + dist) % GROUP,), device_id_type=MESH).start()
        return carry

    lax.fori_loop(1, GROUP, vec_send, 0)

    def arrivals(stage, hops, onward):
        def one_chunk(chunk, carry):
            for color in range(COLORS):
                owner = me + sum(flips[color][hop] for hop in hops)
                wait_bytes(weights_ref.at[owner, rows_at(color, chunk)], recv_sem.at[stage, color, chunk])
                for next_stage, hop in onward:
                    link_copy(next_stage, owner, color, chunk, hop).start()
                core_copy(owner, color, chunk).start()
            return carry

        lax.fori_loop(0, CHUNKS, one_chunk, 0)

    arrivals(0, (0,), ((2, 1), (4, 2)))
    arrivals(1, (1,), ((5, 2),))
    arrivals(3, (2,), ())
    arrivals(2, (0, 1), ((6, 2),))
    arrivals(4, (0, 2), ())
    arrivals(5, (1, 2), ())
    arrivals(6, (0, 1, 2), ())

    for color in range(COLORS):
        eight = weights_ref.at[pl.ds(0, 8), pl.ds(color * color_rows, color_rows)]
        wait_bytes(weights_ref.at[pl.ds(0, 7), pl.ds(color * color_rows, color_rows)], send_sem.at[color])
        wait_bytes(eight, core_send_sem.at[color])
        wait_bytes(eight, core_recv_sem.at[color])
    for index in (5, 6):
        wait_bytes(vec_weights_ref.at[pl.ds(0, GROUP - 1)], small_sem.at[index])
    for chunk in range(RING, CHUNKS):
        wait_bytes(keep.at[chunk], send3_sem.at[chunk])
    wait_bytes(vec_land.at[pl.ds(0, GROUP - 1)], small_sem.at[0])
    wait_bytes(square_land.at[pl.ds(0, GROUP - 1)], small_sem.at[3])


def step_call(grad_mat, grad_vec, states, vec_states):
    share = grad_mat.shape[1] // GROUP
    vec_share = grad_vec.shape[1] // GROUP
    rows = share // COLORS // CHUNKS // LANES
    hbm_spec = pl.BlockSpec(memory_space=pltpu.HBM)
    vmem_spec = pl.BlockSpec(memory_space=pltpu.VMEM)
    f32, bf16 = jnp.float32, jnp.bfloat16
    dma = pltpu.SemaphoreType.DMA
    return pl.pallas_call(
        functools.partial(step_kernel, rows, share, vec_share),
        name='adam_step',
        out_shape=(pltpu.VMEM((share // LANES, LANES), f32),) * 3 + (pltpu.VMEM((1, vec_share), f32),) * 3 + (
            pltpu.VMEM((GROUP, share // LANES, LANES), bf16),
            pltpu.VMEM((GROUP, vec_share // LANES, LANES), f32),
            jax.ShapeDtypeStruct((COLORS, CHUNKS, 4, 3 * rows, LANES), bf16),
            jax.ShapeDtypeStruct((CHUNKS, COLORS, 2, rows, LANES), f32)),
        in_specs=[hbm_spec] * 5 + [vmem_spec] * 3,
        out_specs=(vmem_spec,) * 8 + (hbm_spec,) * 2,
        scratch_shapes=[
            pltpu.VMEM((2, COLORS, 1, rows * LANES), bf16),
            pltpu.VMEM((CHUNKS, COLORS, rows, LANES), f32),
            pltpu.VMEM((COLORS, 2, rows, LANES), f32),
            pltpu.VMEM((CHUNKS, COLORS, rows, LANES), f32),
            pltpu.VMEM((GROUP, 1, vec_share), bf16),
            pltpu.VMEM((GROUP, 1, LANES), f32),
            pltpu.VMEM((8, LANES), f32),
            dma((2, COLORS)), dma((2, COLORS)), dma((COLORS,)), dma((RING, 3)),
            dma((CHUNKS,)), dma((2,)), dma((CHUNKS,)),
            dma((COLORS, CHUNKS)), dma((COLORS, CHUNKS)), dma((COLORS, CHUNKS)), dma((7,)),
            dma((COLORS,)), dma((7, COLORS, CHUNKS)), dma((COLORS,)), dma((COLORS,)),
        ],
        compiler_params=pltpu.CompilerParams(has_side_effects=True, vmem_limit_bytes=SCRATCH_BYTES),
    )(grad_mat, grad_vec, *states, *vec_states)[:8]


def store_kernel(*refs):
    ins, outs, (vec_weights, sems) = refs[:8], refs[8:16], refs[16:]
    land, vec_land = ins[6:]
    copies = [pltpu.make_async_copy(source, target, sems.at[index])
              for index, (source, target) in enumerate(zip(ins[:6], outs[:6]))]
    for owner in range(GROUP):
        copies.append(pltpu.make_async_copy(land.at[owner], outs[6].at[owner], sems.at[6 + owner]))
    for copy in copies:
        copy.start()
    vec_rows = vec_land.shape[1]
    for owner in range(GROUP):
        vec_weights[owner * vec_rows:(owner + 1) * vec_rows, :] = vec_land[owner]
    outs[7][...] = vec_weights[...].astype(jnp.bfloat16)
    for copy in copies:
        copy.wait()


def store_call(results):
    vmem_spec = pl.BlockSpec(memory_space=pltpu.VMEM)
    hbm_spec = pl.BlockSpec(memory_space=pltpu.HBM)
    dma = pltpu.SemaphoreType.DMA
    vec_rows = results[7].size // LANES
    return pl.pallas_call(
        store_kernel,
        name='store_results',
        out_shape=tuple(jax.ShapeDtypeStruct(result.shape, result.dtype) for result in results[:7]) + (
            jax.ShapeDtypeStruct((vec_rows, LANES), jnp.bfloat16),),
        in_specs=[vmem_spec] * 8,
        out_specs=(hbm_spec,) * 7 + (vmem_spec,),
        scratch_shapes=[pltpu.VMEM((vec_rows, LANES), jnp.float32), dma((6 + GROUP,))],
        compiler_params=pltpu.CompilerParams(vmem_limit_bytes=SCRATCH_BYTES),
    )(*[pltpu.with_memory_space_constraint(result, pltpu.VMEM) for result in results])


def solution(mesh):
    def local_step(grad_mat, grad_vec, master_mat, moment_mat, second_mat, master_vec, moment_vec, second_vec):
        states = [state.reshape(-1, LANES) for state in (master_mat, moment_mat, second_mat)]
        vec_states = [state.reshape(1, -1) for state in (master_vec, moment_vec, second_vec)]
        results = store_call(step_call(grad_mat, grad_vec, states, vec_states))
        return tuple(result.reshape(-1) for result in results)

    row_spec = P(AXIS, None)
    flat_spec = P(AXIS)
    whole_spec = P()
    return jax.shard_map(local_step, mesh=mesh,
                         in_specs=(row_spec, row_spec) + (flat_spec,) * 6,
                         out_specs=(flat_spec,) * 6 + (whole_spec, whole_spec),
                         check_vma=False)
```

```python
import functools

import jax
import jax.numpy as jnp
from jax import lax
from jax.experimental import pallas as pl
from jax.experimental.pallas import tpu as pltpu
from jax.sharding import PartitionSpec as P

STEP = 4
LEARN_RATE = 1e-3
BETA_ONE = 0.9
BETA_TWO = 0.999
ADAM_EPS = 1e-8
DECAY = 0.01
NORM_EPS = 1e-6
FIX_ONE = 1.0 - BETA_ONE ** STEP
FIX_TWO = 1.0 - BETA_TWO ** STEP

AXIS = 'fsdp'
MESH = pl.DeviceIdType.MESH
GROUP = 16
LANES = 128
ORDERS = ((2, 4, 8), (4, 8, 2), (8, 2, 4))
COLORS = len(ORDERS)
CHUNKS = 8
AHEAD = 3
SUB_ROWS = 80
UPDATE_ROWS = 80
RING = 4
STATE_PARTS = 2
ITEMS = 12
SCRATCH_BYTES = 12_700_000


def adam_update(grad_sum, clip_coef, master, moment, second, decay):
    clip_grad = clip_coef * grad_sum
    new_moment = BETA_ONE * moment + (1.0 - BETA_ONE) * clip_grad
    new_second = BETA_TWO * second + (1.0 - BETA_TWO) * clip_grad * clip_grad
    step_dir = (new_moment / FIX_ONE) / (jnp.sqrt(new_second / FIX_TWO) + ADAM_EPS)
    new_master = master - LEARN_RATE * (step_dir + decay * master)
    return new_master, new_moment, new_second


def flip_of(me, bit):
    return bit * (1 - 2 * ((me // bit) % 2))


def step_kernel(rows, share, vec_share, grad_ref, vec_ref, master_ref, moment_ref, second_ref,
                vec_master_ref, vec_moment_ref, vec_second_ref,
                new_master_ref, new_moment_ref, new_second_ref,
                vec_new_master_ref, vec_new_moment_ref, vec_new_second_ref, weights_ref, vec_weights_ref,
                land_ref, recv2,
                pad_in, keep, recv2_in, recv3, vec_land, square_land, square_acc,
                pad_sem, part_sem, recv2_in_sem, state_sem,
                send1_sem, send2_sem, send3_sem, recv1_sem, recv2_sem, recv3_sem, small_sem,
                send_sem, recv_sem, core_send_sem, core_recv_sem):
    me = lax.axis_index(AXIS)
    core = me % 2
    partner = me + flip_of(me, 1)
    block = rows * LANES
    color_len = share // COLORS
    color_rows = color_len // LANES
    flips = [[flip_of(me, bit) for bit in order] for order in ORDERS]
    per_owner = share // LANES // rows
    neighbours = [partner] + [me + flip_of(me, bit) + other for bit in ORDERS[0] for other in (0, flip_of(me, 1))]
    others = [me + sum(flip_of(me, bit) for bit in (1, 2, 4, 8) if mask & bit)
              for mask in sorted(range(1, GROUP), key=lambda mask: (-(mask >> 1).bit_count(), mask))]

    def wait_bytes(ref, sem):
        pltpu.make_async_copy(ref, ref, sem).wait()

    def rows_at(color, chunk):
        return pl.ds(pl.multiple_of(color * color_rows + chunk * rows, rows), rows)

    def piece_at(owner, color, chunk):
        start = pl.multiple_of(owner * share + color * color_len + chunk * block, block)
        return grad_ref.at[:, pl.ds(start, block)]

    def packed_at(index):
        return index // per_owner, pl.multiple_of((index % per_owner) * rows, rows)

    def packed_index(color, chunk, item):
        return (chunk * COLORS + color) * ITEMS + item

    part_owner = COLORS * CHUNKS * ITEMS // per_owner
    part_rows = 3 * rows

    def part_at(slot, color):
        return (slot * COLORS + color) * part_rows

    def route(item, color):
        place, kind = item // 3, (item + 1) % 3
        flip1, flip2, flip3 = flips[color]
        local = (2 - kind) // 2
        target_core = local * (1 - core) + (1 - local) * (kind - 1)
        target = me - core + (1 - local) * flip1 + target_core
        owner = target + (1 - place // 2) * flip2 + (1 - place % 2) * flip3
        source = (1 - local) * (1 + core)
        return owner, target, source, place

    def in_copy(chunk, item, color):
        owner = route(item, color)[0]
        return pltpu.make_async_copy(piece_at(owner, color, chunk), pad_in.at[item % 2, color], pad_sem.at[item % 2, color])

    def start_in(chunk, item):
        for color in range(COLORS):
            in_copy(chunk, item, color).start()

    def pack_item(chunk, item):
        for color in range(COLORS):
            in_copy(chunk, item, color).wait()
            place_owner, place_row = packed_at(packed_index(color, chunk, item))

            def pack(sub, inner):
                off = pl.multiple_of(sub * SUB_ROWS * LANES, SUB_ROWS * LANES)
                vals = pad_in[item % 2, color, :, pl.ds(off, SUB_ROWS * LANES)].astype(jnp.float32)
                to = pl.multiple_of(place_row + sub * SUB_ROWS, SUB_ROWS)
                weights_ref[place_owner, pl.ds(to, SUB_ROWS), :] = (
                    vals.reshape(SUB_ROWS, LANES).astype(jnp.bfloat16))
                return inner

            lax.fori_loop(0, rows // SUB_ROWS, pack, 0, unroll=True)

    def send_item(chunk, item):
        for color in range(COLORS):
            owner, target, source, place = route(item, color)
            place_owner, place_row = packed_at(packed_index(color, chunk, item))
            pltpu.make_async_remote_copy(
                weights_ref.at[place_owner, pl.ds(place_row, rows)],
                land_ref.at[color, chunk, place, pl.ds(pl.multiple_of(source * rows, rows), rows)],
                send1_sem.at[chunk], recv1_sem.at[color, chunk], device_id=(target,), device_id_type=MESH).start()

    def pack_and_send(chunk, first):
        def one_item(item, carry):
            @pl.when(item + 1 < ITEMS)
            def _():
                start_in(chunk, item + 1)

            pack_item(chunk, item)
            send_item(chunk, item)
            return carry

        lax.fori_loop(first, ITEMS, one_item, 0)

    def part_copies(chunk, place, color, slot):
        flip1, flip2, flip3 = flips[color]
        owner = me + (1 - place // 2) * flip2 + (1 - place % 2) * flip3
        return (pltpu.make_async_copy(land_ref.at[color, chunk, place],
                                      weights_ref.at[part_owner, pl.ds(part_at(slot, color), part_rows)],
                                      part_sem.at[slot, color]),
                pltpu.make_async_copy(piece_at(owner, color, chunk), pad_in.at[slot, color], pad_sem.at[slot, color]))

    def first_sums(chunk):
        for color in range(COLORS):
            wait_bytes(land_ref.at[color, chunk], recv1_sem.at[color, chunk])
            for copy in part_copies(chunk, 0, color, 0):
                copy.start()
        for place in range(4):
            slot = place % 2
            for color in range(COLORS):
                if place < 3:
                    for copy in part_copies(chunk, place + 1, color, (place + 1) % 2):
                        copy.start()
                for copy in part_copies(chunk, place, color, slot):
                    copy.wait()
                at = rows_at(color, chunk)
                total = (new_moment_ref.at[at], new_second_ref.at[at], keep.at[chunk, color], new_master_ref.at[at])[place]

                def add(sub, inner):
                    off = pl.multiple_of(sub * SUB_ROWS * LANES, SUB_ROWS * LANES)
                    to = pl.ds(pl.multiple_of(sub * SUB_ROWS, SUB_ROWS), SUB_ROWS)
                    vals = pad_in[slot, color, :, pl.ds(off, SUB_ROWS * LANES)].astype(jnp.float32)
                    vals = vals.reshape(SUB_ROWS, LANES)
                    for source in range(3):
                        row = pl.multiple_of(part_at(slot, color) + source * rows + sub * SUB_ROWS, SUB_ROWS)
                        vals = vals + weights_ref[part_owner, pl.ds(row, SUB_ROWS), :].astype(jnp.float32)
                    total[to, :] = vals
                    return inner

                lax.fori_loop(0, rows // SUB_ROWS, add, 0, unroll=True)
                if place < 2:
                    pltpu.make_async_remote_copy(
                        total, recv2.at[chunk, color, place], send2_sem.at[place], recv2_sem.at[color, chunk],
                        device_id=(me + flips[color][1],), device_id_type=MESH).start()

    start_in(0, 0)
    start_in(0, 1)
    barrier = pltpu.get_barrier_semaphore()
    for neighbour in neighbours:
        pl.semaphore_signal(barrier, inc=1, device_id=(neighbour,), device_id_type=MESH)
    pack_item(0, 0)
    pl.semaphore_wait(barrier, len(neighbours))
    send_item(0, 0)
    pack_and_send(0, 1)

    def pack_ahead(chunk, carry):
        start_in(chunk, 0)
        pack_and_send(chunk, 0)
        return carry

    lax.fori_loop(1, AHEAD, pack_ahead, 0)

    def first_stage(chunk, carry):
        first_sums(chunk)

        @pl.when(chunk + AHEAD < CHUNKS)
        def _():
            start_in(chunk + AHEAD, 0)
            pack_and_send(chunk + AHEAD, 0)

        return carry

    lax.fori_loop(0, CHUNKS, first_stage, 0)

    def second_stage(chunk, carry):
        copies = [pltpu.make_async_copy(recv2.at[chunk, color], recv2_in.at[color], recv2_in_sem.at[color])
                  for color in range(COLORS)]
        for color in range(COLORS):
            wait_bytes(recv2.at[chunk, color], recv2_sem.at[color, chunk])
            copies[color].start()
        for color in range(COLORS):
            copies[color].wait()
            base = color * color_rows + chunk * rows

            def add(sub, inner):
                to = pl.ds(pl.multiple_of(sub * SUB_ROWS, SUB_ROWS), SUB_ROWS)
                out = pl.ds(pl.multiple_of(base + sub * SUB_ROWS, SUB_ROWS), SUB_ROWS)
                keep[chunk, color, to, :] += recv2_in[color, 0, to, :]
                new_master_ref[out, :] += recv2_in[color, 1, to, :]
                return inner

            lax.fori_loop(0, rows // SUB_ROWS, add, 0)
            pltpu.make_async_remote_copy(
                keep.at[chunk, color], recv3.at[chunk, color], send3_sem.at[chunk], recv3_sem.at[color, chunk],
                device_id=(me + flips[color][2],), device_id_type=MESH).start()
        return carry

    second_stage(0, 0)
    for other in others:
        pltpu.make_async_remote_copy(
            vec_ref.at[:, pl.ds(pl.multiple_of(other * vec_share, vec_share), vec_share)], vec_land.at[me],
            small_sem.at[0], small_sem.at[1], device_id=(other,), device_id_type=MESH).start()
    vec_own = pltpu.make_async_copy(
        vec_ref.at[:, pl.ds(pl.multiple_of(me * vec_share, vec_share), vec_share)], vec_land.at[me], small_sem.at[2])
    vec_own.start()
    lax.fori_loop(1, CHUNKS, second_stage, 0)

    square_acc[...] = jnp.zeros_like(square_acc)

    def third_stage(chunk, carry):
        for color in range(COLORS):
            wait_bytes(recv3.at[chunk, color], recv3_sem.at[color, chunk])
            base = color * color_rows + chunk * rows

            def add(sub, inner):
                to = pl.ds(pl.multiple_of(sub * SUB_ROWS, SUB_ROWS), SUB_ROWS)
                out = pl.ds(pl.multiple_of(base + sub * SUB_ROWS, SUB_ROWS), SUB_ROWS)
                vals = new_master_ref[out, :] + recv3[chunk, color, to, :]
                new_master_ref[out, :] = vals
                square_acc[...] += jnp.sum((vals * vals).reshape(SUB_ROWS // 8, 8, LANES), axis=0)
                return inner

            lax.fori_loop(0, rows // SUB_ROWS, add, 0)
        return carry

    def state_copies(chunk, color):
        slot = (chunk * COLORS + color) % RING
        at = rows_at(color, chunk)
        return [pltpu.make_async_copy(ref.at[at], keep.at[slot, index], state_sem.at[slot, index])
                for index, ref in enumerate((master_ref, moment_ref, second_ref))]

    lax.fori_loop(0, CHUNKS - 2, third_stage, 0)
    for chunk in range(RING):
        wait_bytes(keep.at[chunk], send3_sem.at[chunk])
    for item in range(RING):
        for copy in state_copies(item // COLORS, item % COLORS):
            copy.start()
    third_stage(CHUNKS - 2, 0)

    vec_own.wait()
    wait_bytes(vec_land.at[pl.ds(0, GROUP - 1)], small_sem.at[1])
    vec_sum = jnp.sum(vec_land[...].astype(jnp.float32), axis=0)
    vec_square = sum(vec_sum[:, part * LANES:(part + 1) * LANES] ** 2 for part in range(vec_share // LANES))

    def wait_packed(chunk, carry):
        wait_bytes(weights_ref.at[pl.ds(0, COLORS), pl.ds(0, ITEMS * rows)], send1_sem.at[chunk])
        return carry

    lax.fori_loop(0, CHUNKS, wait_packed, 0)
    third_stage(CHUNKS - 1, 0)
    square_land[me] = jnp.sum(square_acc[...], axis=0, keepdims=True) + vec_square

    for other in others:
        pltpu.make_async_remote_copy(
            square_land.at[me], square_land.at[me], small_sem.at[3], small_sem.at[4],
            device_id=(other,), device_id_type=MESH).start()
    wait_bytes(new_moment_ref, send2_sem.at[0])
    wait_bytes(new_second_ref, send2_sem.at[1])
    wait_bytes(square_land.at[pl.ds(0, GROUP - 1)], small_sem.at[4])
    norm = jnp.sqrt(jnp.sum(jnp.sum(square_land[...], axis=0), axis=1, keepdims=True))
    clip_coef = jnp.minimum(1.0, 1.0 / (norm + NORM_EPS))

    def link_copy(stage, owner, color, chunk, hop):
        piece = weights_ref.at[owner, rows_at(color, chunk)]
        return pltpu.make_async_remote_copy(
            piece, piece, send_sem.at[color], recv_sem.at[stage, color, chunk],
            device_id=(me + flips[color][hop],), device_id_type=MESH)

    def core_copy(owner, color, chunk):
        piece = weights_ref.at[owner, rows_at(color, chunk)]
        return pltpu.make_async_remote_copy(
            piece, piece, core_send_sem.at[color], core_recv_sem.at[color],
            device_id=(partner,), device_id_type=MESH)

    def update_chunk(chunk, carry):
        for color in range(COLORS):
            item = chunk * COLORS + color
            slot = item % RING
            for copy in state_copies(chunk, color):
                copy.wait()
            base = color * color_rows + chunk * rows

            def update(sub, inner):
                to = pl.ds(pl.multiple_of(sub * UPDATE_ROWS, UPDATE_ROWS), UPDATE_ROWS)
                out = pl.ds(pl.multiple_of(base + sub * UPDATE_ROWS, UPDATE_ROWS), UPDATE_ROWS)
                master, moment, second = adam_update(
                    new_master_ref[out, :], clip_coef, keep[slot, 0, to, :],
                    keep[slot, 1, to, :], keep[slot, 2, to, :], DECAY)
                new_master_ref[out, :] = master
                new_moment_ref[out, :] = moment
                new_second_ref[out, :] = second
                weights_ref[me, out, :] = master.astype(jnp.bfloat16)
                return inner

            lax.fori_loop(0, rows // UPDATE_ROWS, update, 0)
            link_copy(0, me, color, chunk, 0).start()

            @pl.when(chunk == 0)
            def _():
                link_copy(1, me, color, chunk, 1).start()
                link_copy(3, me, color, chunk, 2).start()

            @pl.when(item + RING < CHUNKS * COLORS)
            def _():
                for copy in state_copies((item + RING) // COLORS, (item + RING) % COLORS):
                    copy.start()
        return carry

    lax.fori_loop(0, CHUNKS, update_chunk, 0)

    vec_new = adam_update(vec_sum, clip_coef, vec_master_ref[...], vec_moment_ref[...], vec_second_ref[...], 0.0)
    vec_new_master_ref[...], vec_new_moment_ref[...], vec_new_second_ref[...] = vec_new
    vec_weights_ref[me] = vec_new[0].reshape(vec_share // LANES, LANES)

    def own_sends(chunk, carry):
        for color in range(COLORS):
            @pl.when(chunk > 0)
            def _():
                link_copy(1, me, color, chunk, 1).start()

            core_copy(me, color, chunk).start()
        return carry

    lax.fori_loop(0, CHUNKS, own_sends, 0)

    def own_sends_last(chunk, carry):
        for color in range(COLORS):
            link_copy(3, me, color, chunk, 2).start()
        return carry

    lax.fori_loop(1, CHUNKS, own_sends_last, 0)

    for other in others:
        pltpu.make_async_remote_copy(
            vec_weights_ref.at[me], vec_weights_ref.at[me], small_sem.at[5], small_sem.at[6],
            device_id=(other,), device_id_type=MESH).start()

    def arrivals(stage, hops, onward):
        def one_chunk(chunk, carry):
            for color in range(COLORS):
                owner = me + sum(flips[color][hop] for hop in hops)
                wait_bytes(weights_ref.at[owner, rows_at(color, chunk)], recv_sem.at[stage, color, chunk])
                for next_stage, hop in onward:
                    link_copy(next_stage, owner, color, chunk, hop).start()
                core_copy(owner, color, chunk).start()
            return carry

        lax.fori_loop(0, CHUNKS, one_chunk, 0)

    arrivals(0, (0,), ((2, 1), (4, 2)))
    arrivals(1, (1,), ((5, 2),))
    arrivals(3, (2,), ())
    arrivals(2, (0, 1), ((6, 2),))
    arrivals(4, (0, 2), ())
    arrivals(5, (1, 2), ())
    arrivals(6, (0, 1, 2), ())

    for color in range(COLORS):
        eight = weights_ref.at[pl.ds(0, 8), pl.ds(color * color_rows, color_rows)]
        wait_bytes(weights_ref.at[pl.ds(0, 7), pl.ds(color * color_rows, color_rows)], send_sem.at[color])
        wait_bytes(eight, core_send_sem.at[color])
        wait_bytes(eight, core_recv_sem.at[color])
    for index in (5, 6):
        wait_bytes(vec_weights_ref.at[pl.ds(0, GROUP - 1)], small_sem.at[index])
    for chunk in range(RING, CHUNKS):
        wait_bytes(keep.at[chunk], send3_sem.at[chunk])
    wait_bytes(vec_land.at[pl.ds(0, GROUP - 1)], small_sem.at[0])
    wait_bytes(square_land.at[pl.ds(0, GROUP - 1)], small_sem.at[3])


def step_call(grad_mat, grad_vec, states, vec_states):
    share = grad_mat.shape[1] // GROUP
    vec_share = grad_vec.shape[1] // GROUP
    rows = share // COLORS // CHUNKS // LANES
    hbm_spec = pl.BlockSpec(memory_space=pltpu.HBM)
    vmem_spec = pl.BlockSpec(memory_space=pltpu.VMEM)
    f32, bf16 = jnp.float32, jnp.bfloat16
    dma = pltpu.SemaphoreType.DMA
    return pl.pallas_call(
        functools.partial(step_kernel, rows, share, vec_share),
        name='adam_step',
        out_shape=(pltpu.VMEM((share // LANES, LANES), f32),) * 3 + (pltpu.VMEM((1, vec_share), f32),) * 3 + (
            pltpu.VMEM((GROUP, share // LANES, LANES), bf16),
            pltpu.VMEM((GROUP, vec_share // LANES, LANES), f32),
            jax.ShapeDtypeStruct((COLORS, CHUNKS, 4, 3 * rows, LANES), bf16),
            jax.ShapeDtypeStruct((CHUNKS, COLORS, 2, rows, LANES), f32)),
        in_specs=[hbm_spec] * 5 + [vmem_spec] * 3,
        out_specs=(vmem_spec,) * 8 + (hbm_spec,) * 2,
        scratch_shapes=[
            pltpu.VMEM((2, COLORS, 1, rows * LANES), bf16),
            pltpu.VMEM((CHUNKS, COLORS, rows, LANES), f32),
            pltpu.VMEM((COLORS, 2, rows, LANES), f32),
            pltpu.VMEM((CHUNKS, COLORS, rows, LANES), f32),
            pltpu.VMEM((GROUP, 1, vec_share), bf16),
            pltpu.VMEM((GROUP, 1, LANES), f32),
            pltpu.VMEM((8, LANES), f32),
            dma((2, COLORS)), dma((2, COLORS)), dma((COLORS,)), dma((RING, 3)),
            dma((CHUNKS,)), dma((2,)), dma((CHUNKS,)),
            dma((COLORS, CHUNKS)), dma((COLORS, CHUNKS)), dma((COLORS, CHUNKS)), dma((7,)),
            dma((COLORS,)), dma((7, COLORS, CHUNKS)), dma((COLORS,)), dma((COLORS,)),
        ],
        compiler_params=pltpu.CompilerParams(
            collective_id=0, has_side_effects=True, vmem_limit_bytes=SCRATCH_BYTES),
    )(grad_mat, grad_vec, *states, *vec_states)[:8]


def store_kernel(*refs):
    ins, outs, (vec_weights, sems) = refs[:8], refs[8:16], refs[16:]
    land, vec_land = ins[6:]
    places = [(ins[index], outs[index]) for index in range(3, 6)]
    for index in range(3):
        part = ins[index].shape[0] // STATE_PARTS
        places += [(ins[index].at[pl.ds(at * part, part)], outs[index].at[pl.ds(at * part, part)]) for at in range(STATE_PARTS)]
    for owner in range(GROUP):
        places.append((land.at[owner], outs[6].at[owner]))
    copies = [pltpu.make_async_copy(source, target, sems.at[index]) for index, (source, target) in enumerate(places)]
    for copy in copies:
        copy.start()
    vec_rows = vec_land.shape[1]
    for owner in range(GROUP):
        vec_weights[owner * vec_rows:(owner + 1) * vec_rows, :] = vec_land[owner]
    outs[7][...] = vec_weights[...].astype(jnp.bfloat16)
    for copy in copies:
        copy.wait()


def store_call(results):
    vmem_spec = pl.BlockSpec(memory_space=pltpu.VMEM)
    hbm_spec = pl.BlockSpec(memory_space=pltpu.HBM)
    dma = pltpu.SemaphoreType.DMA
    vec_rows = results[7].size // LANES
    return pl.pallas_call(
        store_kernel,
        name='store_results',
        out_shape=tuple(jax.ShapeDtypeStruct(result.shape, result.dtype) for result in results[:7]) + (
            jax.ShapeDtypeStruct((vec_rows, LANES), jnp.bfloat16),),
        in_specs=[vmem_spec] * 8,
        out_specs=(hbm_spec,) * 7 + (vmem_spec,),
        scratch_shapes=[pltpu.VMEM((vec_rows, LANES), jnp.float32), dma((3 + 3 * STATE_PARTS + GROUP,))],
        compiler_params=pltpu.CompilerParams(vmem_limit_bytes=SCRATCH_BYTES),
    )(*[pltpu.with_memory_space_constraint(result, pltpu.VMEM) for result in results])


def solution(mesh):
    def local_step(grad_mat, grad_vec, master_mat, moment_mat, second_mat, master_vec, moment_vec, second_vec):
        states = [state.reshape(-1, LANES) for state in (master_mat, moment_mat, second_mat)]
        vec_states = [state.reshape(1, -1) for state in (master_vec, moment_vec, second_vec)]
        results = store_call(step_call(grad_mat, grad_vec, states, vec_states))
        return tuple(result.reshape(-1) for result in results)

    row_spec = P(AXIS, None)
    flat_spec = P(AXIS)
    whole_spec = P()
    return jax.shard_map(local_step, mesh=mesh,
                         in_specs=(row_spec, row_spec) + (flat_spec,) * 6,
                         out_specs=(flat_spec,) * 6 + (whole_spec, whole_spec),
                         check_vma=False)
```

```python
import functools

import jax
import jax.numpy as jnp
from jax import lax
from jax.experimental import pallas as pl
from jax.experimental.pallas import tpu as pltpu
from jax.sharding import PartitionSpec as P

STEP = 4
LEARN_RATE = 1e-3
BETA_ONE = 0.9
BETA_TWO = 0.999
ADAM_EPS = 1e-8
DECAY = 0.01
NORM_EPS = 1e-6
FIX_ONE = 1.0 - BETA_ONE ** STEP
FIX_TWO = 1.0 - BETA_TWO ** STEP

AXIS = 'fsdp'
MESH = pl.DeviceIdType.MESH
GROUP = 16
LANES = 128
ORDERS = ((2, 4, 8), (4, 8, 2), (8, 2, 4))
COLORS = len(ORDERS)
CHUNKS = 8
AHEAD = 3
SUB_ROWS = 80
UPDATE_ROWS = 80
RING = 4
STATE_PARTS = 2
ITEMS = 12
SCRATCH_BYTES = 12_700_000


def adam_update(grad_sum, clip_coef, master, moment, second, decay):
    clip_grad = clip_coef * grad_sum
    new_moment = BETA_ONE * moment + (1.0 - BETA_ONE) * clip_grad
    new_second = BETA_TWO * second + (1.0 - BETA_TWO) * clip_grad * clip_grad
    step_dir = (new_moment / FIX_ONE) / (jnp.sqrt(new_second / FIX_TWO) + ADAM_EPS)
    new_master = master - LEARN_RATE * (step_dir + decay * master)
    return new_master, new_moment, new_second


def flip_of(me, bit):
    return bit * (1 - 2 * ((me // bit) % 2))


def step_kernel(rows, share, vec_share, grad_ref, vec_ref, master_ref, moment_ref, second_ref,
                vec_master_ref, vec_moment_ref, vec_second_ref,
                new_master_ref, new_moment_ref, new_second_ref,
                vec_new_master_ref, vec_new_moment_ref, vec_new_second_ref, weights_ref, vec_weights_ref,
                land_ref, recv2,
                pad_in, keep, recv2_in, recv3, vec_land, square_land, square_acc,
                pad_sem, part_sem, recv2_in_sem, state_sem,
                send1_sem, send2_sem, send3_sem, recv1_sem, recv2_sem, recv3_sem, small_sem,
                send_sem, recv_sem, core_send_sem, core_recv_sem):
    me = lax.axis_index(AXIS)
    core = me % 2
    partner = me + flip_of(me, 1)
    block = rows * LANES
    color_len = share // COLORS
    color_rows = color_len // LANES
    flips = [[flip_of(me, bit) for bit in order] for order in ORDERS]
    per_owner = share // LANES // rows
    neighbours = [partner] + [me + flip_of(me, bit) + other for bit in ORDERS[0] for other in (0, flip_of(me, 1))]
    others = [me + sum(flip_of(me, bit) for bit in (1, 2, 4, 8) if mask & bit)
              for mask in sorted(range(1, GROUP), key=lambda mask: (-(mask >> 1).bit_count(), mask))]

    def wait_bytes(ref, sem):
        pltpu.make_async_copy(ref, ref, sem).wait()

    def rows_at(color, chunk):
        return pl.ds(pl.multiple_of(color * color_rows + chunk * rows, rows), rows)

    def piece_at(owner, color, chunk):
        start = pl.multiple_of(owner * share + color * color_len + chunk * block, block)
        return grad_ref.at[:, pl.ds(start, block)]

    def packed_at(index):
        return index // per_owner, pl.multiple_of((index % per_owner) * rows, rows)

    def packed_index(color, chunk, item):
        return (chunk * COLORS + color) * ITEMS + item

    part_owner = COLORS * CHUNKS * ITEMS // per_owner
    part_rows = 3 * rows

    def part_at(slot, color):
        return (slot * COLORS + color) * part_rows

    def route(item, color):
        place, kind = item // 3, (item + 1) % 3
        flip1, flip2, flip3 = flips[color]
        local = (2 - kind) // 2
        target_core = local * (1 - core) + (1 - local) * (kind - 1)
        target = me - core + (1 - local) * flip1 + target_core
        owner = target + (1 - place // 2) * flip2 + (1 - place % 2) * flip3
        source = (1 - local) * (1 + core)
        return owner, target, source, place

    def in_copy(chunk, item, color):
        owner = route(item, color)[0]
        return pltpu.make_async_copy(piece_at(owner, color, chunk), pad_in.at[item % 2, color], pad_sem.at[item % 2, color])

    def start_in(chunk, item):
        for color in range(COLORS):
            in_copy(chunk, item, color).start()

    def pack_item(chunk, item):
        for color in range(COLORS):
            in_copy(chunk, item, color).wait()
            place_owner, place_row = packed_at(packed_index(color, chunk, item))

            def pack(sub, inner):
                off = pl.multiple_of(sub * SUB_ROWS * LANES, SUB_ROWS * LANES)
                vals = pad_in[item % 2, color, :, pl.ds(off, SUB_ROWS * LANES)].astype(jnp.float32)
                to = pl.multiple_of(place_row + sub * SUB_ROWS, SUB_ROWS)
                weights_ref[place_owner, pl.ds(to, SUB_ROWS), :] = (
                    vals.reshape(SUB_ROWS, LANES).astype(jnp.bfloat16))
                return inner

            lax.fori_loop(0, rows // SUB_ROWS, pack, 0, unroll=True)

    def send_item(chunk, item):
        for color in range(COLORS):
            owner, target, source, place = route(item, color)
            place_owner, place_row = packed_at(packed_index(color, chunk, item))
            pltpu.make_async_remote_copy(
                weights_ref.at[place_owner, pl.ds(place_row, rows)],
                land_ref.at[color, chunk, place, pl.ds(pl.multiple_of(source * rows, rows), rows)],
                send1_sem.at[chunk], recv1_sem.at[color, chunk], device_id=(target,), device_id_type=MESH).start()

    def pack_and_send(chunk, first):
        def one_item(item, carry):
            @pl.when(item + 1 < ITEMS)
            def _():
                start_in(chunk, item + 1)

            pack_item(chunk, item)
            send_item(chunk, item)
            return carry

        lax.fori_loop(first, ITEMS, one_item, 0)

    def part_copies(chunk, place, color, slot):
        flip1, flip2, flip3 = flips[color]
        owner = me + (1 - place // 2) * flip2 + (1 - place % 2) * flip3
        return (pltpu.make_async_copy(land_ref.at[color, chunk, place],
                                      weights_ref.at[part_owner, pl.ds(part_at(slot, color), part_rows)],
                                      part_sem.at[slot, color]),
                pltpu.make_async_copy(piece_at(owner, color, chunk), pad_in.at[slot, color], pad_sem.at[slot, color]))

    def first_sums(chunk):
        for color in range(COLORS):
            wait_bytes(land_ref.at[color, chunk], recv1_sem.at[color, chunk])
            for copy in part_copies(chunk, 0, color, 0):
                copy.start()
        for place in range(4):
            slot = place % 2
            for color in range(COLORS):
                if place < 3:
                    for copy in part_copies(chunk, place + 1, color, (place + 1) % 2):
                        copy.start()
                for copy in part_copies(chunk, place, color, slot):
                    copy.wait()
                at = rows_at(color, chunk)
                total = (new_moment_ref.at[at], new_second_ref.at[at], keep.at[chunk, color], new_master_ref.at[at])[place]

                def add(sub, inner):
                    off = pl.multiple_of(sub * SUB_ROWS * LANES, SUB_ROWS * LANES)
                    to = pl.ds(pl.multiple_of(sub * SUB_ROWS, SUB_ROWS), SUB_ROWS)
                    vals = pad_in[slot, color, :, pl.ds(off, SUB_ROWS * LANES)].astype(jnp.float32)
                    vals = vals.reshape(SUB_ROWS, LANES)
                    for source in range(3):
                        row = pl.multiple_of(part_at(slot, color) + source * rows + sub * SUB_ROWS, SUB_ROWS)
                        vals = vals + weights_ref[part_owner, pl.ds(row, SUB_ROWS), :].astype(jnp.float32)
                    total[to, :] = vals
                    return inner

                lax.fori_loop(0, rows // SUB_ROWS, add, 0, unroll=True)
                if place < 2:
                    pltpu.make_async_remote_copy(
                        total, recv2.at[chunk, color, place], send2_sem.at[place], recv2_sem.at[color, chunk],
                        device_id=(me + flips[color][1],), device_id_type=MESH).start()

    start_in(0, 0)
    start_in(0, 1)
    barrier = pltpu.get_barrier_semaphore()
    for neighbour in neighbours:
        pl.semaphore_signal(barrier, inc=1, device_id=(neighbour,), device_id_type=MESH)
    pack_item(0, 0)
    pl.semaphore_wait(barrier, len(neighbours))
    send_item(0, 0)
    pack_and_send(0, 1)

    def pack_ahead(chunk, carry):
        start_in(chunk, 0)
        pack_and_send(chunk, 0)
        return carry

    lax.fori_loop(1, AHEAD, pack_ahead, 0)

    def first_stage(chunk, carry):
        first_sums(chunk)

        @pl.when(chunk + AHEAD < CHUNKS)
        def _():
            start_in(chunk + AHEAD, 0)
            pack_and_send(chunk + AHEAD, 0)

        return carry

    lax.fori_loop(0, CHUNKS, first_stage, 0)

    def second_stage(chunk, carry):
        copies = [pltpu.make_async_copy(recv2.at[chunk, color], recv2_in.at[color], recv2_in_sem.at[color])
                  for color in range(COLORS)]
        for color in range(COLORS):
            wait_bytes(recv2.at[chunk, color], recv2_sem.at[color, chunk])
            copies[color].start()
        for color in range(COLORS):
            copies[color].wait()
            base = color * color_rows + chunk * rows

            def add(sub, inner):
                to = pl.ds(pl.multiple_of(sub * SUB_ROWS, SUB_ROWS), SUB_ROWS)
                out = pl.ds(pl.multiple_of(base + sub * SUB_ROWS, SUB_ROWS), SUB_ROWS)
                keep[chunk, color, to, :] += recv2_in[color, 0, to, :]
                new_master_ref[out, :] += recv2_in[color, 1, to, :]
                return inner

            lax.fori_loop(0, rows // SUB_ROWS, add, 0)
            pltpu.make_async_remote_copy(
                keep.at[chunk, color], recv3.at[chunk, color], send3_sem.at[chunk], recv3_sem.at[color, chunk],
                device_id=(me + flips[color][2],), device_id_type=MESH).start()
        return carry

    second_stage(0, 0)
    for other in others:
        pltpu.make_async_remote_copy(
            vec_ref.at[:, pl.ds(pl.multiple_of(other * vec_share, vec_share), vec_share)], vec_land.at[me],
            small_sem.at[0], small_sem.at[1], device_id=(other,), device_id_type=MESH).start()
    vec_own = pltpu.make_async_copy(
        vec_ref.at[:, pl.ds(pl.multiple_of(me * vec_share, vec_share), vec_share)], vec_land.at[me], small_sem.at[2])
    vec_own.start()
    lax.fori_loop(1, CHUNKS, second_stage, 0)

    square_acc[...] = jnp.zeros_like(square_acc)

    def third_stage(chunk, carry):
        for color in range(COLORS):
            wait_bytes(recv3.at[chunk, color], recv3_sem.at[color, chunk])
            base = color * color_rows + chunk * rows

            def add(sub, squares):
                to = pl.ds(pl.multiple_of(sub * SUB_ROWS, SUB_ROWS), SUB_ROWS)
                out = pl.ds(pl.multiple_of(base + sub * SUB_ROWS, SUB_ROWS), SUB_ROWS)
                vals = new_master_ref[out, :] + recv3[chunk, color, to, :]
                new_master_ref[out, :] = vals
                return squares + jnp.sum((vals * vals).reshape(SUB_ROWS // 8, 8, LANES), axis=0)

            squares = lax.fori_loop(0, rows // SUB_ROWS, add, jnp.zeros((8, LANES), jnp.float32), unroll=True)
            square_acc[...] += squares
        return carry

    def state_copies(chunk, color):
        slot = (chunk * COLORS + color) % RING
        at = rows_at(color, chunk)
        return [pltpu.make_async_copy(ref.at[at], keep.at[slot, index], state_sem.at[slot, index])
                for index, ref in enumerate((master_ref, moment_ref, second_ref))]

    lax.fori_loop(0, CHUNKS - 2, third_stage, 0)
    for chunk in range(RING):
        wait_bytes(keep.at[chunk], send3_sem.at[chunk])
    for item in range(RING):
        for copy in state_copies(item // COLORS, item % COLORS):
            copy.start()
    third_stage(CHUNKS - 2, 0)

    vec_own.wait()
    wait_bytes(vec_land.at[pl.ds(0, GROUP - 1)], small_sem.at[1])
    vec_sum = jnp.sum(vec_land[...].astype(jnp.float32), axis=0)
    vec_square = sum(vec_sum[:, part * LANES:(part + 1) * LANES] ** 2 for part in range(vec_share // LANES))

    def wait_packed(chunk, carry):
        wait_bytes(weights_ref.at[pl.ds(0, COLORS), pl.ds(0, ITEMS * rows)], send1_sem.at[chunk])
        return carry

    lax.fori_loop(0, CHUNKS, wait_packed, 0)
    third_stage(CHUNKS - 1, 0)
    square_land[me] = jnp.sum(square_acc[...], axis=0, keepdims=True) + vec_square

    for other in others:
        pltpu.make_async_remote_copy(
            square_land.at[me], square_land.at[me], small_sem.at[3], small_sem.at[4],
            device_id=(other,), device_id_type=MESH).start()
    wait_bytes(new_moment_ref, send2_sem.at[0])
    wait_bytes(new_second_ref, send2_sem.at[1])
    wait_bytes(square_land.at[pl.ds(0, GROUP - 1)], small_sem.at[4])
    norm = jnp.sqrt(jnp.sum(jnp.sum(square_land[...], axis=0), axis=1, keepdims=True))
    clip_coef = jnp.minimum(1.0, 1.0 / (norm + NORM_EPS))

    def link_copy(stage, owner, color, chunk, hop, part=None):
        piece = weights_ref.at[owner, rows_at(color, chunk) if part is None else part]
        return pltpu.make_async_remote_copy(
            piece, piece, send_sem.at[color], recv_sem.at[stage, color, chunk],
            device_id=(me + flips[color][hop],), device_id_type=MESH)

    def core_copy(owner, color, chunk):
        piece = weights_ref.at[owner, rows_at(color, chunk)]
        return pltpu.make_async_remote_copy(
            piece, piece, core_send_sem.at[color], core_recv_sem.at[color],
            device_id=(partner,), device_id_type=MESH)

    def update_chunk(chunk, first):
        for color in range(COLORS):
            item = chunk * COLORS + color
            slot = item % RING
            for copy in state_copies(chunk, color):
                copy.wait()
            base = color * color_rows + chunk * rows

            def update(sub, inner):
                to = pl.ds(pl.multiple_of(sub * UPDATE_ROWS, UPDATE_ROWS), UPDATE_ROWS)
                out = pl.ds(pl.multiple_of(base + sub * UPDATE_ROWS, UPDATE_ROWS), UPDATE_ROWS)
                master, moment, second = adam_update(
                    new_master_ref[out, :], clip_coef, keep[slot, 0, to, :],
                    keep[slot, 1, to, :], keep[slot, 2, to, :], DECAY)
                new_master_ref[out, :] = master
                new_moment_ref[out, :] = moment
                new_second_ref[out, :] = second
                weights_ref[me, out, :] = master.astype(jnp.bfloat16)
                if first:
                    for stage, hop in ((0, 0), (1, 1), (3, 2)):
                        link_copy(stage, me, color, chunk, hop, out).start()
                return inner

            lax.fori_loop(0, rows // UPDATE_ROWS, update, 0)
            if not first:
                link_copy(0, me, color, chunk, 0).start()

            @pl.when(item + RING < CHUNKS * COLORS)
            def _():
                for copy in state_copies((item + RING) // COLORS, (item + RING) % COLORS):
                    copy.start()

    def update_later(chunk, carry):
        update_chunk(chunk, False)
        return carry

    update_chunk(0, True)
    lax.fori_loop(1, CHUNKS, update_later, 0)

    vec_new = adam_update(vec_sum, clip_coef, vec_master_ref[...], vec_moment_ref[...], vec_second_ref[...], 0.0)
    vec_new_master_ref[...], vec_new_moment_ref[...], vec_new_second_ref[...] = vec_new
    vec_weights_ref[me] = vec_new[0].reshape(vec_share // LANES, LANES)

    def own_sends(chunk, carry):
        for color in range(COLORS):
            @pl.when(chunk > 0)
            def _():
                link_copy(1, me, color, chunk, 1).start()

            core_copy(me, color, chunk).start()
        return carry

    lax.fori_loop(0, CHUNKS, own_sends, 0)

    def own_sends_last(chunk, carry):
        for color in range(COLORS):
            link_copy(3, me, color, chunk, 2).start()
        return carry

    lax.fori_loop(1, CHUNKS, own_sends_last, 0)

    for other in others:
        pltpu.make_async_remote_copy(
            vec_weights_ref.at[me], vec_weights_ref.at[me], small_sem.at[5], small_sem.at[6],
            device_id=(other,), device_id_type=MESH).start()

    def arrivals(stage, hops, onward):
        def one_chunk(chunk, carry):
            for color in range(COLORS):
                owner = me + sum(flips[color][hop] for hop in hops)
                wait_bytes(weights_ref.at[owner, rows_at(color, chunk)], recv_sem.at[stage, color, chunk])
                for next_stage, hop in onward:
                    link_copy(next_stage, owner, color, chunk, hop).start()
                core_copy(owner, color, chunk).start()
            return carry

        lax.fori_loop(0, CHUNKS, one_chunk, 0)

    arrivals(0, (0,), ((2, 1), (4, 2)))
    arrivals(1, (1,), ((5, 2),))
    arrivals(3, (2,), ())
    arrivals(2, (0, 1), ((6, 2),))
    arrivals(4, (0, 2), ())
    arrivals(5, (1, 2), ())
    arrivals(6, (0, 1, 2), ())

    for color in range(COLORS):
        eight = weights_ref.at[pl.ds(0, 8), pl.ds(color * color_rows, color_rows)]
        wait_bytes(weights_ref.at[pl.ds(0, 7), pl.ds(color * color_rows, color_rows)], send_sem.at[color])
        wait_bytes(eight, core_send_sem.at[color])
        wait_bytes(eight, core_recv_sem.at[color])
    for index in (5, 6):
        wait_bytes(vec_weights_ref.at[pl.ds(0, GROUP - 1)], small_sem.at[index])
    for chunk in range(RING, CHUNKS):
        wait_bytes(keep.at[chunk], send3_sem.at[chunk])
    wait_bytes(vec_land.at[pl.ds(0, GROUP - 1)], small_sem.at[0])
    wait_bytes(square_land.at[pl.ds(0, GROUP - 1)], small_sem.at[3])


def step_call(grad_mat, grad_vec, states, vec_states):
    share = grad_mat.shape[1] // GROUP
    vec_share = grad_vec.shape[1] // GROUP
    rows = share // COLORS // CHUNKS // LANES
    hbm_spec = pl.BlockSpec(memory_space=pltpu.HBM)
    vmem_spec = pl.BlockSpec(memory_space=pltpu.VMEM)
    f32, bf16 = jnp.float32, jnp.bfloat16
    dma = pltpu.SemaphoreType.DMA
    return pl.pallas_call(
        functools.partial(step_kernel, rows, share, vec_share),
        name='adam_step',
        out_shape=(pltpu.VMEM((share // LANES, LANES), f32),) * 3 + (pltpu.VMEM((1, vec_share), f32),) * 3 + (
            pltpu.VMEM((GROUP, share // LANES, LANES), bf16),
            pltpu.VMEM((GROUP, vec_share // LANES, LANES), f32),
            jax.ShapeDtypeStruct((COLORS, CHUNKS, 4, 3 * rows, LANES), bf16),
            jax.ShapeDtypeStruct((CHUNKS, COLORS, 2, rows, LANES), f32)),
        in_specs=[hbm_spec] * 5 + [vmem_spec] * 3,
        out_specs=(vmem_spec,) * 8 + (hbm_spec,) * 2,
        scratch_shapes=[
            pltpu.VMEM((2, COLORS, 1, rows * LANES), bf16),
            pltpu.VMEM((CHUNKS, COLORS, rows, LANES), f32),
            pltpu.VMEM((COLORS, 2, rows, LANES), f32),
            pltpu.VMEM((CHUNKS, COLORS, rows, LANES), f32),
            pltpu.VMEM((GROUP, 1, vec_share), bf16),
            pltpu.VMEM((GROUP, 1, LANES), f32),
            pltpu.VMEM((8, LANES), f32),
            dma((2, COLORS)), dma((2, COLORS)), dma((COLORS,)), dma((RING, 3)),
            dma((CHUNKS,)), dma((2,)), dma((CHUNKS,)),
            dma((COLORS, CHUNKS)), dma((COLORS, CHUNKS)), dma((COLORS, CHUNKS)), dma((7,)),
            dma((COLORS,)), dma((7, COLORS, CHUNKS)), dma((COLORS,)), dma((COLORS,)),
        ],
        compiler_params=pltpu.CompilerParams(
            collective_id=0, has_side_effects=True, vmem_limit_bytes=SCRATCH_BYTES),
    )(grad_mat, grad_vec, *states, *vec_states)[:8]


def store_kernel(*refs):
    ins, outs, (vec_weights, sems) = refs[:8], refs[8:16], refs[16:]
    land, vec_land = ins[6:]
    places = [(ins[index], outs[index]) for index in range(3, 6)]
    for index in range(3):
        part = ins[index].shape[0] // STATE_PARTS
        places += [(ins[index].at[pl.ds(at * part, part)], outs[index].at[pl.ds(at * part, part)]) for at in range(STATE_PARTS)]
    for owner in range(GROUP):
        places.append((land.at[owner], outs[6].at[owner]))
    copies = [pltpu.make_async_copy(source, target, sems.at[index]) for index, (source, target) in enumerate(places)]
    for copy in copies:
        copy.start()
    vec_rows = vec_land.shape[1]
    for owner in range(GROUP):
        vec_weights[owner * vec_rows:(owner + 1) * vec_rows, :] = vec_land[owner]
    outs[7][...] = vec_weights[...].astype(jnp.bfloat16)
    for copy in copies:
        copy.wait()


def store_call(results):
    vmem_spec = pl.BlockSpec(memory_space=pltpu.VMEM)
    hbm_spec = pl.BlockSpec(memory_space=pltpu.HBM)
    dma = pltpu.SemaphoreType.DMA
    vec_rows = results[7].size // LANES
    return pl.pallas_call(
        store_kernel,
        name='store_results',
        out_shape=tuple(jax.ShapeDtypeStruct(result.shape, result.dtype) for result in results[:7]) + (
            jax.ShapeDtypeStruct((vec_rows, LANES), jnp.bfloat16),),
        in_specs=[vmem_spec] * 8,
        out_specs=(hbm_spec,) * 7 + (vmem_spec,),
        scratch_shapes=[pltpu.VMEM((vec_rows, LANES), jnp.float32), dma((3 + 3 * STATE_PARTS + GROUP,))],
        compiler_params=pltpu.CompilerParams(vmem_limit_bytes=SCRATCH_BYTES),
    )(*[pltpu.with_memory_space_constraint(result, pltpu.VMEM) for result in results])


def solution(mesh):
    def local_step(grad_mat, grad_vec, master_mat, moment_mat, second_mat, master_vec, moment_vec, second_vec):
        states = [state.reshape(-1, LANES) for state in (master_mat, moment_mat, second_mat)]
        vec_states = [state.reshape(1, -1) for state in (master_vec, moment_vec, second_vec)]
        results = store_call(step_call(grad_mat, grad_vec, states, vec_states))
        return tuple(result.reshape(-1) for result in results)

    row_spec = P(AXIS, None)
    flat_spec = P(AXIS)
    whole_spec = P()
    return jax.shard_map(local_step, mesh=mesh,
                         in_specs=(row_spec, row_spec) + (flat_spec,) * 6,
                         out_specs=(flat_spec,) * 6 + (whole_spec, whole_spec),
                         check_vma=False)
```

```python
import functools

import jax
import jax.numpy as jnp
from jax import lax
from jax.experimental import pallas as pl
from jax.experimental.pallas import tpu as pltpu
from jax.sharding import PartitionSpec as P

STEP = 4
LEARN_RATE = 1e-3
BETA_ONE = 0.9
BETA_TWO = 0.999
ADAM_EPS = 1e-8
DECAY = 0.01
NORM_EPS = 1e-6
FIX_ONE = 1.0 - BETA_ONE ** STEP
FIX_TWO = 1.0 - BETA_TWO ** STEP

AXIS = 'fsdp'
MESH = pl.DeviceIdType.MESH
GROUP = 16
LANES = 128
ORDERS = ((2, 4, 8), (4, 8, 2), (8, 2, 4))
COLORS = len(ORDERS)
CHUNKS = 8
AHEAD = 3
SLOTS = 3
SUB_ROWS = 80
UPDATE_ROWS = 80
RING = 4
STATE_PARTS = 2
ITEMS = 12
SCRATCH_BYTES = 12_800_000


def adam_update(grad_sum, clip_coef, master, moment, second, decay):
    clip_grad = clip_coef * grad_sum
    new_moment = BETA_ONE * moment + (1.0 - BETA_ONE) * clip_grad
    new_second = BETA_TWO * second + (1.0 - BETA_TWO) * clip_grad * clip_grad
    step_dir = (new_moment / FIX_ONE) / (jnp.sqrt(new_second / FIX_TWO) + ADAM_EPS)
    new_master = master - LEARN_RATE * (step_dir + decay * master)
    return new_master, new_moment, new_second


def flip_of(me, bit):
    return bit * (1 - 2 * ((me // bit) % 2))


def step_kernel(rows, share, vec_share, grad_ref, vec_ref, master_ref, moment_ref, second_ref,
                vec_master_ref, vec_moment_ref, vec_second_ref,
                new_master_ref, new_moment_ref, new_second_ref,
                vec_new_master_ref, vec_new_moment_ref, vec_new_second_ref, weights_ref, vec_weights_ref,
                land_ref, recv2,
                pad_in, keep, recv2_in, recv3, vec_land, square_land, square_acc,
                pad_sem, part_sem, recv2_in_sem, state_sem,
                send1_sem, send2_sem, send3_sem, recv1_sem, recv2_sem, recv3_sem, small_sem,
                send_sem, recv_sem, core_send_sem, core_recv_sem):
    me = lax.axis_index(AXIS)
    core = me % 2
    partner = me + flip_of(me, 1)
    block = rows * LANES
    color_len = share // COLORS
    color_rows = color_len // LANES
    flips = [[flip_of(me, bit) for bit in order] for order in ORDERS]
    per_owner = share // LANES // rows
    neighbours = [partner] + [me + flip_of(me, bit) + other for bit in ORDERS[0] for other in (0, flip_of(me, 1))]
    others = [me + sum(flip_of(me, bit) for bit in (1, 2, 4, 8) if mask & bit)
              for mask in sorted(range(1, GROUP), key=lambda mask: (-(mask >> 1).bit_count(), mask))]

    def wait_bytes(ref, sem):
        pltpu.make_async_copy(ref, ref, sem).wait()

    def rows_at(color, chunk):
        return pl.ds(pl.multiple_of(color * color_rows + chunk * rows, rows), rows)

    def piece_at(owner, color, chunk):
        start = pl.multiple_of(owner * share + color * color_len + chunk * block, block)
        return grad_ref.at[:, pl.ds(start, block)]

    def packed_at(index):
        return index // per_owner, pl.multiple_of((index % per_owner) * rows, rows)

    def packed_index(color, chunk, item):
        return (chunk * COLORS + color) * ITEMS + item

    part_owner = COLORS * CHUNKS * ITEMS // per_owner
    part_rows = 3 * rows

    def route(item, color):
        place, kind = item // 3, (item + 1) % 3
        flip1, flip2, flip3 = flips[color]
        local = (2 - kind) // 2
        target_core = local * (1 - core) + (1 - local) * (kind - 1)
        target = me - core + (1 - local) * flip1 + target_core
        owner = target + (1 - place // 2) * flip2 + (1 - place % 2) * flip3
        source = (1 - local) * (1 + core)
        return owner, target, source, place

    def in_copy(chunk, item, color):
        owner = route(item, color)[0]
        return pltpu.make_async_copy(piece_at(owner, color, chunk), pad_in.at[item % SLOTS, color], pad_sem.at[item % SLOTS])

    def start_in(chunk, item):
        for color in range(COLORS):
            in_copy(chunk, item, color).start()

    def pack_item(chunk, item):
        wait_bytes(pad_in.at[item % SLOTS], pad_sem.at[item % SLOTS])
        for color in range(COLORS):
            place_owner, place_row = packed_at(packed_index(color, chunk, item))

            def pack(sub, inner):
                off = pl.multiple_of(sub * SUB_ROWS * LANES, SUB_ROWS * LANES)
                vals = pad_in[item % SLOTS, color, :, pl.ds(off, SUB_ROWS * LANES)].astype(jnp.float32)
                to = pl.multiple_of(place_row + sub * SUB_ROWS, SUB_ROWS)
                weights_ref[place_owner, pl.ds(to, SUB_ROWS), :] = (
                    vals.reshape(SUB_ROWS, LANES).astype(jnp.bfloat16))
                return inner

            lax.fori_loop(0, rows // SUB_ROWS, pack, 0, unroll=True)

    def send_item(chunk, item):
        for color in range(COLORS):
            owner, target, source, place = route(item, color)
            place_owner, place_row = packed_at(packed_index(color, chunk, item))
            pltpu.make_async_remote_copy(
                weights_ref.at[place_owner, pl.ds(place_row, rows)],
                land_ref.at[color, chunk, place, pl.ds(pl.multiple_of(source * rows, rows), rows)],
                send1_sem.at[chunk], recv1_sem.at[color, chunk], device_id=(target,), device_id_type=MESH).start()

    def pack_and_send(chunk, first):
        def one_item(item, carry):
            @pl.when(item + SLOTS - 1 < ITEMS)
            def _():
                start_in(chunk, item + SLOTS - 1)

            pack_item(chunk, item)
            send_item(chunk, item)
            return carry

        lax.fori_loop(first, ITEMS, one_item, 0)

    def start_parts(chunk, place):
        slot = place % SLOTS
        for color in range(COLORS):
            flip1, flip2, flip3 = flips[color]
            owner = me + (1 - place // 2) * flip2 + (1 - place % 2) * flip3
            pltpu.make_async_copy(land_ref.at[color, chunk, place],
                                  weights_ref.at[part_owner + slot, pl.ds(color * part_rows, part_rows)],
                                  part_sem.at[slot]).start()
            pltpu.make_async_copy(piece_at(owner, color, chunk), pad_in.at[slot, color], pad_sem.at[slot]).start()

    def first_sums(chunk):
        for color in range(COLORS):
            wait_bytes(land_ref.at[color, chunk], recv1_sem.at[color, chunk])
        for place in range(SLOTS - 1):
            start_parts(chunk, place)
        for place in range(4):
            slot = place % SLOTS
            if place + SLOTS - 1 < 4:
                start_parts(chunk, place + SLOTS - 1)
            wait_bytes(weights_ref.at[part_owner + slot, pl.ds(0, COLORS * part_rows)], part_sem.at[slot])
            wait_bytes(pad_in.at[slot], pad_sem.at[slot])
            for color in range(COLORS):
                at = rows_at(color, chunk)
                total = (new_moment_ref.at[at], new_second_ref.at[at], keep.at[chunk, color], new_master_ref.at[at])[place]

                def add(sub, inner):
                    off = pl.multiple_of(sub * SUB_ROWS * LANES, SUB_ROWS * LANES)
                    to = pl.ds(pl.multiple_of(sub * SUB_ROWS, SUB_ROWS), SUB_ROWS)
                    vals = pad_in[slot, color, :, pl.ds(off, SUB_ROWS * LANES)].astype(jnp.float32)
                    vals = vals.reshape(SUB_ROWS, LANES)
                    for source in range(3):
                        row = pl.multiple_of(color * part_rows + source * rows + sub * SUB_ROWS, SUB_ROWS)
                        vals = vals + weights_ref[part_owner + slot, pl.ds(row, SUB_ROWS), :].astype(jnp.float32)
                    total[to, :] = vals
                    return inner

                lax.fori_loop(0, rows // SUB_ROWS, add, 0, unroll=True)
                if place < 2:
                    pltpu.make_async_remote_copy(
                        total, recv2.at[chunk, color, place], send2_sem.at[place], recv2_sem.at[color, chunk],
                        device_id=(me + flips[color][1],), device_id_type=MESH).start()

    for item in range(SLOTS):
        start_in(0, item)
    barrier = pltpu.get_barrier_semaphore()
    for neighbour in neighbours:
        pl.semaphore_signal(barrier, inc=1, device_id=(neighbour,), device_id_type=MESH)
    pack_item(0, 0)
    pl.semaphore_wait(barrier, len(neighbours))
    send_item(0, 0)
    pack_and_send(0, 1)

    def pack_ahead(chunk, carry):
        for item in range(SLOTS - 1):
            start_in(chunk, item)
        pack_and_send(chunk, 0)
        return carry

    lax.fori_loop(1, AHEAD, pack_ahead, 0)

    def first_stage(chunk, carry):
        first_sums(chunk)

        @pl.when(chunk + AHEAD < CHUNKS)
        def _():
            for item in range(SLOTS - 1):
                start_in(chunk + AHEAD, item)
            pack_and_send(chunk + AHEAD, 0)

        return carry

    lax.fori_loop(0, CHUNKS, first_stage, 0)

    def second_stage(chunk, carry):
        copies = [pltpu.make_async_copy(recv2.at[chunk, color], recv2_in.at[color % 2], recv2_in_sem.at[color % 2])
                  for color in range(COLORS)]

        def fetch(color):
            wait_bytes(recv2.at[chunk, color], recv2_sem.at[color, chunk])
            copies[color].start()

        fetch(0)
        fetch(1)
        for color in range(COLORS):
            copies[color].wait()
            base = color * color_rows + chunk * rows

            def add(sub, inner):
                to = pl.ds(pl.multiple_of(sub * SUB_ROWS, SUB_ROWS), SUB_ROWS)
                out = pl.ds(pl.multiple_of(base + sub * SUB_ROWS, SUB_ROWS), SUB_ROWS)
                keep[chunk, color, to, :] += recv2_in[color % 2, 0, to, :]
                new_master_ref[out, :] += recv2_in[color % 2, 1, to, :]
                return inner

            lax.fori_loop(0, rows // SUB_ROWS, add, 0)
            pltpu.make_async_remote_copy(
                keep.at[chunk, color], recv3.at[chunk, color], send3_sem.at[chunk], recv3_sem.at[color, chunk],
                device_id=(me + flips[color][2],), device_id_type=MESH).start()
            if color == 0:
                fetch(2)
        return carry

    second_stage(0, 0)
    for other in others:
        pltpu.make_async_remote_copy(
            vec_ref.at[:, pl.ds(pl.multiple_of(other * vec_share, vec_share), vec_share)], vec_land.at[me],
            small_sem.at[0], small_sem.at[1], device_id=(other,), device_id_type=MESH).start()
    vec_own = pltpu.make_async_copy(
        vec_ref.at[:, pl.ds(pl.multiple_of(me * vec_share, vec_share), vec_share)], vec_land.at[me], small_sem.at[2])
    vec_own.start()
    lax.fori_loop(1, CHUNKS, second_stage, 0)

    square_acc[...] = jnp.zeros_like(square_acc)

    def third_stage(chunk, carry):
        for color in range(COLORS):
            wait_bytes(recv3.at[chunk, color], recv3_sem.at[color, chunk])
            base = color * color_rows + chunk * rows

            def add(sub, squares):
                to = pl.ds(pl.multiple_of(sub * SUB_ROWS, SUB_ROWS), SUB_ROWS)
                out = pl.ds(pl.multiple_of(base + sub * SUB_ROWS, SUB_ROWS), SUB_ROWS)
                vals = new_master_ref[out, :] + recv3[chunk, color, to, :]
                new_master_ref[out, :] = vals
                return squares + jnp.sum((vals * vals).reshape(SUB_ROWS // 8, 8, LANES), axis=0)

            squares = lax.fori_loop(0, rows // SUB_ROWS, add, jnp.zeros((8, LANES), jnp.float32), unroll=True)
            square_acc[...] += squares
        return carry

    def state_copies(chunk, color):
        slot = (chunk * COLORS + color) % RING
        at = rows_at(color, chunk)
        return [pltpu.make_async_copy(ref.at[at], keep.at[slot, index], state_sem.at[slot])
                for index, ref in enumerate((master_ref, moment_ref, second_ref))]

    lax.fori_loop(0, CHUNKS - 2, third_stage, 0)
    for chunk in range(RING):
        wait_bytes(keep.at[chunk], send3_sem.at[chunk])
    for item in range(RING):
        for copy in state_copies(item // COLORS, item % COLORS):
            copy.start()
    third_stage(CHUNKS - 2, 0)

    vec_own.wait()
    wait_bytes(vec_land.at[pl.ds(0, GROUP - 1)], small_sem.at[1])
    vec_sum = jnp.sum(vec_land[...].astype(jnp.float32), axis=0)
    vec_square = sum(vec_sum[:, part * LANES:(part + 1) * LANES] ** 2 for part in range(vec_share // LANES))

    def wait_packed(chunk, carry):
        wait_bytes(weights_ref.at[pl.ds(0, COLORS), pl.ds(0, ITEMS * rows)], send1_sem.at[chunk])
        return carry

    lax.fori_loop(0, CHUNKS, wait_packed, 0)
    third_stage(CHUNKS - 1, 0)
    square_land[me] = jnp.sum(square_acc[...], axis=0, keepdims=True) + vec_square

    for other in others:
        pltpu.make_async_remote_copy(
            square_land.at[me], square_land.at[me], small_sem.at[3], small_sem.at[4],
            device_id=(other,), device_id_type=MESH).start()
    wait_bytes(new_moment_ref, send2_sem.at[0])
    wait_bytes(new_second_ref, send2_sem.at[1])
    wait_bytes(square_land.at[pl.ds(0, GROUP - 1)], small_sem.at[4])
    norm = jnp.sqrt(jnp.sum(jnp.sum(square_land[...], axis=0), axis=1, keepdims=True))
    clip_coef = jnp.minimum(1.0, 1.0 / (norm + NORM_EPS))

    def link_copy(stage, owner, color, chunk, hop, part=None):
        piece = weights_ref.at[owner, rows_at(color, chunk) if part is None else part]
        return pltpu.make_async_remote_copy(
            piece, piece, send_sem.at[color], recv_sem.at[stage, color, chunk],
            device_id=(me + flips[color][hop],), device_id_type=MESH)

    def core_copy(owner, color, chunk):
        piece = weights_ref.at[owner, rows_at(color, chunk)]
        return pltpu.make_async_remote_copy(
            piece, piece, core_send_sem.at[color], core_recv_sem.at[color],
            device_id=(partner,), device_id_type=MESH)

    def update_chunk(chunk, first):
        for color in range(COLORS):
            item = chunk * COLORS + color
            slot = item % RING
            wait_bytes(keep.at[slot], state_sem.at[slot])
            base = color * color_rows + chunk * rows

            def update(sub, inner):
                to = pl.ds(pl.multiple_of(sub * UPDATE_ROWS, UPDATE_ROWS), UPDATE_ROWS)
                out = pl.ds(pl.multiple_of(base + sub * UPDATE_ROWS, UPDATE_ROWS), UPDATE_ROWS)
                master, moment, second = adam_update(
                    new_master_ref[out, :], clip_coef, keep[slot, 0, to, :],
                    keep[slot, 1, to, :], keep[slot, 2, to, :], DECAY)
                new_master_ref[out, :] = master
                new_moment_ref[out, :] = moment
                new_second_ref[out, :] = second
                weights_ref[me, out, :] = master.astype(jnp.bfloat16)
                if first:
                    for stage, hop in ((0, 0), (1, 1), (3, 2)):
                        link_copy(stage, me, color, chunk, hop, out).start()
                return inner

            lax.fori_loop(0, rows // UPDATE_ROWS, update, 0)
            if not first:
                link_copy(0, me, color, chunk, 0).start()

            @pl.when(item + RING < CHUNKS * COLORS)
            def _():
                for copy in state_copies((item + RING) // COLORS, (item + RING) % COLORS):
                    copy.start()

    def update_later(chunk, carry):
        update_chunk(chunk, False)
        return carry

    update_chunk(0, True)
    lax.fori_loop(1, CHUNKS, update_later, 0)

    vec_new = adam_update(vec_sum, clip_coef, vec_master_ref[...], vec_moment_ref[...], vec_second_ref[...], 0.0)
    vec_new_master_ref[...], vec_new_moment_ref[...], vec_new_second_ref[...] = vec_new
    vec_weights_ref[me] = vec_new[0].reshape(vec_share // LANES, LANES)

    def own_sends(chunk, carry):
        for color in range(COLORS):
            @pl.when(chunk > 0)
            def _():
                link_copy(1, me, color, chunk, 1).start()

            core_copy(me, color, chunk).start()
        return carry

    lax.fori_loop(0, CHUNKS, own_sends, 0)

    def own_sends_last(chunk, carry):
        for color in range(COLORS):
            link_copy(3, me, color, chunk, 2).start()
        return carry

    lax.fori_loop(1, CHUNKS, own_sends_last, 0)

    for other in others:
        pltpu.make_async_remote_copy(
            vec_weights_ref.at[me], vec_weights_ref.at[me], small_sem.at[5], small_sem.at[6],
            device_id=(other,), device_id_type=MESH).start()

    def arrivals(stage, hops, onward):
        def one_chunk(chunk, carry):
            for color in range(COLORS):
                owner = me + sum(flips[color][hop] for hop in hops)
                wait_bytes(weights_ref.at[owner, rows_at(color, chunk)], recv_sem.at[stage, color, chunk])
                for next_stage, hop in onward:
                    link_copy(next_stage, owner, color, chunk, hop).start()
                core_copy(owner, color, chunk).start()
            return carry

        lax.fori_loop(0, CHUNKS, one_chunk, 0)

    arrivals(0, (0,), ((2, 1), (4, 2)))
    arrivals(1, (1,), ((5, 2),))
    arrivals(3, (2,), ())
    arrivals(2, (0, 1), ((6, 2),))
    arrivals(4, (0, 2), ())
    arrivals(5, (1, 2), ())
    arrivals(6, (0, 1, 2), ())

    for color in range(COLORS):
        eight = weights_ref.at[pl.ds(0, 8), pl.ds(color * color_rows, color_rows)]
        wait_bytes(weights_ref.at[pl.ds(0, 7), pl.ds(color * color_rows, color_rows)], send_sem.at[color])
        wait_bytes(eight, core_send_sem.at[color])
        wait_bytes(eight, core_recv_sem.at[color])
    for index in (5, 6):
        wait_bytes(vec_weights_ref.at[pl.ds(0, GROUP - 1)], small_sem.at[index])
    for chunk in range(RING, CHUNKS):
        wait_bytes(keep.at[chunk], send3_sem.at[chunk])
    wait_bytes(vec_land.at[pl.ds(0, GROUP - 1)], small_sem.at[0])
    wait_bytes(square_land.at[pl.ds(0, GROUP - 1)], small_sem.at[3])


def step_call(grad_mat, grad_vec, states, vec_states):
    share = grad_mat.shape[1] // GROUP
    vec_share = grad_vec.shape[1] // GROUP
    rows = share // COLORS // CHUNKS // LANES
    hbm_spec = pl.BlockSpec(memory_space=pltpu.HBM)
    vmem_spec = pl.BlockSpec(memory_space=pltpu.VMEM)
    f32, bf16 = jnp.float32, jnp.bfloat16
    dma = pltpu.SemaphoreType.DMA
    return pl.pallas_call(
        functools.partial(step_kernel, rows, share, vec_share),
        name='adam_step',
        out_shape=(pltpu.VMEM((share // LANES, LANES), f32),) * 3 + (pltpu.VMEM((1, vec_share), f32),) * 3 + (
            pltpu.VMEM((GROUP, share // LANES, LANES), bf16),
            pltpu.VMEM((GROUP, vec_share // LANES, LANES), f32),
            jax.ShapeDtypeStruct((COLORS, CHUNKS, 4, 3 * rows, LANES), bf16),
            jax.ShapeDtypeStruct((CHUNKS, COLORS, 2, rows, LANES), f32)),
        in_specs=[hbm_spec] * 5 + [vmem_spec] * 3,
        out_specs=(vmem_spec,) * 8 + (hbm_spec,) * 2,
        scratch_shapes=[
            pltpu.VMEM((SLOTS, COLORS, 1, rows * LANES), bf16),
            pltpu.VMEM((CHUNKS, COLORS, rows, LANES), f32),
            pltpu.VMEM((2, 2, rows, LANES), f32),
            pltpu.VMEM((CHUNKS, COLORS, rows, LANES), f32),
            pltpu.VMEM((GROUP, 1, vec_share), bf16),
            pltpu.VMEM((GROUP, 1, LANES), f32),
            pltpu.VMEM((8, LANES), f32),
            dma((SLOTS,)), dma((SLOTS,)), dma((2,)), dma((RING,)),
            dma((CHUNKS,)), dma((2,)), dma((CHUNKS,)),
            dma((COLORS, CHUNKS)), dma((COLORS, CHUNKS)), dma((COLORS, CHUNKS)), dma((7,)),
            dma((COLORS,)), dma((7, COLORS, CHUNKS)), dma((COLORS,)), dma((COLORS,)),
        ],
        compiler_params=pltpu.CompilerParams(
            collective_id=0, has_side_effects=True, vmem_limit_bytes=SCRATCH_BYTES),
    )(grad_mat, grad_vec, *states, *vec_states)[:8]


def store_kernel(*refs):
    ins, outs, (vec_weights, sems) = refs[:8], refs[8:16], refs[16:]
    land, vec_land = ins[6:]
    places = [(ins[index], outs[index]) for index in range(3, 6)]
    for index in range(3):
        part = ins[index].shape[0] // STATE_PARTS
        places += [(ins[index].at[pl.ds(at * part, part)], outs[index].at[pl.ds(at * part, part)]) for at in range(STATE_PARTS)]
    for owner in range(GROUP):
        places.append((land.at[owner], outs[6].at[owner]))
    copies = [pltpu.make_async_copy(source, target, sems.at[index]) for index, (source, target) in enumerate(places)]
    for copy in copies:
        copy.start()
    vec_rows = vec_land.shape[1]
    for owner in range(GROUP):
        vec_weights[owner * vec_rows:(owner + 1) * vec_rows, :] = vec_land[owner]
    outs[7][...] = vec_weights[...].astype(jnp.bfloat16)
    for copy in copies:
        copy.wait()


def store_call(results):
    vmem_spec = pl.BlockSpec(memory_space=pltpu.VMEM)
    hbm_spec = pl.BlockSpec(memory_space=pltpu.HBM)
    dma = pltpu.SemaphoreType.DMA
    vec_rows = results[7].size // LANES
    return pl.pallas_call(
        store_kernel,
        name='store_results',
        out_shape=tuple(jax.ShapeDtypeStruct(result.shape, result.dtype) for result in results[:7]) + (
            jax.ShapeDtypeStruct((vec_rows, LANES), jnp.bfloat16),),
        in_specs=[vmem_spec] * 8,
        out_specs=(hbm_spec,) * 7 + (vmem_spec,),
        scratch_shapes=[pltpu.VMEM((vec_rows, LANES), jnp.float32), dma((3 + 3 * STATE_PARTS + GROUP,))],
        compiler_params=pltpu.CompilerParams(vmem_limit_bytes=SCRATCH_BYTES),
    )(*[pltpu.with_memory_space_constraint(result, pltpu.VMEM) for result in results])


def solution(mesh):
    def local_step(grad_mat, grad_vec, master_mat, moment_mat, second_mat, master_vec, moment_vec, second_vec):
        states = [state.reshape(-1, LANES) for state in (master_mat, moment_mat, second_mat)]
        vec_states = [state.reshape(1, -1) for state in (master_vec, moment_vec, second_vec)]
        results = store_call(step_call(grad_mat, grad_vec, states, vec_states))
        return tuple(result.reshape(-1) for result in results)

    row_spec = P(AXIS, None)
    flat_spec = P(AXIS)
    whole_spec = P()
    return jax.shard_map(local_step, mesh=mesh,
                         in_specs=(row_spec, row_spec) + (flat_spec,) * 6,
                         out_specs=(flat_spec,) * 6 + (whole_spec, whole_spec),
                         check_vma=False)
```

```python
import functools

import jax
import jax.numpy as jnp
from jax import lax
from jax.experimental import pallas as pl
from jax.experimental.pallas import tpu as pltpu
from jax.sharding import PartitionSpec as P

STEP = 4
LEARN_RATE = 1e-3
BETA_ONE = 0.9
BETA_TWO = 0.999
ADAM_EPS = 1e-8
DECAY = 0.01
NORM_EPS = 1e-6
FIX_ONE = 1.0 - BETA_ONE ** STEP
FIX_TWO = 1.0 - BETA_TWO ** STEP

AXIS = 'fsdp'
MESH = pl.DeviceIdType.MESH
GROUP = 16
LANES = 128
ORDERS = ((2, 4, 8), (4, 8, 2), (8, 2, 4))
COLORS = len(ORDERS)
CHUNKS = 10
AHEAD = 2
SLOTS = 3
SUB_ROWS = 80
UPDATE_ROWS = 80
RING = 4
STATE_PARTS = 2
ITEMS = 12
SCRATCH_BYTES = 12_800_000


def adam_update(grad_sum, clip_coef, master, moment, second, decay):
    clip_grad = clip_coef * grad_sum
    new_moment = BETA_ONE * moment + (1.0 - BETA_ONE) * clip_grad
    new_second = BETA_TWO * second + (1.0 - BETA_TWO) * clip_grad * clip_grad
    step_dir = (new_moment / FIX_ONE) / (jnp.sqrt(new_second / FIX_TWO) + ADAM_EPS)
    new_master = master - LEARN_RATE * (step_dir + decay * master)
    return new_master, new_moment, new_second


def flip_of(me, bit):
    return bit * (1 - 2 * ((me // bit) % 2))


def step_kernel(rows, share, vec_share, grad_ref, vec_ref, master_ref, moment_ref, second_ref,
                vec_master_ref, vec_moment_ref, vec_second_ref,
                new_master_ref, new_moment_ref, new_second_ref,
                vec_new_master_ref, vec_new_moment_ref, vec_new_second_ref, weights_ref, vec_weights_ref,
                land_ref, recv2,
                pad_in, keep, recv2_in, recv3, vec_land, square_land, square_acc,
                pad_sem, part_sem, recv2_in_sem, state_sem,
                send1_sem, send2_sem, send3_sem, recv1_sem, recv2_sem, recv3_sem, small_sem,
                send_sem, recv_sem, core_send_sem, core_recv_sem):
    me = lax.axis_index(AXIS)
    core = me % 2
    partner = me + flip_of(me, 1)
    block = rows * LANES
    color_len = share // COLORS
    color_rows = color_len // LANES
    flips = [[flip_of(me, bit) for bit in order] for order in ORDERS]
    per_owner = share // LANES // rows
    neighbours = [partner] + [me + flip_of(me, bit) + other for bit in ORDERS[0] for other in (0, flip_of(me, 1))]
    others = [me + sum(flip_of(me, bit) for bit in (1, 2, 4, 8) if mask & bit)
              for mask in sorted(range(1, GROUP), key=lambda mask: (-(mask >> 1).bit_count(), mask))]

    def wait_bytes(ref, sem):
        pltpu.make_async_copy(ref, ref, sem).wait()

    def rows_at(color, chunk):
        return pl.ds(pl.multiple_of(color * color_rows + chunk * rows, rows), rows)

    def piece_at(owner, color, chunk):
        start = pl.multiple_of(owner * share + color * color_len + chunk * block, block)
        return grad_ref.at[:, pl.ds(start, block)]

    def packed_at(index):
        return index // per_owner, pl.multiple_of((index % per_owner) * rows, rows)

    def packed_index(color, chunk, item):
        return (chunk * COLORS + color) * ITEMS + item

    part_owner = COLORS * CHUNKS * ITEMS // per_owner
    part_rows = 3 * rows

    def route(item, color):
        place, kind = item // 3, (item + 1) % 3
        flip1, flip2, flip3 = flips[color]
        local = (2 - kind) // 2
        target_core = local * (1 - core) + (1 - local) * (kind - 1)
        target = me - core + (1 - local) * flip1 + target_core
        owner = target + (1 - place // 2) * flip2 + (1 - place % 2) * flip3
        source = (1 - local) * (1 + core)
        return owner, target, source, place

    def in_copy(chunk, item, color):
        owner = route(item, color)[0]
        return pltpu.make_async_copy(piece_at(owner, color, chunk), pad_in.at[item % SLOTS, color], pad_sem.at[item % SLOTS])

    def start_in(chunk, item):
        for color in range(COLORS):
            in_copy(chunk, item, color).start()

    def pack_item(chunk, item):
        wait_bytes(pad_in.at[item % SLOTS], pad_sem.at[item % SLOTS])
        for color in range(COLORS):
            place_owner, place_row = packed_at(packed_index(color, chunk, item))

            def pack(sub, inner):
                off = pl.multiple_of(sub * SUB_ROWS * LANES, SUB_ROWS * LANES)
                vals = pad_in[item % SLOTS, color, :, pl.ds(off, SUB_ROWS * LANES)].astype(jnp.float32)
                to = pl.multiple_of(place_row + sub * SUB_ROWS, SUB_ROWS)
                weights_ref[place_owner, pl.ds(to, SUB_ROWS), :] = (
                    vals.reshape(SUB_ROWS, LANES).astype(jnp.bfloat16))
                return inner

            lax.fori_loop(0, rows // SUB_ROWS, pack, 0, unroll=True)

    def send_item(chunk, item):
        for color in range(COLORS):
            owner, target, source, place = route(item, color)
            place_owner, place_row = packed_at(packed_index(color, chunk, item))
            pltpu.make_async_remote_copy(
                weights_ref.at[place_owner, pl.ds(place_row, rows)],
                land_ref.at[color, chunk, place, pl.ds(pl.multiple_of(source * rows, rows), rows)],
                send1_sem.at[chunk], recv1_sem.at[color, chunk, place], device_id=(target,), device_id_type=MESH).start()

    def pack_and_send(chunk, first):
        def one_item(item, carry):
            @pl.when(item + SLOTS - 1 < ITEMS)
            def _():
                start_in(chunk, item + SLOTS - 1)

            pack_item(chunk, item)
            send_item(chunk, item)
            return carry

        lax.fori_loop(first, ITEMS, one_item, 0)

    def first_sums(chunk, place, pack_chunk):
        if pack_chunk is not None:
            for item in range(SLOTS):
                start_in(pack_chunk, place * SLOTS + item)
        owners = [me + (1 - place // 2) * flip2 + (1 - place % 2) * flip3 for _, flip2, flip3 in flips]
        for color in range(COLORS):
            pltpu.make_async_copy(piece_at(owners[color], color, chunk), pad_in.at[SLOTS, color], pad_sem.at[SLOTS]).start()
        slot = place % 2
        for color in range(COLORS):
            wait_bytes(land_ref.at[color, chunk, place], recv1_sem.at[color, chunk, place])
            pltpu.make_async_copy(land_ref.at[color, chunk, place],
                                  weights_ref.at[part_owner + slot, pl.ds(color * part_rows, part_rows)],
                                  part_sem.at[slot]).start()
        if pack_chunk is not None:
            def one_item(item, carry):
                pack_item(pack_chunk, item)
                send_item(pack_chunk, item)
                return carry

            lax.fori_loop(place * SLOTS, (place + 1) * SLOTS, one_item, 0)
        wait_bytes(pad_in.at[SLOTS], pad_sem.at[SLOTS])
        wait_bytes(weights_ref.at[part_owner + slot, pl.ds(0, COLORS * part_rows)], part_sem.at[slot])
        for color in range(COLORS):
            at = rows_at(color, chunk)
            total = (new_moment_ref.at[at], new_second_ref.at[at], keep.at[chunk, color], new_master_ref.at[at])[place]

            def add(sub, inner):
                off = pl.multiple_of(sub * SUB_ROWS * LANES, SUB_ROWS * LANES)
                to = pl.ds(pl.multiple_of(sub * SUB_ROWS, SUB_ROWS), SUB_ROWS)
                vals = pad_in[SLOTS, color, :, pl.ds(off, SUB_ROWS * LANES)].astype(jnp.float32)
                vals = vals.reshape(SUB_ROWS, LANES)
                for source in range(3):
                    row = pl.multiple_of(color * part_rows + source * rows + sub * SUB_ROWS, SUB_ROWS)
                    vals = vals + weights_ref[part_owner + slot, pl.ds(row, SUB_ROWS), :].astype(jnp.float32)
                total[to, :] = vals
                return inner

            lax.fori_loop(0, rows // SUB_ROWS, add, 0, unroll=True)
            if place < 2:
                pltpu.make_async_remote_copy(
                    total, recv2.at[chunk, color, place], send2_sem.at[place], recv2_sem.at[color, chunk],
                    device_id=(me + flips[color][1],), device_id_type=MESH).start()

    for item in range(SLOTS):
        start_in(0, item)
    barrier = pltpu.get_barrier_semaphore()
    for neighbour in neighbours:
        pl.semaphore_signal(barrier, inc=1, device_id=(neighbour,), device_id_type=MESH)
    pack_item(0, 0)
    pl.semaphore_wait(barrier, len(neighbours))
    send_item(0, 0)
    pack_and_send(0, 1)

    def pack_ahead(chunk, carry):
        for item in range(SLOTS - 1):
            start_in(chunk, item)
        pack_and_send(chunk, 0)
        return carry

    lax.fori_loop(1, AHEAD, pack_ahead, 0)

    def first_stage(chunk, carry):
        for place in range(4):
            first_sums(chunk, place, chunk + AHEAD)
        return carry

    def first_stage_last(chunk, carry):
        for place in range(4):
            first_sums(chunk, place, None)
        return carry

    lax.fori_loop(0, CHUNKS - AHEAD, first_stage, 0)
    lax.fori_loop(CHUNKS - AHEAD, CHUNKS, first_stage_last, 0)

    def second_stage(chunk, carry):
        for color in range(COLORS):
            wait_bytes(recv2.at[chunk, color], recv2_sem.at[color, chunk])
            copy = pltpu.make_async_copy(recv2.at[chunk, color], recv2_in, recv2_in_sem)
            copy.start()
            copy.wait()
            base = color * color_rows + chunk * rows

            def add(sub, inner):
                to = pl.ds(pl.multiple_of(sub * SUB_ROWS, SUB_ROWS), SUB_ROWS)
                out = pl.ds(pl.multiple_of(base + sub * SUB_ROWS, SUB_ROWS), SUB_ROWS)
                keep[chunk, color, to, :] += recv2_in[0, to, :]
                new_master_ref[out, :] += recv2_in[1, to, :]
                return inner

            lax.fori_loop(0, rows // SUB_ROWS, add, 0, unroll=True)
            pltpu.make_async_remote_copy(
                keep.at[chunk, color], recv3.at[chunk, color], send3_sem.at[chunk], recv3_sem.at[color, chunk],
                device_id=(me + flips[color][2],), device_id_type=MESH).start()
        return carry

    second_stage(0, 0)
    for other in others:
        pltpu.make_async_remote_copy(
            vec_ref.at[:, pl.ds(pl.multiple_of(other * vec_share, vec_share), vec_share)], vec_land.at[me],
            small_sem.at[0], small_sem.at[1], device_id=(other,), device_id_type=MESH).start()
    vec_own = pltpu.make_async_copy(
        vec_ref.at[:, pl.ds(pl.multiple_of(me * vec_share, vec_share), vec_share)], vec_land.at[me], small_sem.at[2])
    vec_own.start()
    lax.fori_loop(1, CHUNKS, second_stage, 0)

    square_acc[...] = jnp.zeros_like(square_acc)

    def third_stage(chunk, carry):
        for color in range(COLORS):
            wait_bytes(recv3.at[chunk, color], recv3_sem.at[color, chunk])
            base = color * color_rows + chunk * rows

            def add(sub, squares):
                to = pl.ds(pl.multiple_of(sub * SUB_ROWS, SUB_ROWS), SUB_ROWS)
                out = pl.ds(pl.multiple_of(base + sub * SUB_ROWS, SUB_ROWS), SUB_ROWS)
                vals = new_master_ref[out, :] + recv3[chunk, color, to, :]
                new_master_ref[out, :] = vals
                return squares + jnp.sum((vals * vals).reshape(SUB_ROWS // 8, 8, LANES), axis=0)

            squares = lax.fori_loop(0, rows // SUB_ROWS, add, jnp.zeros((8, LANES), jnp.float32), unroll=True)
            square_acc[...] += squares
        return carry

    def state_copies(chunk, color):
        slot = (chunk * COLORS + color) % RING
        at = rows_at(color, chunk)
        return [pltpu.make_async_copy(ref.at[at], keep.at[slot, index], state_sem.at[slot])
                for index, ref in enumerate((master_ref, moment_ref, second_ref))]

    lax.fori_loop(0, CHUNKS - 2, third_stage, 0)
    for chunk in range(RING):
        wait_bytes(keep.at[chunk], send3_sem.at[chunk])
    for item in range(RING):
        for copy in state_copies(item // COLORS, item % COLORS):
            copy.start()
    third_stage(CHUNKS - 2, 0)

    vec_own.wait()
    wait_bytes(vec_land.at[pl.ds(0, GROUP - 1)], small_sem.at[1])
    vec_sum = jnp.sum(vec_land[...].astype(jnp.float32), axis=0)
    vec_square = sum(vec_sum[:, part * LANES:(part + 1) * LANES] ** 2 for part in range(vec_share // LANES))

    def wait_packed(chunk, carry):
        wait_bytes(weights_ref.at[pl.ds(0, COLORS), pl.ds(0, ITEMS * rows)], send1_sem.at[chunk])
        return carry

    lax.fori_loop(0, CHUNKS, wait_packed, 0)
    third_stage(CHUNKS - 1, 0)
    square_land[me] = jnp.sum(square_acc[...], axis=0, keepdims=True) + vec_square

    for other in others:
        pltpu.make_async_remote_copy(
            square_land.at[me], square_land.at[me], small_sem.at[3], small_sem.at[4],
            device_id=(other,), device_id_type=MESH).start()
    wait_bytes(new_moment_ref, send2_sem.at[0])
    wait_bytes(new_second_ref, send2_sem.at[1])
    wait_bytes(square_land.at[pl.ds(0, GROUP - 1)], small_sem.at[4])
    norm = jnp.sqrt(jnp.sum(jnp.sum(square_land[...], axis=0), axis=1, keepdims=True))
    clip_coef = jnp.minimum(1.0, 1.0 / (norm + NORM_EPS))

    def link_copy(stage, owner, color, chunk, hop, part=None):
        piece = weights_ref.at[owner, rows_at(color, chunk) if part is None else part]
        return pltpu.make_async_remote_copy(
            piece, piece, send_sem.at[color], recv_sem.at[stage, color, chunk],
            device_id=(me + flips[color][hop],), device_id_type=MESH)

    def core_copy(owner, color, chunk):
        piece = weights_ref.at[owner, rows_at(color, chunk)]
        return pltpu.make_async_remote_copy(
            piece, piece, core_send_sem.at[color], core_recv_sem.at[color],
            device_id=(partner,), device_id_type=MESH)

    def update_chunk(chunk, first):
        for color in range(COLORS):
            item = chunk * COLORS + color
            slot = item % RING
            wait_bytes(keep.at[slot], state_sem.at[slot])
            base = color * color_rows + chunk * rows

            def update(sub, inner):
                to = pl.ds(pl.multiple_of(sub * UPDATE_ROWS, UPDATE_ROWS), UPDATE_ROWS)
                out = pl.ds(pl.multiple_of(base + sub * UPDATE_ROWS, UPDATE_ROWS), UPDATE_ROWS)
                master, moment, second = adam_update(
                    new_master_ref[out, :], clip_coef, keep[slot, 0, to, :],
                    keep[slot, 1, to, :], keep[slot, 2, to, :], DECAY)
                new_master_ref[out, :] = master
                new_moment_ref[out, :] = moment
                new_second_ref[out, :] = second
                weights_ref[me, out, :] = master.astype(jnp.bfloat16)
                if first:
                    for stage, hop in ((0, 0), (1, 1), (3, 2)):
                        link_copy(stage, me, color, chunk, hop, out).start()
                return inner

            lax.fori_loop(0, rows // UPDATE_ROWS, update, 0)
            if not first:
                link_copy(0, me, color, chunk, 0).start()

            @pl.when(item + RING < CHUNKS * COLORS)
            def _():
                for copy in state_copies((item + RING) // COLORS, (item + RING) % COLORS):
                    copy.start()

    def update_later(chunk, carry):
        update_chunk(chunk, False)
        return carry

    update_chunk(0, True)
    lax.fori_loop(1, CHUNKS, update_later, 0)

    vec_new = adam_update(vec_sum, clip_coef, vec_master_ref[...], vec_moment_ref[...], vec_second_ref[...], 0.0)
    vec_new_master_ref[...], vec_new_moment_ref[...], vec_new_second_ref[...] = vec_new
    vec_weights_ref[me] = vec_new[0].reshape(vec_share // LANES, LANES)

    def own_sends(chunk, carry):
        for color in range(COLORS):
            @pl.when(chunk > 0)
            def _():
                link_copy(1, me, color, chunk, 1).start()

            core_copy(me, color, chunk).start()
        return carry

    lax.fori_loop(0, CHUNKS, own_sends, 0)

    def own_sends_last(chunk, carry):
        for color in range(COLORS):
            link_copy(3, me, color, chunk, 2).start()
        return carry

    lax.fori_loop(1, CHUNKS, own_sends_last, 0)

    for other in others:
        pltpu.make_async_remote_copy(
            vec_weights_ref.at[me], vec_weights_ref.at[me], small_sem.at[5], small_sem.at[6],
            device_id=(other,), device_id_type=MESH).start()

    def arrivals(stage, hops, onward):
        def one_chunk(chunk, carry):
            for color in range(COLORS):
                owner = me + sum(flips[color][hop] for hop in hops)
                wait_bytes(weights_ref.at[owner, rows_at(color, chunk)], recv_sem.at[stage, color, chunk])
                for next_stage, hop in onward:
                    link_copy(next_stage, owner, color, chunk, hop).start()
                core_copy(owner, color, chunk).start()
            return carry

        lax.fori_loop(0, CHUNKS, one_chunk, 0)

    arrivals(0, (0,), ((2, 1), (4, 2)))
    arrivals(1, (1,), ((5, 2),))
    arrivals(3, (2,), ())
    arrivals(2, (0, 1), ((6, 2),))
    arrivals(4, (0, 2), ())
    arrivals(5, (1, 2), ())
    arrivals(6, (0, 1, 2), ())

    for color in range(COLORS):
        eight = weights_ref.at[pl.ds(0, 8), pl.ds(color * color_rows, color_rows)]
        wait_bytes(weights_ref.at[pl.ds(0, 7), pl.ds(color * color_rows, color_rows)], send_sem.at[color])
        wait_bytes(eight, core_send_sem.at[color])
        wait_bytes(eight, core_recv_sem.at[color])
    for index in (5, 6):
        wait_bytes(vec_weights_ref.at[pl.ds(0, GROUP - 1)], small_sem.at[index])
    for chunk in range(RING, CHUNKS):
        wait_bytes(keep.at[chunk], send3_sem.at[chunk])
    wait_bytes(vec_land.at[pl.ds(0, GROUP - 1)], small_sem.at[0])
    wait_bytes(square_land.at[pl.ds(0, GROUP - 1)], small_sem.at[3])


def step_call(grad_mat, grad_vec, states, vec_states):
    share = grad_mat.shape[1] // GROUP
    vec_share = grad_vec.shape[1] // GROUP
    rows = share // COLORS // CHUNKS // LANES
    hbm_spec = pl.BlockSpec(memory_space=pltpu.HBM)
    vmem_spec = pl.BlockSpec(memory_space=pltpu.VMEM)
    f32, bf16 = jnp.float32, jnp.bfloat16
    dma = pltpu.SemaphoreType.DMA
    return pl.pallas_call(
        functools.partial(step_kernel, rows, share, vec_share),
        name='adam_step',
        out_shape=(pltpu.VMEM((share // LANES, LANES), f32),) * 3 + (pltpu.VMEM((1, vec_share), f32),) * 3 + (
            pltpu.VMEM((GROUP, share // LANES, LANES), bf16),
            pltpu.VMEM((GROUP, vec_share // LANES, LANES), f32),
            jax.ShapeDtypeStruct((COLORS, CHUNKS, 4, 3 * rows, LANES), bf16),
            jax.ShapeDtypeStruct((CHUNKS, COLORS, 2, rows, LANES), f32)),
        in_specs=[hbm_spec] * 5 + [vmem_spec] * 3,
        out_specs=(vmem_spec,) * 8 + (hbm_spec,) * 2,
        scratch_shapes=[
            pltpu.VMEM((SLOTS + 1, COLORS, 1, rows * LANES), bf16),
            pltpu.VMEM((CHUNKS, COLORS, rows, LANES), f32),
            pltpu.VMEM((2, rows, LANES), f32),
            pltpu.VMEM((CHUNKS, COLORS, rows, LANES), f32),
            pltpu.VMEM((GROUP, 1, vec_share), bf16),
            pltpu.VMEM((GROUP, 1, LANES), f32),
            pltpu.VMEM((8, LANES), f32),
            dma((SLOTS + 1,)), dma((2,)), dma, dma((RING,)),
            dma((CHUNKS,)), dma((2,)), dma((CHUNKS,)),
            dma((COLORS, CHUNKS, 4)), dma((COLORS, CHUNKS)), dma((COLORS, CHUNKS)), dma((7,)),
            dma((COLORS,)), dma((7, COLORS, CHUNKS)), dma((COLORS,)), dma((COLORS,)),
        ],
        compiler_params=pltpu.CompilerParams(
            collective_id=0, has_side_effects=True, vmem_limit_bytes=SCRATCH_BYTES),
    )(grad_mat, grad_vec, *states, *vec_states)[:8]


def store_kernel(*refs):
    ins, outs, (vec_weights, sems) = refs[:8], refs[8:16], refs[16:]
    land, vec_land = ins[6:]
    places = [(ins[index], outs[index]) for index in range(3, 6)]
    for index in range(3):
        part = ins[index].shape[0] // STATE_PARTS
        places += [(ins[index].at[pl.ds(at * part, part)], outs[index].at[pl.ds(at * part, part)]) for at in range(STATE_PARTS)]
    for owner in range(GROUP):
        places.append((land.at[owner], outs[6].at[owner]))
    copies = [pltpu.make_async_copy(source, target, sems.at[index]) for index, (source, target) in enumerate(places)]
    for copy in copies:
        copy.start()
    vec_rows = vec_land.shape[1]
    for owner in range(GROUP):
        vec_weights[owner * vec_rows:(owner + 1) * vec_rows, :] = vec_land[owner]
    outs[7][...] = vec_weights[...].astype(jnp.bfloat16)
    for copy in copies:
        copy.wait()


def store_call(results):
    vmem_spec = pl.BlockSpec(memory_space=pltpu.VMEM)
    hbm_spec = pl.BlockSpec(memory_space=pltpu.HBM)
    dma = pltpu.SemaphoreType.DMA
    vec_rows = results[7].size // LANES
    return pl.pallas_call(
        store_kernel,
        name='store_results',
        out_shape=tuple(jax.ShapeDtypeStruct(result.shape, result.dtype) for result in results[:7]) + (
            jax.ShapeDtypeStruct((vec_rows, LANES), jnp.bfloat16),),
        in_specs=[vmem_spec] * 8,
        out_specs=(hbm_spec,) * 7 + (vmem_spec,),
        scratch_shapes=[pltpu.VMEM((vec_rows, LANES), jnp.float32), dma((3 + 3 * STATE_PARTS + GROUP,))],
        compiler_params=pltpu.CompilerParams(vmem_limit_bytes=SCRATCH_BYTES),
    )(*[pltpu.with_memory_space_constraint(result, pltpu.VMEM) for result in results])


def solution(mesh):
    def local_step(grad_mat, grad_vec, master_mat, moment_mat, second_mat, master_vec, moment_vec, second_vec):
        states = [state.reshape(-1, LANES) for state in (master_mat, moment_mat, second_mat)]
        vec_states = [state.reshape(1, -1) for state in (master_vec, moment_vec, second_vec)]
        results = store_call(step_call(grad_mat, grad_vec, states, vec_states))
        return tuple(result.reshape(-1) for result in results)

    row_spec = P(AXIS, None)
    flat_spec = P(AXIS)
    whole_spec = P()
    return jax.shard_map(local_step, mesh=mesh,
                         in_specs=(row_spec, row_spec) + (flat_spec,) * 6,
                         out_specs=(flat_spec,) * 6 + (whole_spec, whole_spec),
                         check_vma=False)
```

```python
import functools

import jax
import jax.numpy as jnp
from jax import lax
from jax.experimental import pallas as pl
from jax.experimental.pallas import tpu as pltpu
from jax.sharding import PartitionSpec as P

STEP = 4
LEARN_RATE = 1e-3
BETA_ONE = 0.9
BETA_TWO = 0.999
ADAM_EPS = 1e-8
DECAY = 0.01
NORM_EPS = 1e-6
FIX_ONE = 1.0 - BETA_ONE ** STEP
FIX_TWO = 1.0 - BETA_TWO ** STEP

AXIS = 'fsdp'
MESH = pl.DeviceIdType.MESH
GROUP = 16
LANES = 128
ORDERS = ((2, 4, 8), (4, 8, 2), (8, 2, 4))
COLORS = len(ORDERS)
CHUNKS = 8
AHEAD = 3
SLOTS = 3
PIECES = 4
SUB_ROWS = 80
UPDATE_ROWS = 80
RING = 4
STATE_PARTS = 2
ITEMS = 12
SCRATCH_BYTES = 12_800_000


def adam_update(grad_sum, clip_coef, master, moment, second, decay):
    clip_grad = clip_coef * grad_sum
    new_moment = BETA_ONE * moment + (1.0 - BETA_ONE) * clip_grad
    new_second = BETA_TWO * second + (1.0 - BETA_TWO) * clip_grad * clip_grad
    step_dir = (new_moment / FIX_ONE) / (jnp.sqrt(new_second / FIX_TWO) + ADAM_EPS)
    new_master = master - LEARN_RATE * (step_dir + decay * master)
    return new_master, new_moment, new_second


def flip_of(me, bit):
    return bit * (1 - 2 * ((me // bit) % 2))


def step_kernel(rows, share, vec_share, grad_ref, vec_ref, master_ref, moment_ref, second_ref,
                vec_master_ref, vec_moment_ref, vec_second_ref,
                new_master_ref, new_moment_ref, new_second_ref,
                vec_new_master_ref, vec_new_moment_ref, vec_new_second_ref, weights_ref, vec_weights_ref,
                land_ref, recv2,
                pad_in, keep, recv2_in, recv3, vec_land, square_land, square_acc,
                pad_sem, part_sem, recv2_in_sem, state_sem,
                send1_sem, send2_sem, send3_sem, recv1_sem, recv2_sem, recv3_sem, small_sem,
                send_sem, recv_sem, core_send_sem, core_recv_sem):
    me = lax.axis_index(AXIS)
    core = me % 2
    partner = me + flip_of(me, 1)
    block = rows * LANES
    color_len = share // COLORS
    color_rows = color_len // LANES
    flips = [[flip_of(me, bit) for bit in order] for order in ORDERS]
    per_owner = share // LANES // rows
    neighbours = [partner] + [me + flip_of(me, bit) + other for bit in ORDERS[0] for other in (0, flip_of(me, 1))]
    others = [me + sum(flip_of(me, bit) for bit in (1, 2, 4, 8) if mask & bit)
              for mask in sorted(range(1, GROUP), key=lambda mask: (-(mask >> 1).bit_count(), mask))]

    def wait_bytes(ref, sem):
        pltpu.make_async_copy(ref, ref, sem).wait()

    def rows_at(color, chunk):
        return pl.ds(pl.multiple_of(color * color_rows + chunk * rows, rows), rows)

    def piece_at(owner, color, chunk):
        start = pl.multiple_of(owner * share + color * color_len + chunk * block, block)
        return grad_ref.at[:, pl.ds(start, block)]

    def packed_at(index):
        return index // per_owner, pl.multiple_of((index % per_owner) * rows, rows)

    def packed_index(color, chunk, item):
        return (chunk * COLORS + color) * ITEMS + item

    part_owner = COLORS * CHUNKS * ITEMS // per_owner
    part_rows = 3 * rows

    def route(item, color):
        place, kind = item // 3, (item + 1) % 3
        flip1, flip2, flip3 = flips[color]
        local = (2 - kind) // 2
        target_core = local * (1 - core) + (1 - local) * (kind - 1)
        target = me - core + (1 - local) * flip1 + target_core
        owner = target + (1 - place // 2) * flip2 + (1 - place % 2) * flip3
        source = (1 - local) * (1 + core)
        return owner, target, source, place

    def in_copy(chunk, item, color):
        owner = route(item, color)[0]
        return pltpu.make_async_copy(piece_at(owner, color, chunk), pad_in.at[item % SLOTS, color], pad_sem.at[item % SLOTS])

    def start_in(chunk, item):
        for color in range(COLORS):
            in_copy(chunk, item, color).start()

    def pack_item(chunk, item):
        wait_bytes(pad_in.at[item % SLOTS], pad_sem.at[item % SLOTS])
        for color in range(COLORS):
            place_owner, place_row = packed_at(packed_index(color, chunk, item))

            def pack(sub, inner):
                off = pl.multiple_of(sub * SUB_ROWS * LANES, SUB_ROWS * LANES)
                vals = pad_in[item % SLOTS, color, :, pl.ds(off, SUB_ROWS * LANES)].astype(jnp.float32)
                to = pl.multiple_of(place_row + sub * SUB_ROWS, SUB_ROWS)
                weights_ref[place_owner, pl.ds(to, SUB_ROWS), :] = (
                    vals.reshape(SUB_ROWS, LANES).astype(jnp.bfloat16))
                return inner

            lax.fori_loop(0, rows // SUB_ROWS, pack, 0, unroll=True)

    def send_item(chunk, item):
        for color in range(COLORS):
            owner, target, source, place = route(item, color)
            place_owner, place_row = packed_at(packed_index(color, chunk, item))
            pltpu.make_async_remote_copy(
                weights_ref.at[place_owner, pl.ds(place_row, rows)],
                land_ref.at[color, chunk, place, pl.ds(pl.multiple_of(source * rows, rows), rows)],
                send1_sem.at[chunk], recv1_sem.at[color, chunk], device_id=(target,), device_id_type=MESH).start()

    def pack_and_send(chunk, first):
        def one_item(item, carry):
            @pl.when(item + SLOTS - 1 < ITEMS)
            def _():
                start_in(chunk, item + SLOTS - 1)

            pack_item(chunk, item)
            send_item(chunk, item)
            return carry

        lax.fori_loop(first, ITEMS, one_item, 0)

    def start_parts(chunk, place):
        slot = place % SLOTS
        for color in range(COLORS):
            flip1, flip2, flip3 = flips[color]
            owner = me + (1 - place // 2) * flip2 + (1 - place % 2) * flip3
            pltpu.make_async_copy(land_ref.at[color, chunk, place],
                                  weights_ref.at[part_owner + slot, pl.ds(color * part_rows, part_rows)],
                                  part_sem.at[slot]).start()
            pltpu.make_async_copy(piece_at(owner, color, chunk), pad_in.at[slot, color], pad_sem.at[slot]).start()

    def first_sums(chunk):
        for color in range(COLORS):
            wait_bytes(land_ref.at[color, chunk], recv1_sem.at[color, chunk])
        for place in range(SLOTS - 1):
            start_parts(chunk, place)
        for place in range(4):
            slot = place % SLOTS
            if place + SLOTS - 1 < 4:
                start_parts(chunk, place + SLOTS - 1)
            wait_bytes(weights_ref.at[part_owner + slot, pl.ds(0, COLORS * part_rows)], part_sem.at[slot])
            wait_bytes(pad_in.at[slot], pad_sem.at[slot])
            for color in range(COLORS):
                at = rows_at(color, chunk)
                total = (new_moment_ref.at[at], new_second_ref.at[at], keep.at[chunk, color], new_master_ref.at[at])[place]

                def add(sub, inner):
                    off = pl.multiple_of(sub * SUB_ROWS * LANES, SUB_ROWS * LANES)
                    to = pl.ds(pl.multiple_of(sub * SUB_ROWS, SUB_ROWS), SUB_ROWS)
                    vals = pad_in[slot, color, :, pl.ds(off, SUB_ROWS * LANES)].astype(jnp.float32)
                    vals = vals.reshape(SUB_ROWS, LANES)
                    for source in range(3):
                        row = pl.multiple_of(color * part_rows + source * rows + sub * SUB_ROWS, SUB_ROWS)
                        vals = vals + weights_ref[part_owner + slot, pl.ds(row, SUB_ROWS), :].astype(jnp.float32)
                    total[to, :] = vals
                    return inner

                lax.fori_loop(0, rows // SUB_ROWS, add, 0, unroll=True)
                if place < 2:
                    pltpu.make_async_remote_copy(
                        total, recv2.at[chunk, color, place], send2_sem.at[place], recv2_sem.at[color, chunk],
                        device_id=(me + flips[color][1],), device_id_type=MESH).start()

    for item in range(SLOTS):
        start_in(0, item)
    barrier = pltpu.get_barrier_semaphore()
    for neighbour in neighbours:
        pl.semaphore_signal(barrier, inc=1, device_id=(neighbour,), device_id_type=MESH)
    pack_item(0, 0)
    pl.semaphore_wait(barrier, len(neighbours))
    send_item(0, 0)
    pack_and_send(0, 1)

    def pack_ahead(chunk, carry):
        for item in range(SLOTS - 1):
            start_in(chunk, item)
        pack_and_send(chunk, 0)
        return carry

    lax.fori_loop(1, AHEAD, pack_ahead, 0)

    def first_stage(chunk, carry):
        first_sums(chunk)

        @pl.when(chunk + AHEAD < CHUNKS)
        def _():
            for item in range(SLOTS - 1):
                start_in(chunk + AHEAD, item)
            pack_and_send(chunk + AHEAD, 0)

        return carry

    lax.fori_loop(0, CHUNKS, first_stage, 0)

    def second_stage(chunk, carry):
        copies = [pltpu.make_async_copy(recv2.at[chunk, color], recv2_in.at[color % 2], recv2_in_sem.at[color % 2])
                  for color in range(COLORS)]

        def fetch(color):
            wait_bytes(recv2.at[chunk, color], recv2_sem.at[color, chunk])
            copies[color].start()

        fetch(0)
        fetch(1)
        for color in range(COLORS):
            copies[color].wait()
            base = color * color_rows + chunk * rows

            def add(sub, inner):
                to = pl.ds(pl.multiple_of(sub * SUB_ROWS, SUB_ROWS), SUB_ROWS)
                out = pl.ds(pl.multiple_of(base + sub * SUB_ROWS, SUB_ROWS), SUB_ROWS)
                keep[chunk, color, to, :] += recv2_in[color % 2, 0, to, :]
                new_master_ref[out, :] += recv2_in[color % 2, 1, to, :]
                return inner

            lax.fori_loop(0, rows // SUB_ROWS, add, 0)
            pltpu.make_async_remote_copy(
                keep.at[chunk, color], recv3.at[chunk, color], send3_sem.at[chunk], recv3_sem.at[color, chunk],
                device_id=(me + flips[color][2],), device_id_type=MESH).start()
            if color == 0:
                fetch(2)
        return carry

    second_stage(0, 0)
    for other in others:
        pltpu.make_async_remote_copy(
            vec_ref.at[:, pl.ds(pl.multiple_of(other * vec_share, vec_share), vec_share)], vec_land.at[me],
            small_sem.at[0], small_sem.at[1], device_id=(other,), device_id_type=MESH).start()
    vec_own = pltpu.make_async_copy(
        vec_ref.at[:, pl.ds(pl.multiple_of(me * vec_share, vec_share), vec_share)], vec_land.at[me], small_sem.at[2])
    vec_own.start()
    lax.fori_loop(1, CHUNKS, second_stage, 0)

    square_acc[...] = jnp.zeros_like(square_acc)

    def third_stage(chunk, carry):
        for color in range(COLORS):
            wait_bytes(recv3.at[chunk, color], recv3_sem.at[color, chunk])
            base = color * color_rows + chunk * rows

            def add(sub, squares):
                to = pl.ds(pl.multiple_of(sub * SUB_ROWS, SUB_ROWS), SUB_ROWS)
                out = pl.ds(pl.multiple_of(base + sub * SUB_ROWS, SUB_ROWS), SUB_ROWS)
                vals = new_master_ref[out, :] + recv3[chunk, color, to, :]
                new_master_ref[out, :] = vals
                return squares + jnp.sum((vals * vals).reshape(SUB_ROWS // 8, 8, LANES), axis=0)

            squares = lax.fori_loop(0, rows // SUB_ROWS, add, jnp.zeros((8, LANES), jnp.float32), unroll=True)
            square_acc[...] += squares
        return carry

    def state_copies(chunk, color):
        slot = (chunk * COLORS + color) % RING
        at = rows_at(color, chunk)
        return [pltpu.make_async_copy(ref.at[at], keep.at[slot, index], state_sem.at[slot])
                for index, ref in enumerate((master_ref, moment_ref, second_ref))]

    lax.fori_loop(0, CHUNKS - 2, third_stage, 0)
    for chunk in range(RING):
        wait_bytes(keep.at[chunk], send3_sem.at[chunk])
    for item in range(RING):
        for copy in state_copies(item // COLORS, item % COLORS):
            copy.start()
    third_stage(CHUNKS - 2, 0)

    vec_own.wait()
    wait_bytes(vec_land.at[pl.ds(0, GROUP - 1)], small_sem.at[1])
    vec_sum = jnp.sum(vec_land[...].astype(jnp.float32), axis=0)
    vec_square = sum(vec_sum[:, part * LANES:(part + 1) * LANES] ** 2 for part in range(vec_share // LANES))

    def wait_packed(chunk, carry):
        wait_bytes(weights_ref.at[pl.ds(0, COLORS), pl.ds(0, ITEMS * rows)], send1_sem.at[chunk])
        return carry

    lax.fori_loop(0, CHUNKS, wait_packed, 0)
    third_stage(CHUNKS - 1, 0)
    square_land[me] = jnp.sum(square_acc[...], axis=0, keepdims=True) + vec_square

    for other in others:
        pltpu.make_async_remote_copy(
            square_land.at[me], square_land.at[me], small_sem.at[3], small_sem.at[4],
            device_id=(other,), device_id_type=MESH).start()
    wait_bytes(new_moment_ref, send2_sem.at[0])
    wait_bytes(new_second_ref, send2_sem.at[1])
    wait_bytes(square_land.at[pl.ds(0, GROUP - 1)], small_sem.at[4])
    norm = jnp.sqrt(jnp.sum(jnp.sum(square_land[...], axis=0), axis=1, keepdims=True))
    clip_coef = jnp.minimum(1.0, 1.0 / (norm + NORM_EPS))

    piece_rows = CHUNKS * rows // PIECES

    def piece_rows_at(color, piece):
        return pl.ds(pl.multiple_of(color * color_rows + piece * piece_rows, piece_rows), piece_rows)

    def link_copy(stage, owner, color, piece, hop, part=None):
        place = weights_ref.at[owner, piece_rows_at(color, piece) if part is None else part]
        return pltpu.make_async_remote_copy(
            place, place, send_sem.at[color], recv_sem.at[stage, color, piece],
            device_id=(me + flips[color][hop],), device_id_type=MESH)

    def core_copy(owner, color, piece):
        place = weights_ref.at[owner, piece_rows_at(color, piece)]
        return pltpu.make_async_remote_copy(
            place, place, core_send_sem.at[color], core_recv_sem.at[color],
            device_id=(partner,), device_id_type=MESH)

    def update_chunk(chunk, form):
        for color in range(COLORS):
            item = chunk * COLORS + color
            slot = item % RING
            wait_bytes(keep.at[slot], state_sem.at[slot])
            base = color * color_rows + chunk * rows

            def update(sub, inner):
                to = pl.ds(pl.multiple_of(sub * UPDATE_ROWS, UPDATE_ROWS), UPDATE_ROWS)
                out = pl.ds(pl.multiple_of(base + sub * UPDATE_ROWS, UPDATE_ROWS), UPDATE_ROWS)
                master, moment, second = adam_update(
                    new_master_ref[out, :], clip_coef, keep[slot, 0, to, :],
                    keep[slot, 1, to, :], keep[slot, 2, to, :], DECAY)
                new_master_ref[out, :] = master
                new_moment_ref[out, :] = moment
                new_second_ref[out, :] = second
                weights_ref[me, out, :] = master.astype(jnp.bfloat16)
                if form == 'parts':
                    for stage, hop in ((0, 0), (1, 1), (3, 2)):
                        link_copy(stage, me, color, 0, hop, out).start()
                return inner

            lax.fori_loop(0, rows // UPDATE_ROWS, update, 0)
            if form == 'chunk':
                for stage, hop in ((0, 0), (1, 1), (3, 2)):
                    link_copy(stage, me, color, 0, hop, rows_at(color, chunk)).start()
            if form == 'piece':
                link_copy(0, me, color, chunk // 2, 0).start()

            @pl.when(item + RING < CHUNKS * COLORS)
            def _():
                for copy in state_copies((item + RING) // COLORS, (item + RING) % COLORS):
                    copy.start()

    def update_later(piece, carry):
        update_chunk(piece * 2, None)
        update_chunk(piece * 2 + 1, 'piece')
        return carry

    update_chunk(0, 'parts')
    update_chunk(1, 'chunk')
    lax.fori_loop(1, PIECES, update_later, 0)

    vec_new = adam_update(vec_sum, clip_coef, vec_master_ref[...], vec_moment_ref[...], vec_second_ref[...], 0.0)
    vec_new_master_ref[...], vec_new_moment_ref[...], vec_new_second_ref[...] = vec_new
    vec_weights_ref[me] = vec_new[0].reshape(vec_share // LANES, LANES)

    def own_sends(piece, carry):
        for color in range(COLORS):
            @pl.when(piece > 0)
            def _():
                link_copy(1, me, color, piece, 1).start()

            core_copy(me, color, piece).start()
        return carry

    lax.fori_loop(0, PIECES, own_sends, 0)

    def own_sends_last(piece, carry):
        for color in range(COLORS):
            link_copy(3, me, color, piece, 2).start()
        return carry

    lax.fori_loop(1, PIECES, own_sends_last, 0)

    for other in others:
        pltpu.make_async_remote_copy(
            vec_weights_ref.at[me], vec_weights_ref.at[me], small_sem.at[5], small_sem.at[6],
            device_id=(other,), device_id_type=MESH).start()

    def arrivals(stage, hops, onward):
        def one_piece(piece, carry):
            for color in range(COLORS):
                owner = me + sum(flips[color][hop] for hop in hops)
                wait_bytes(weights_ref.at[owner, piece_rows_at(color, piece)], recv_sem.at[stage, color, piece])
                for next_stage, hop in onward:
                    link_copy(next_stage, owner, color, piece, hop).start()
                core_copy(owner, color, piece).start()
            return carry

        lax.fori_loop(0, PIECES, one_piece, 0)

    arrivals(0, (0,), ((2, 1), (4, 2)))
    arrivals(1, (1,), ((5, 2),))
    arrivals(3, (2,), ())
    arrivals(2, (0, 1), ((6, 2),))
    arrivals(4, (0, 2), ())
    arrivals(5, (1, 2), ())
    arrivals(6, (0, 1, 2), ())

    for color in range(COLORS):
        eight = weights_ref.at[pl.ds(0, 8), pl.ds(color * color_rows, color_rows)]
        wait_bytes(weights_ref.at[pl.ds(0, 7), pl.ds(color * color_rows, color_rows)], send_sem.at[color])
        wait_bytes(eight, core_send_sem.at[color])
        wait_bytes(eight, core_recv_sem.at[color])
    for index in (5, 6):
        wait_bytes(vec_weights_ref.at[pl.ds(0, GROUP - 1)], small_sem.at[index])
    for chunk in range(RING, CHUNKS):
        wait_bytes(keep.at[chunk], send3_sem.at[chunk])
    wait_bytes(vec_land.at[pl.ds(0, GROUP - 1)], small_sem.at[0])
    wait_bytes(square_land.at[pl.ds(0, GROUP - 1)], small_sem.at[3])


def step_call(grad_mat, grad_vec, states, vec_states):
    share = grad_mat.shape[1] // GROUP
    vec_share = grad_vec.shape[1] // GROUP
    rows = share // COLORS // CHUNKS // LANES
    hbm_spec = pl.BlockSpec(memory_space=pltpu.HBM)
    vmem_spec = pl.BlockSpec(memory_space=pltpu.VMEM)
    f32, bf16 = jnp.float32, jnp.bfloat16
    dma = pltpu.SemaphoreType.DMA
    return pl.pallas_call(
        functools.partial(step_kernel, rows, share, vec_share),
        name='adam_step',
        out_shape=(pltpu.VMEM((share // LANES, LANES), f32),) * 3 + (pltpu.VMEM((1, vec_share), f32),) * 3 + (
            pltpu.VMEM((GROUP, share // LANES, LANES), bf16),
            pltpu.VMEM((GROUP, vec_share // LANES, LANES), f32),
            jax.ShapeDtypeStruct((COLORS, CHUNKS, 4, 3 * rows, LANES), bf16),
            jax.ShapeDtypeStruct((CHUNKS, COLORS, 2, rows, LANES), f32)),
        in_specs=[hbm_spec] * 5 + [vmem_spec] * 3,
        out_specs=(vmem_spec,) * 8 + (hbm_spec,) * 2,
        scratch_shapes=[
            pltpu.VMEM((SLOTS, COLORS, 1, rows * LANES), bf16),
            pltpu.VMEM((CHUNKS, COLORS, rows, LANES), f32),
            pltpu.VMEM((2, 2, rows, LANES), f32),
            pltpu.VMEM((CHUNKS, COLORS, rows, LANES), f32),
            pltpu.VMEM((GROUP, 1, vec_share), bf16),
            pltpu.VMEM((GROUP, 1, LANES), f32),
            pltpu.VMEM((8, LANES), f32),
            dma((SLOTS,)), dma((SLOTS,)), dma((2,)), dma((RING,)),
            dma((CHUNKS,)), dma((2,)), dma((CHUNKS,)),
            dma((COLORS, CHUNKS)), dma((COLORS, CHUNKS)), dma((COLORS, CHUNKS)), dma((7,)),
            dma((COLORS,)), dma((7, COLORS, PIECES)), dma((COLORS,)), dma((COLORS,)),
        ],
        compiler_params=pltpu.CompilerParams(
            collective_id=0, has_side_effects=True, vmem_limit_bytes=SCRATCH_BYTES),
    )(grad_mat, grad_vec, *states, *vec_states)[:8]


def store_kernel(*refs):
    ins, outs, (vec_weights, sems) = refs[:8], refs[8:16], refs[16:]
    land, vec_land = ins[6:]
    places = [(ins[index], outs[index]) for index in range(3, 6)]
    for index in range(3):
        part = ins[index].shape[0] // STATE_PARTS
        places += [(ins[index].at[pl.ds(at * part, part)], outs[index].at[pl.ds(at * part, part)]) for at in range(STATE_PARTS)]
    for owner in range(GROUP):
        places.append((land.at[owner], outs[6].at[owner]))
    copies = [pltpu.make_async_copy(source, target, sems.at[index]) for index, (source, target) in enumerate(places)]
    for copy in copies:
        copy.start()
    vec_rows = vec_land.shape[1]
    for owner in range(GROUP):
        vec_weights[owner * vec_rows:(owner + 1) * vec_rows, :] = vec_land[owner]
    outs[7][...] = vec_weights[...].astype(jnp.bfloat16)
    for copy in copies:
        copy.wait()


def store_call(results):
    vmem_spec = pl.BlockSpec(memory_space=pltpu.VMEM)
    hbm_spec = pl.BlockSpec(memory_space=pltpu.HBM)
    dma = pltpu.SemaphoreType.DMA
    vec_rows = results[7].size // LANES
    return pl.pallas_call(
        store_kernel,
        name='store_results',
        out_shape=tuple(jax.ShapeDtypeStruct(result.shape, result.dtype) for result in results[:7]) + (
            jax.ShapeDtypeStruct((vec_rows, LANES), jnp.bfloat16),),
        in_specs=[vmem_spec] * 8,
        out_specs=(hbm_spec,) * 7 + (vmem_spec,),
        scratch_shapes=[pltpu.VMEM((vec_rows, LANES), jnp.float32), dma((3 + 3 * STATE_PARTS + GROUP,))],
        compiler_params=pltpu.CompilerParams(vmem_limit_bytes=SCRATCH_BYTES),
    )(*[pltpu.with_memory_space_constraint(result, pltpu.VMEM) for result in results])


def solution(mesh):
    def local_step(grad_mat, grad_vec, master_mat, moment_mat, second_mat, master_vec, moment_vec, second_vec):
        states = [state.reshape(-1, LANES) for state in (master_mat, moment_mat, second_mat)]
        vec_states = [state.reshape(1, -1) for state in (master_vec, moment_vec, second_vec)]
        results = store_call(step_call(grad_mat, grad_vec, states, vec_states))
        return tuple(result.reshape(-1) for result in results)

    row_spec = P(AXIS, None)
    flat_spec = P(AXIS)
    whole_spec = P()
    return jax.shard_map(local_step, mesh=mesh,
                         in_specs=(row_spec, row_spec) + (flat_spec,) * 6,
                         out_specs=(flat_spec,) * 6 + (whole_spec, whole_spec),
                         check_vma=False)
```

```python
import functools

import jax
import jax.numpy as jnp
from jax import lax
from jax.experimental import pallas as pl
from jax.experimental.pallas import tpu as pltpu
from jax.sharding import PartitionSpec as P

STEP = 4
LEARN_RATE = 1e-3
BETA_ONE = 0.9
BETA_TWO = 0.999
ADAM_EPS = 1e-8
DECAY = 0.01
NORM_EPS = 1e-6
FIX_ONE = 1.0 - BETA_ONE ** STEP
FIX_TWO = 1.0 - BETA_TWO ** STEP

AXIS = 'fsdp'
MESH = pl.DeviceIdType.MESH
GROUP = 16
LANES = 128
ORDERS = ((2, 4, 8), (4, 8, 2), (8, 2, 4))
COLORS = len(ORDERS)
CHUNKS = 8
AHEAD = 2
SLOTS = 3
PIECES = 4
SUB_ROWS = 80
UPDATE_ROWS = 80
RING = 4
STATE_PARTS = 2
ITEMS = 12
SCRATCH_BYTES = 12_800_000


def adam_update(grad_sum, clip_coef, master, moment, second, decay):
    clip_grad = clip_coef * grad_sum
    new_moment = BETA_ONE * moment + (1.0 - BETA_ONE) * clip_grad
    new_second = BETA_TWO * second + (1.0 - BETA_TWO) * clip_grad * clip_grad
    step_dir = (new_moment / FIX_ONE) / (jnp.sqrt(new_second / FIX_TWO) + ADAM_EPS)
    new_master = master - LEARN_RATE * (step_dir + decay * master)
    return new_master, new_moment, new_second


def flip_of(me, bit):
    return bit * (1 - 2 * ((me // bit) % 2))


def step_kernel(rows, share, vec_share, grad_ref, vec_ref, master_ref, moment_ref, second_ref,
                vec_master_ref, vec_moment_ref, vec_second_ref,
                new_master_ref, new_moment_ref, new_second_ref,
                vec_new_master_ref, vec_new_moment_ref, vec_new_second_ref, weights_ref, vec_weights_ref,
                land_ref, recv2,
                pad_in, keep, recv2_in, recv3, vec_land, square_land, square_acc,
                pad_sem, part_sem, recv2_in_sem, state_sem,
                send1_sem, send2_sem, send3_sem, recv1_sem, recv2_sem, recv3_sem, small_sem,
                send_sem, recv_sem, core_send_sem, core_recv_sem):
    me = lax.axis_index(AXIS)
    core = me % 2
    partner = me + flip_of(me, 1)
    block = rows * LANES
    color_len = share // COLORS
    color_rows = color_len // LANES
    flips = [[flip_of(me, bit) for bit in order] for order in ORDERS]
    piece_rows = CHUNKS * rows // PIECES
    per_owner = share // LANES // piece_rows
    neighbours = [partner] + [me + flip_of(me, bit) + other for bit in ORDERS[0] for other in (0, flip_of(me, 1))]
    others = [me + sum(flip_of(me, bit) for bit in (1, 2, 4, 8) if mask & bit)
              for mask in sorted(range(1, GROUP), key=lambda mask: (-(mask >> 1).bit_count(), mask))]

    def wait_bytes(ref, sem):
        pltpu.make_async_copy(ref, ref, sem).wait()

    def rows_at(color, chunk):
        return pl.ds(pl.multiple_of(color * color_rows + chunk * rows, rows), rows)

    def piece_at(owner, color, chunk):
        start = pl.multiple_of(owner * share + color * color_len + chunk * block, block)
        return grad_ref.at[:, pl.ds(start, block)]

    def packed_at(color, piece, item):
        index = (piece * COLORS + color) * ITEMS + item
        return index // per_owner, pl.multiple_of((index % per_owner) * piece_rows, piece_rows)

    part_owner = COLORS * PIECES * ITEMS // per_owner
    part_rows = 3 * rows

    def route(item, color):
        place, kind = item // 3, (item + 1) % 3
        flip1, flip2, flip3 = flips[color]
        local = (2 - kind) // 2
        target_core = local * (1 - core) + (1 - local) * (kind - 1)
        target = me - core + (1 - local) * flip1 + target_core
        owner = target + (1 - place // 2) * flip2 + (1 - place % 2) * flip3
        source = (1 - local) * (1 + core)
        return owner, target, source, place

    def start_in(piece, step):
        for color in range(COLORS):
            owner = route(step // 2, color)[0]
            pltpu.make_async_copy(piece_at(owner, color, piece * 2 + step % 2), pad_in.at[step % SLOTS, color],
                                  pad_sem.at[step % SLOTS]).start()

    def pack_step(piece, step):
        wait_bytes(pad_in.at[step % SLOTS], pad_sem.at[step % SLOTS])
        for color in range(COLORS):
            place_owner, place_row = packed_at(color, piece, step // 2)

            def pack(sub, inner):
                off = pl.multiple_of(sub * SUB_ROWS * LANES, SUB_ROWS * LANES)
                vals = pad_in[step % SLOTS, color, :, pl.ds(off, SUB_ROWS * LANES)].astype(jnp.float32)
                to = pl.multiple_of(place_row + (step % 2) * rows + sub * SUB_ROWS, SUB_ROWS)
                weights_ref[place_owner, pl.ds(to, SUB_ROWS), :] = (
                    vals.reshape(SUB_ROWS, LANES).astype(jnp.bfloat16))
                return inner

            lax.fori_loop(0, rows // SUB_ROWS, pack, 0, unroll=True)

    def send_item(piece, item, start=0, size=None):
        size = piece_rows if size is None else size
        for color in range(COLORS):
            owner, target, source, place = route(item, color)
            place_owner, place_row = packed_at(color, piece, item)
            from_row = pl.multiple_of(place_row + start, rows)
            to_row = pl.multiple_of(source * piece_rows + start, rows)
            pltpu.make_async_remote_copy(
                weights_ref.at[place_owner, pl.ds(from_row, size)],
                land_ref.at[color, piece, place, pl.ds(to_row, size)],
                send1_sem.at[piece], recv1_sem.at[color, piece], device_id=(target,), device_id_type=MESH).start()

    def pack_and_send(piece, first):
        def one_step(step, carry):
            @pl.when(step + SLOTS - 1 < 2 * ITEMS)
            def _():
                start_in(piece, step + SLOTS - 1)

            pack_step(piece, step)

            @pl.when(step % 2 == 1)
            def _():
                send_item(piece, step // 2)

            return carry

        lax.fori_loop(first, 2 * ITEMS, one_step, 0)

    def start_parts(chunk, place):
        slot = place % SLOTS
        for color in range(COLORS):
            flip1, flip2, flip3 = flips[color]
            owner = me + (1 - place // 2) * flip2 + (1 - place % 2) * flip3
            for source in range(3):
                row = pl.multiple_of(source * piece_rows + (chunk % 2) * rows, rows)
                pltpu.make_async_copy(land_ref.at[color, chunk // 2, place, pl.ds(row, rows)],
                                      weights_ref.at[part_owner + slot, pl.ds(color * part_rows + source * rows, rows)],
                                      part_sem.at[slot]).start()
            pltpu.make_async_copy(piece_at(owner, color, chunk), pad_in.at[slot, color], pad_sem.at[slot]).start()

    def first_sums(chunk):
        for place in range(SLOTS - 1):
            start_parts(chunk, place)
        for place in range(4):
            slot = place % SLOTS
            if place + SLOTS - 1 < 4:
                start_parts(chunk, place + SLOTS - 1)
            wait_bytes(weights_ref.at[part_owner + slot, pl.ds(0, COLORS * part_rows)], part_sem.at[slot])
            wait_bytes(pad_in.at[slot], pad_sem.at[slot])
            for color in range(COLORS):
                at = rows_at(color, chunk)
                total = (new_moment_ref.at[at], new_second_ref.at[at], keep.at[chunk, color], new_master_ref.at[at])[place]

                def add(sub, inner):
                    off = pl.multiple_of(sub * SUB_ROWS * LANES, SUB_ROWS * LANES)
                    to = pl.ds(pl.multiple_of(sub * SUB_ROWS, SUB_ROWS), SUB_ROWS)
                    vals = pad_in[slot, color, :, pl.ds(off, SUB_ROWS * LANES)].astype(jnp.float32)
                    vals = vals.reshape(SUB_ROWS, LANES)
                    for source in range(3):
                        row = pl.multiple_of(color * part_rows + source * rows + sub * SUB_ROWS, SUB_ROWS)
                        vals = vals + weights_ref[part_owner + slot, pl.ds(row, SUB_ROWS), :].astype(jnp.float32)
                    total[to, :] = vals
                    return inner

                lax.fori_loop(0, rows // SUB_ROWS, add, 0, unroll=True)
                if place < 2:
                    pltpu.make_async_remote_copy(
                        total, recv2.at[chunk, color, place], send2_sem.at[place], recv2_sem.at[color, chunk],
                        device_id=(me + flips[color][1],), device_id_type=MESH).start()

    for step in range(SLOTS):
        start_in(0, step)
    barrier = pltpu.get_barrier_semaphore()
    for neighbour in neighbours:
        pl.semaphore_signal(barrier, inc=1, device_id=(neighbour,), device_id_type=MESH)
    pack_step(0, 0)
    pl.semaphore_wait(barrier, len(neighbours))
    send_item(0, 0, 0, rows)
    start_in(0, SLOTS)
    pack_step(0, 1)
    send_item(0, 0, rows, rows)
    pack_and_send(0, 2)

    def pack_ahead(piece, carry):
        for step in range(SLOTS - 1):
            start_in(piece, step)
        pack_and_send(piece, 0)
        return carry

    lax.fori_loop(1, AHEAD, pack_ahead, 0)

    def first_stage(piece, carry):
        for color in range(COLORS):
            wait_bytes(land_ref.at[color, piece], recv1_sem.at[color, piece])

        def one_chunk(chunk, inner):
            first_sums(chunk)
            return inner

        lax.fori_loop(2 * piece, 2 * piece + 2, one_chunk, 0)

        @pl.when(piece + AHEAD < PIECES)
        def _():
            for step in range(SLOTS - 1):
                start_in(piece + AHEAD, step)
            pack_and_send(piece + AHEAD, 0)

        return carry

    lax.fori_loop(0, PIECES, first_stage, 0)

    def second_stage(chunk, carry):
        copies = [pltpu.make_async_copy(recv2.at[chunk, color], recv2_in.at[color % 2], recv2_in_sem.at[color % 2])
                  for color in range(COLORS)]

        def fetch(color):
            wait_bytes(recv2.at[chunk, color], recv2_sem.at[color, chunk])
            copies[color].start()

        fetch(0)
        fetch(1)
        for color in range(COLORS):
            copies[color].wait()
            base = color * color_rows + chunk * rows

            def add(sub, inner):
                to = pl.ds(pl.multiple_of(sub * SUB_ROWS, SUB_ROWS), SUB_ROWS)
                out = pl.ds(pl.multiple_of(base + sub * SUB_ROWS, SUB_ROWS), SUB_ROWS)
                keep[chunk, color, to, :] += recv2_in[color % 2, 0, to, :]
                new_master_ref[out, :] += recv2_in[color % 2, 1, to, :]
                return inner

            lax.fori_loop(0, rows // SUB_ROWS, add, 0)
            pltpu.make_async_remote_copy(
                keep.at[chunk, color], recv3.at[chunk, color], send3_sem.at[chunk], recv3_sem.at[color, chunk],
                device_id=(me + flips[color][2],), device_id_type=MESH).start()
            if color == 0:
                fetch(2)
        return carry

    second_stage(0, 0)
    for other in others:
        pltpu.make_async_remote_copy(
            vec_ref.at[:, pl.ds(pl.multiple_of(other * vec_share, vec_share), vec_share)], vec_land.at[me],
            small_sem.at[0], small_sem.at[1], device_id=(other,), device_id_type=MESH).start()
    vec_own = pltpu.make_async_copy(
        vec_ref.at[:, pl.ds(pl.multiple_of(me * vec_share, vec_share), vec_share)], vec_land.at[me], small_sem.at[2])
    vec_own.start()
    lax.fori_loop(1, CHUNKS, second_stage, 0)

    square_acc[...] = jnp.zeros_like(square_acc)

    def third_stage(chunk, carry):
        for color in range(COLORS):
            wait_bytes(recv3.at[chunk, color], recv3_sem.at[color, chunk])
            base = color * color_rows + chunk * rows

            def add(sub, squares):
                to = pl.ds(pl.multiple_of(sub * SUB_ROWS, SUB_ROWS), SUB_ROWS)
                out = pl.ds(pl.multiple_of(base + sub * SUB_ROWS, SUB_ROWS), SUB_ROWS)
                vals = new_master_ref[out, :] + recv3[chunk, color, to, :]
                new_master_ref[out, :] = vals
                return squares + jnp.sum((vals * vals).reshape(SUB_ROWS // 8, 8, LANES), axis=0)

            squares = lax.fori_loop(0, rows // SUB_ROWS, add, jnp.zeros((8, LANES), jnp.float32), unroll=True)
            square_acc[...] += squares
        return carry

    def state_copies(chunk, color):
        slot = (chunk * COLORS + color) % RING
        at = rows_at(color, chunk)
        return [pltpu.make_async_copy(ref.at[at], keep.at[slot, index], state_sem.at[slot])
                for index, ref in enumerate((master_ref, moment_ref, second_ref))]

    lax.fori_loop(0, CHUNKS - 2, third_stage, 0)
    for chunk in range(RING):
        wait_bytes(keep.at[chunk], send3_sem.at[chunk])
    for item in range(RING):
        for copy in state_copies(item // COLORS, item % COLORS):
            copy.start()
    third_stage(CHUNKS - 2, 0)

    vec_own.wait()
    wait_bytes(vec_land.at[pl.ds(0, GROUP - 1)], small_sem.at[1])
    vec_sum = jnp.sum(vec_land[...].astype(jnp.float32), axis=0)
    vec_square = sum(vec_sum[:, part * LANES:(part + 1) * LANES] ** 2 for part in range(vec_share // LANES))

    def wait_packed(piece, carry):
        wait_bytes(weights_ref.at[pl.ds(0, COLORS), pl.ds(0, ITEMS * piece_rows)], send1_sem.at[piece])
        return carry

    lax.fori_loop(0, PIECES, wait_packed, 0)
    third_stage(CHUNKS - 1, 0)
    square_land[me] = jnp.sum(square_acc[...], axis=0, keepdims=True) + vec_square

    for other in others:
        pltpu.make_async_remote_copy(
            square_land.at[me], square_land.at[me], small_sem.at[3], small_sem.at[4],
            device_id=(other,), device_id_type=MESH).start()
    wait_bytes(new_moment_ref, send2_sem.at[0])
    wait_bytes(new_second_ref, send2_sem.at[1])
    wait_bytes(square_land.at[pl.ds(0, GROUP - 1)], small_sem.at[4])
    norm = jnp.sqrt(jnp.sum(jnp.sum(square_land[...], axis=0), axis=1, keepdims=True))
    clip_coef = jnp.minimum(1.0, 1.0 / (norm + NORM_EPS))

    def piece_rows_at(color, piece):
        return pl.ds(pl.multiple_of(color * color_rows + piece * piece_rows, piece_rows), piece_rows)

    def link_copy(stage, owner, color, piece, hop, part=None):
        place = weights_ref.at[owner, piece_rows_at(color, piece) if part is None else part]
        return pltpu.make_async_remote_copy(
            place, place, send_sem.at[color], recv_sem.at[stage, color, piece],
            device_id=(me + flips[color][hop],), device_id_type=MESH)

    def core_copy(owner, color, piece):
        place = weights_ref.at[owner, piece_rows_at(color, piece)]
        return pltpu.make_async_remote_copy(
            place, place, core_send_sem.at[color], core_recv_sem.at[color],
            device_id=(partner,), device_id_type=MESH)

    def update_chunk(chunk, form):
        for color in range(COLORS):
            item = chunk * COLORS + color
            slot = item % RING
            wait_bytes(keep.at[slot], state_sem.at[slot])
            base = color * color_rows + chunk * rows

            def update(sub, inner):
                to = pl.ds(pl.multiple_of(sub * UPDATE_ROWS, UPDATE_ROWS), UPDATE_ROWS)
                out = pl.ds(pl.multiple_of(base + sub * UPDATE_ROWS, UPDATE_ROWS), UPDATE_ROWS)
                master, moment, second = adam_update(
                    new_master_ref[out, :], clip_coef, keep[slot, 0, to, :],
                    keep[slot, 1, to, :], keep[slot, 2, to, :], DECAY)
                new_master_ref[out, :] = master
                new_moment_ref[out, :] = moment
                new_second_ref[out, :] = second
                weights_ref[me, out, :] = master.astype(jnp.bfloat16)
                if form == 'parts':
                    for stage, hop in ((0, 0), (1, 1), (3, 2)):
                        link_copy(stage, me, color, 0, hop, out).start()
                return inner

            lax.fori_loop(0, rows // UPDATE_ROWS, update, 0)
            if form == 'chunk':
                for stage, hop in ((0, 0), (1, 1), (3, 2)):
                    link_copy(stage, me, color, 0, hop, rows_at(color, chunk)).start()
            if form == 'piece':
                link_copy(0, me, color, chunk // 2, 0).start()

            @pl.when(item + RING < CHUNKS * COLORS)
            def _():
                for copy in state_copies((item + RING) // COLORS, (item + RING) % COLORS):
                    copy.start()

    def update_later(piece, carry):
        update_chunk(piece * 2, None)
        update_chunk(piece * 2 + 1, 'piece')
        return carry

    update_chunk(0, 'parts')
    update_chunk(1, 'chunk')
    lax.fori_loop(1, PIECES, update_later, 0)

    vec_new = adam_update(vec_sum, clip_coef, vec_master_ref[...], vec_moment_ref[...], vec_second_ref[...], 0.0)
    vec_new_master_ref[...], vec_new_moment_ref[...], vec_new_second_ref[...] = vec_new
    vec_weights_ref[me] = vec_new[0].reshape(vec_share // LANES, LANES)

    def own_sends(piece, carry):
        for color in range(COLORS):
            @pl.when(piece > 0)
            def _():
                link_copy(1, me, color, piece, 1).start()

            core_copy(me, color, piece).start()
        return carry

    lax.fori_loop(0, PIECES, own_sends, 0)

    def own_sends_last(piece, carry):
        for color in range(COLORS):
            link_copy(3, me, color, piece, 2).start()
        return carry

    lax.fori_loop(1, PIECES, own_sends_last, 0)

    for other in others:
        pltpu.make_async_remote_copy(
            vec_weights_ref.at[me], vec_weights_ref.at[me], small_sem.at[5], small_sem.at[6],
            device_id=(other,), device_id_type=MESH).start()

    def arrivals(stage, hops, onward):
        def one_piece(piece, carry):
            for color in range(COLORS):
                owner = me + sum(flips[color][hop] for hop in hops)
                wait_bytes(weights_ref.at[owner, piece_rows_at(color, piece)], recv_sem.at[stage, color, piece])
                for next_stage, hop in onward:
                    link_copy(next_stage, owner, color, piece, hop).start()
                core_copy(owner, color, piece).start()
            return carry

        lax.fori_loop(0, PIECES, one_piece, 0)

    arrivals(0, (0,), ((2, 1), (4, 2)))
    arrivals(1, (1,), ((5, 2),))
    arrivals(3, (2,), ())
    arrivals(2, (0, 1), ((6, 2),))
    arrivals(4, (0, 2), ())
    arrivals(5, (1, 2), ())
    arrivals(6, (0, 1, 2), ())

    for color in range(COLORS):
        eight = weights_ref.at[pl.ds(0, 8), pl.ds(color * color_rows, color_rows)]
        wait_bytes(weights_ref.at[pl.ds(0, 7), pl.ds(color * color_rows, color_rows)], send_sem.at[color])
        wait_bytes(eight, core_send_sem.at[color])
        wait_bytes(eight, core_recv_sem.at[color])
    for index in (5, 6):
        wait_bytes(vec_weights_ref.at[pl.ds(0, GROUP - 1)], small_sem.at[index])
    for chunk in range(RING, CHUNKS):
        wait_bytes(keep.at[chunk], send3_sem.at[chunk])
    wait_bytes(vec_land.at[pl.ds(0, GROUP - 1)], small_sem.at[0])
    wait_bytes(square_land.at[pl.ds(0, GROUP - 1)], small_sem.at[3])


def step_call(grad_mat, grad_vec, states, vec_states):
    share = grad_mat.shape[1] // GROUP
    vec_share = grad_vec.shape[1] // GROUP
    rows = share // COLORS // CHUNKS // LANES
    hbm_spec = pl.BlockSpec(memory_space=pltpu.HBM)
    vmem_spec = pl.BlockSpec(memory_space=pltpu.VMEM)
    f32, bf16 = jnp.float32, jnp.bfloat16
    dma = pltpu.SemaphoreType.DMA
    return pl.pallas_call(
        functools.partial(step_kernel, rows, share, vec_share),
        name='adam_step',
        out_shape=(pltpu.VMEM((share // LANES, LANES), f32),) * 3 + (pltpu.VMEM((1, vec_share), f32),) * 3 + (
            pltpu.VMEM((GROUP, share // LANES, LANES), bf16),
            pltpu.VMEM((GROUP, vec_share // LANES, LANES), f32),
            jax.ShapeDtypeStruct((COLORS, PIECES, 4, 3 * CHUNKS * rows // PIECES, LANES), bf16),
            jax.ShapeDtypeStruct((CHUNKS, COLORS, 2, rows, LANES), f32)),
        in_specs=[hbm_spec] * 5 + [vmem_spec] * 3,
        out_specs=(vmem_spec,) * 8 + (hbm_spec,) * 2,
        scratch_shapes=[
            pltpu.VMEM((SLOTS, COLORS, 1, rows * LANES), bf16),
            pltpu.VMEM((CHUNKS, COLORS, rows, LANES), f32),
            pltpu.VMEM((2, 2, rows, LANES), f32),
            pltpu.VMEM((CHUNKS, COLORS, rows, LANES), f32),
            pltpu.VMEM((GROUP, 1, vec_share), bf16),
            pltpu.VMEM((GROUP, 1, LANES), f32),
            pltpu.VMEM((8, LANES), f32),
            dma((SLOTS,)), dma((SLOTS,)), dma((2,)), dma((RING,)),
            dma((PIECES,)), dma((2,)), dma((CHUNKS,)),
            dma((COLORS, PIECES)), dma((COLORS, CHUNKS)), dma((COLORS, CHUNKS)), dma((7,)),
            dma((COLORS,)), dma((7, COLORS, PIECES)), dma((COLORS,)), dma((COLORS,)),
        ],
        compiler_params=pltpu.CompilerParams(
            collective_id=0, has_side_effects=True, vmem_limit_bytes=SCRATCH_BYTES),
    )(grad_mat, grad_vec, *states, *vec_states)[:8]


def store_kernel(*refs):
    ins, outs, (vec_weights, sems) = refs[:8], refs[8:16], refs[16:]
    land, vec_land = ins[6:]
    places = [(ins[index], outs[index]) for index in range(3, 6)]
    for index in range(3):
        part = ins[index].shape[0] // STATE_PARTS
        places += [(ins[index].at[pl.ds(at * part, part)], outs[index].at[pl.ds(at * part, part)]) for at in range(STATE_PARTS)]
    for owner in range(GROUP):
        places.append((land.at[owner], outs[6].at[owner]))
    copies = [pltpu.make_async_copy(source, target, sems.at[index]) for index, (source, target) in enumerate(places)]
    for copy in copies:
        copy.start()
    vec_rows = vec_land.shape[1]
    for owner in range(GROUP):
        vec_weights[owner * vec_rows:(owner + 1) * vec_rows, :] = vec_land[owner]
    outs[7][...] = vec_weights[...].astype(jnp.bfloat16)
    for copy in copies:
        copy.wait()


def store_call(results):
    vmem_spec = pl.BlockSpec(memory_space=pltpu.VMEM)
    hbm_spec = pl.BlockSpec(memory_space=pltpu.HBM)
    dma = pltpu.SemaphoreType.DMA
    vec_rows = results[7].size // LANES
    return pl.pallas_call(
        store_kernel,
        name='store_results',
        out_shape=tuple(jax.ShapeDtypeStruct(result.shape, result.dtype) for result in results[:7]) + (
            jax.ShapeDtypeStruct((vec_rows, LANES), jnp.bfloat16),),
        in_specs=[vmem_spec] * 8,
        out_specs=(hbm_spec,) * 7 + (vmem_spec,),
        scratch_shapes=[pltpu.VMEM((vec_rows, LANES), jnp.float32), dma((3 + 3 * STATE_PARTS + GROUP,))],
        compiler_params=pltpu.CompilerParams(vmem_limit_bytes=SCRATCH_BYTES),
    )(*[pltpu.with_memory_space_constraint(result, pltpu.VMEM) for result in results])


def solution(mesh):
    def local_step(grad_mat, grad_vec, master_mat, moment_mat, second_mat, master_vec, moment_vec, second_vec):
        states = [state.reshape(-1, LANES) for state in (master_mat, moment_mat, second_mat)]
        vec_states = [state.reshape(1, -1) for state in (master_vec, moment_vec, second_vec)]
        results = store_call(step_call(grad_mat, grad_vec, states, vec_states))
        return tuple(result.reshape(-1) for result in results)

    row_spec = P(AXIS, None)
    flat_spec = P(AXIS)
    whole_spec = P()
    return jax.shard_map(local_step, mesh=mesh,
                         in_specs=(row_spec, row_spec) + (flat_spec,) * 6,
                         out_specs=(flat_spec,) * 6 + (whole_spec, whole_spec),
                         check_vma=False)
```

```python
import functools

import jax
import jax.numpy as jnp
from jax import lax
from jax.experimental import pallas as pl
from jax.experimental.pallas import tpu as pltpu
from jax.sharding import PartitionSpec as P

STEP = 4
LEARN_RATE = 1e-3
BETA_ONE = 0.9
BETA_TWO = 0.999
ADAM_EPS = 1e-8
DECAY = 0.01
NORM_EPS = 1e-6
FIX_ONE = 1.0 - BETA_ONE ** STEP
FIX_TWO = 1.0 - BETA_TWO ** STEP

AXIS = 'fsdp'
MESH = pl.DeviceIdType.MESH
GROUP = 16
LANES = 128
ORDERS = ((2, 4, 8), (4, 8, 2), (8, 2, 4))
COLORS = len(ORDERS)
CHUNKS = 8
AHEAD = 2
SLOTS = 3
PIECES = 4
IN_FLIGHT = 8
SUB_ROWS = 80
UPDATE_ROWS = 80
RING = 4
STATE_PARTS = 2
ITEMS = 12
SCRATCH_BYTES = 12_800_000


def adam_update(grad_sum, clip_coef, master, moment, second, decay):
    clip_grad = clip_coef * grad_sum
    new_moment = BETA_ONE * moment + (1.0 - BETA_ONE) * clip_grad
    new_second = BETA_TWO * second + (1.0 - BETA_TWO) * clip_grad * clip_grad
    step_dir = (new_moment / FIX_ONE) / (jnp.sqrt(new_second / FIX_TWO) + ADAM_EPS)
    new_master = master - LEARN_RATE * (step_dir + decay * master)
    return new_master, new_moment, new_second


def flip_of(me, bit):
    return bit * (1 - 2 * ((me // bit) % 2))


def step_kernel(rows, share, vec_share, grad_ref, vec_ref, master_ref, moment_ref, second_ref,
                vec_master_ref, vec_moment_ref, vec_second_ref,
                new_master_ref, new_moment_ref, new_second_ref,
                vec_new_master_ref, vec_new_moment_ref, vec_new_second_ref, weights_ref, vec_weights_ref,
                land_ref, recv2,
                pad_in, keep, recv2_in, recv3, vec_land, square_land, square_acc,
                pad_sem, part_sem, recv2_in_sem, state_sem,
                send1_sem, send2_sem, send3_sem, recv1_sem, recv2_sem, recv3_sem, small_sem,
                send_sem, recv_sem, core_send_sem, core_recv_sem):
    me = lax.axis_index(AXIS)
    core = me % 2
    partner = me + flip_of(me, 1)
    block = rows * LANES
    color_len = share // COLORS
    color_rows = color_len // LANES
    flips = [[flip_of(me, bit) for bit in order] for order in ORDERS]
    piece_rows = CHUNKS * rows // PIECES
    per_owner = share // LANES // piece_rows
    neighbours = [partner] + [me + flip_of(me, bit) + other for bit in ORDERS[0] for other in (0, flip_of(me, 1))]
    others = [me + sum(flip_of(me, bit) for bit in (1, 2, 4, 8) if mask & bit)
              for mask in sorted(range(1, GROUP), key=lambda mask: (-(mask >> 1).bit_count(), mask))]

    def wait_bytes(ref, sem):
        pltpu.make_async_copy(ref, ref, sem).wait()

    def rows_at(color, chunk):
        return pl.ds(pl.multiple_of(color * color_rows + chunk * rows, rows), rows)

    def piece_at(owner, color, chunk):
        start = pl.multiple_of(owner * share + color * color_len + chunk * block, block)
        return grad_ref.at[:, pl.ds(start, block)]

    def packed_at(color, piece, item):
        index = (piece * COLORS + color) * ITEMS + item
        return index // per_owner, pl.multiple_of((index % per_owner) * piece_rows, piece_rows)

    part_owner = COLORS * PIECES * ITEMS // per_owner
    part_rows = 3 * rows

    def route(item, color):
        place, kind = item // 3, (item + 1) % 3
        flip1, flip2, flip3 = flips[color]
        local = (2 - kind) // 2
        target_core = local * (1 - core) + (1 - local) * (kind - 1)
        target = me - core + (1 - local) * flip1 + target_core
        owner = target + (1 - place // 2) * flip2 + (1 - place % 2) * flip3
        source = (1 - local) * (1 + core)
        return owner, target, source, place

    def start_in(piece, step):
        for color in range(COLORS):
            owner = route(step // 2, color)[0]
            pltpu.make_async_copy(piece_at(owner, color, piece * 2 + step % 2), pad_in.at[step % SLOTS, color],
                                  pad_sem.at[step % SLOTS]).start()

    def pack_step(piece, step):
        wait_bytes(pad_in.at[step % SLOTS], pad_sem.at[step % SLOTS])
        for color in range(COLORS):
            place_owner, place_row = packed_at(color, piece, step // 2)

            def pack(sub, inner):
                off = pl.multiple_of(sub * SUB_ROWS * LANES, SUB_ROWS * LANES)
                vals = pad_in[step % SLOTS, color, :, pl.ds(off, SUB_ROWS * LANES)].astype(jnp.float32)
                to = pl.multiple_of(place_row + (step % 2) * rows + sub * SUB_ROWS, SUB_ROWS)
                weights_ref[place_owner, pl.ds(to, SUB_ROWS), :] = (
                    vals.reshape(SUB_ROWS, LANES).astype(jnp.bfloat16))
                return inner

            lax.fori_loop(0, rows // SUB_ROWS, pack, 0, unroll=True)

    def send_item(piece, item, start=0, size=None):
        size = piece_rows if size is None else size
        for color in range(COLORS):
            owner, target, source, place = route(item, color)
            place_owner, place_row = packed_at(color, piece, item)
            from_row = pl.multiple_of(place_row + start, rows)
            to_row = pl.multiple_of(source * piece_rows + start, rows)
            pltpu.make_async_remote_copy(
                weights_ref.at[place_owner, pl.ds(from_row, size)],
                land_ref.at[color, piece, place, pl.ds(to_row, size)],
                send1_sem.at[(piece * ITEMS + item) % IN_FLIGHT], recv1_sem.at[color, piece], device_id=(target,), device_id_type=MESH).start()

    def wait_left(index):
        wait_bytes(weights_ref.at[0, pl.ds(0, COLORS * piece_rows)], send1_sem.at[index])

    def pack_and_send(piece, first):
        def one_step(step, carry):
            @pl.when(step + SLOTS - 1 < 2 * ITEMS)
            def _():
                start_in(piece, step + SLOTS - 1)

            @pl.when(piece * ITEMS + step // 2 - (step % 2) * ITEMS * PIECES >= IN_FLIGHT)
            def _():
                wait_left((piece * ITEMS + step // 2) % IN_FLIGHT)

            pack_step(piece, step)

            @pl.when(step % 2 == 1)
            def _():
                send_item(piece, step // 2)

            return carry

        lax.fori_loop(first, 2 * ITEMS, one_step, 0)

    def start_parts(chunk, place):
        slot = place % SLOTS
        for color in range(COLORS):
            flip1, flip2, flip3 = flips[color]
            owner = me + (1 - place // 2) * flip2 + (1 - place % 2) * flip3
            for source in range(3):
                row = pl.multiple_of(source * piece_rows + (chunk % 2) * rows, rows)
                pltpu.make_async_copy(land_ref.at[color, chunk // 2, place, pl.ds(row, rows)],
                                      weights_ref.at[part_owner + slot, pl.ds(color * part_rows + source * rows, rows)],
                                      part_sem.at[slot]).start()
            pltpu.make_async_copy(piece_at(owner, color, chunk), pad_in.at[slot, color], pad_sem.at[slot]).start()

    def first_sums(chunk):
        for place in range(SLOTS - 1):
            start_parts(chunk, place)
        for place in range(4):
            slot = place % SLOTS
            if place + SLOTS - 1 < 4:
                start_parts(chunk, place + SLOTS - 1)
            wait_bytes(weights_ref.at[part_owner + slot, pl.ds(0, COLORS * part_rows)], part_sem.at[slot])
            wait_bytes(pad_in.at[slot], pad_sem.at[slot])
            for color in range(COLORS):
                at = rows_at(color, chunk)
                total = (new_moment_ref.at[at], new_second_ref.at[at], keep.at[chunk, color], new_master_ref.at[at])[place]

                def add(sub, inner):
                    off = pl.multiple_of(sub * SUB_ROWS * LANES, SUB_ROWS * LANES)
                    to = pl.ds(pl.multiple_of(sub * SUB_ROWS, SUB_ROWS), SUB_ROWS)
                    vals = pad_in[slot, color, :, pl.ds(off, SUB_ROWS * LANES)].astype(jnp.float32)
                    vals = vals.reshape(SUB_ROWS, LANES)
                    for source in range(3):
                        row = pl.multiple_of(color * part_rows + source * rows + sub * SUB_ROWS, SUB_ROWS)
                        vals = vals + weights_ref[part_owner + slot, pl.ds(row, SUB_ROWS), :].astype(jnp.float32)
                    total[to, :] = vals
                    return inner

                lax.fori_loop(0, rows // SUB_ROWS, add, 0, unroll=True)
                if place < 2:
                    pltpu.make_async_remote_copy(
                        total, recv2.at[chunk, color, place], send2_sem.at[place], recv2_sem.at[color, chunk],
                        device_id=(me + flips[color][1],), device_id_type=MESH).start()

    for step in range(SLOTS):
        start_in(0, step)
    barrier = pltpu.get_barrier_semaphore()
    for neighbour in neighbours:
        pl.semaphore_signal(barrier, inc=1, device_id=(neighbour,), device_id_type=MESH)
    pack_step(0, 0)
    pl.semaphore_wait(barrier, len(neighbours))
    send_item(0, 0, 0, rows)
    start_in(0, SLOTS)
    pack_step(0, 1)
    send_item(0, 0, rows, rows)
    pack_and_send(0, 2)

    def pack_ahead(piece, carry):
        for step in range(SLOTS - 1):
            start_in(piece, step)
        pack_and_send(piece, 0)
        return carry

    lax.fori_loop(1, AHEAD, pack_ahead, 0)

    def first_stage(piece, carry):
        for color in range(COLORS):
            wait_bytes(land_ref.at[color, piece], recv1_sem.at[color, piece])

        def one_chunk(chunk, inner):
            first_sums(chunk)
            return inner

        lax.fori_loop(2 * piece, 2 * piece + 2, one_chunk, 0)

        @pl.when(piece + AHEAD < PIECES)
        def _():
            for step in range(SLOTS - 1):
                start_in(piece + AHEAD, step)
            pack_and_send(piece + AHEAD, 0)

        return carry

    lax.fori_loop(0, PIECES, first_stage, 0)

    def second_stage(chunk, carry):
        copies = [pltpu.make_async_copy(recv2.at[chunk, color], recv2_in.at[color % 2], recv2_in_sem.at[color % 2])
                  for color in range(COLORS)]

        def fetch(color):
            wait_bytes(recv2.at[chunk, color], recv2_sem.at[color, chunk])
            copies[color].start()

        fetch(0)
        fetch(1)
        for color in range(COLORS):
            copies[color].wait()
            base = color * color_rows + chunk * rows

            def add(sub, inner):
                to = pl.ds(pl.multiple_of(sub * SUB_ROWS, SUB_ROWS), SUB_ROWS)
                out = pl.ds(pl.multiple_of(base + sub * SUB_ROWS, SUB_ROWS), SUB_ROWS)
                keep[chunk, color, to, :] += recv2_in[color % 2, 0, to, :]
                new_master_ref[out, :] += recv2_in[color % 2, 1, to, :]
                return inner

            lax.fori_loop(0, rows // SUB_ROWS, add, 0)
            pltpu.make_async_remote_copy(
                keep.at[chunk, color], recv3.at[chunk, color], send3_sem.at[chunk], recv3_sem.at[color, chunk],
                device_id=(me + flips[color][2],), device_id_type=MESH).start()
            if color == 0:
                fetch(2)
        return carry

    second_stage(0, 0)
    for other in others:
        pltpu.make_async_remote_copy(
            vec_ref.at[:, pl.ds(pl.multiple_of(other * vec_share, vec_share), vec_share)], vec_land.at[me],
            small_sem.at[0], small_sem.at[1], device_id=(other,), device_id_type=MESH).start()
    vec_own = pltpu.make_async_copy(
        vec_ref.at[:, pl.ds(pl.multiple_of(me * vec_share, vec_share), vec_share)], vec_land.at[me], small_sem.at[2])
    vec_own.start()
    lax.fori_loop(1, CHUNKS, second_stage, 0)

    square_acc[...] = jnp.zeros_like(square_acc)

    def third_stage(chunk, carry):
        for color in range(COLORS):
            wait_bytes(recv3.at[chunk, color], recv3_sem.at[color, chunk])
            base = color * color_rows + chunk * rows

            def add(sub, squares):
                to = pl.ds(pl.multiple_of(sub * SUB_ROWS, SUB_ROWS), SUB_ROWS)
                out = pl.ds(pl.multiple_of(base + sub * SUB_ROWS, SUB_ROWS), SUB_ROWS)
                vals = new_master_ref[out, :] + recv3[chunk, color, to, :]
                new_master_ref[out, :] = vals
                return squares + jnp.sum((vals * vals).reshape(SUB_ROWS // 8, 8, LANES), axis=0)

            squares = lax.fori_loop(0, rows // SUB_ROWS, add, jnp.zeros((8, LANES), jnp.float32), unroll=True)
            square_acc[...] += squares
        return carry

    def state_copies(chunk, color):
        slot = (chunk * COLORS + color) % RING
        at = rows_at(color, chunk)
        return [pltpu.make_async_copy(ref.at[at], keep.at[slot, index], state_sem.at[slot])
                for index, ref in enumerate((master_ref, moment_ref, second_ref))]

    lax.fori_loop(0, CHUNKS - 2, third_stage, 0)
    for chunk in range(RING):
        wait_bytes(keep.at[chunk], send3_sem.at[chunk])
    for item in range(RING):
        for copy in state_copies(item // COLORS, item % COLORS):
            copy.start()
    third_stage(CHUNKS - 2, 0)

    vec_own.wait()
    wait_bytes(vec_land.at[pl.ds(0, GROUP - 1)], small_sem.at[1])
    vec_sum = jnp.sum(vec_land[...].astype(jnp.float32), axis=0)
    vec_square = sum(vec_sum[:, part * LANES:(part + 1) * LANES] ** 2 for part in range(vec_share // LANES))

    for index in range(IN_FLIGHT):
        wait_left(index)
    third_stage(CHUNKS - 1, 0)
    square_land[me] = jnp.sum(square_acc[...], axis=0, keepdims=True) + vec_square

    for other in others:
        pltpu.make_async_remote_copy(
            square_land.at[me], square_land.at[me], small_sem.at[3], small_sem.at[4],
            device_id=(other,), device_id_type=MESH).start()
    wait_bytes(new_moment_ref, send2_sem.at[0])
    wait_bytes(new_second_ref, send2_sem.at[1])
    wait_bytes(square_land.at[pl.ds(0, GROUP - 1)], small_sem.at[4])
    norm = jnp.sqrt(jnp.sum(jnp.sum(square_land[...], axis=0), axis=1, keepdims=True))
    clip_coef = jnp.minimum(1.0, 1.0 / (norm + NORM_EPS))

    def piece_rows_at(color, piece):
        return pl.ds(pl.multiple_of(color * color_rows + piece * piece_rows, piece_rows), piece_rows)

    def link_copy(stage, owner, color, piece, hop, part=None):
        place = weights_ref.at[owner, piece_rows_at(color, piece) if part is None else part]
        return pltpu.make_async_remote_copy(
            place, place, send_sem.at[color], recv_sem.at[stage, color, piece],
            device_id=(me + flips[color][hop],), device_id_type=MESH)

    def core_copy(owner, color, piece):
        place = weights_ref.at[owner, piece_rows_at(color, piece)]
        return pltpu.make_async_remote_copy(
            place, place, core_send_sem.at[color], core_recv_sem.at[color],
            device_id=(partner,), device_id_type=MESH)

    def update_chunk(chunk, form):
        for color in range(COLORS):
            item = chunk * COLORS + color
            slot = item % RING
            wait_bytes(keep.at[slot], state_sem.at[slot])
            base = color * color_rows + chunk * rows

            def update(sub, inner):
                to = pl.ds(pl.multiple_of(sub * UPDATE_ROWS, UPDATE_ROWS), UPDATE_ROWS)
                out = pl.ds(pl.multiple_of(base + sub * UPDATE_ROWS, UPDATE_ROWS), UPDATE_ROWS)
                master, moment, second = adam_update(
                    new_master_ref[out, :], clip_coef, keep[slot, 0, to, :],
                    keep[slot, 1, to, :], keep[slot, 2, to, :], DECAY)
                new_master_ref[out, :] = master
                new_moment_ref[out, :] = moment
                new_second_ref[out, :] = second
                weights_ref[me, out, :] = master.astype(jnp.bfloat16)
                if form == 'parts':
                    for stage, hop in ((0, 0), (1, 1), (3, 2)):
                        link_copy(stage, me, color, 0, hop, out).start()
                return inner

            lax.fori_loop(0, rows // UPDATE_ROWS, update, 0)
            if form == 'chunk':
                for stage, hop in ((0, 0), (1, 1), (3, 2)):
                    link_copy(stage, me, color, 0, hop, rows_at(color, chunk)).start()
            if form == 'piece':
                link_copy(0, me, color, chunk // 2, 0).start()

            @pl.when(item + RING < CHUNKS * COLORS)
            def _():
                for copy in state_copies((item + RING) // COLORS, (item + RING) % COLORS):
                    copy.start()

    def update_later(piece, carry):
        update_chunk(piece * 2, None)
        update_chunk(piece * 2 + 1, 'piece')
        return carry

    update_chunk(0, 'parts')
    update_chunk(1, 'chunk')
    lax.fori_loop(1, PIECES, update_later, 0)

    vec_new = adam_update(vec_sum, clip_coef, vec_master_ref[...], vec_moment_ref[...], vec_second_ref[...], 0.0)
    vec_new_master_ref[...], vec_new_moment_ref[...], vec_new_second_ref[...] = vec_new
    vec_weights_ref[me] = vec_new[0].reshape(vec_share // LANES, LANES)

    def own_sends(piece, carry):
        for color in range(COLORS):
            @pl.when(piece > 0)
            def _():
                link_copy(1, me, color, piece, 1).start()

            core_copy(me, color, piece).start()
        return carry

    lax.fori_loop(0, PIECES, own_sends, 0)

    def own_sends_last(piece, carry):
        for color in range(COLORS):
            link_copy(3, me, color, piece, 2).start()
        return carry

    lax.fori_loop(1, PIECES, own_sends_last, 0)

    for other in others:
        pltpu.make_async_remote_copy(
            vec_weights_ref.at[me], vec_weights_ref.at[me], small_sem.at[5], small_sem.at[6],
            device_id=(other,), device_id_type=MESH).start()

    def arrivals(stage, hops, onward):
        def one_piece(piece, carry):
            for color in range(COLORS):
                owner = me + sum(flips[color][hop] for hop in hops)
                wait_bytes(weights_ref.at[owner, piece_rows_at(color, piece)], recv_sem.at[stage, color, piece])
                for next_stage, hop in onward:
                    link_copy(next_stage, owner, color, piece, hop).start()
                core_copy(owner, color, piece).start()
            return carry

        lax.fori_loop(0, PIECES, one_piece, 0)

    arrivals(0, (0,), ((2, 1), (4, 2)))
    arrivals(1, (1,), ((5, 2),))
    arrivals(3, (2,), ())
    arrivals(2, (0, 1), ((6, 2),))
    arrivals(4, (0, 2), ())
    arrivals(5, (1, 2), ())
    arrivals(6, (0, 1, 2), ())

    for color in range(COLORS):
        eight = weights_ref.at[pl.ds(0, 8), pl.ds(color * color_rows, color_rows)]
        wait_bytes(weights_ref.at[pl.ds(0, 7), pl.ds(color * color_rows, color_rows)], send_sem.at[color])
        wait_bytes(eight, core_send_sem.at[color])
        wait_bytes(eight, core_recv_sem.at[color])
    for index in (5, 6):
        wait_bytes(vec_weights_ref.at[pl.ds(0, GROUP - 1)], small_sem.at[index])
    for chunk in range(RING, CHUNKS):
        wait_bytes(keep.at[chunk], send3_sem.at[chunk])
    wait_bytes(vec_land.at[pl.ds(0, GROUP - 1)], small_sem.at[0])
    wait_bytes(square_land.at[pl.ds(0, GROUP - 1)], small_sem.at[3])


def step_call(grad_mat, grad_vec, states, vec_states):
    share = grad_mat.shape[1] // GROUP
    vec_share = grad_vec.shape[1] // GROUP
    rows = share // COLORS // CHUNKS // LANES
    hbm_spec = pl.BlockSpec(memory_space=pltpu.HBM)
    vmem_spec = pl.BlockSpec(memory_space=pltpu.VMEM)
    f32, bf16 = jnp.float32, jnp.bfloat16
    dma = pltpu.SemaphoreType.DMA
    return pl.pallas_call(
        functools.partial(step_kernel, rows, share, vec_share),
        name='adam_step',
        out_shape=(pltpu.VMEM((share // LANES, LANES), f32),) * 3 + (pltpu.VMEM((1, vec_share), f32),) * 3 + (
            pltpu.VMEM((GROUP, share // LANES, LANES), bf16),
            pltpu.VMEM((GROUP, vec_share // LANES, LANES), f32),
            jax.ShapeDtypeStruct((COLORS, PIECES, 4, 3 * CHUNKS * rows // PIECES, LANES), bf16),
            jax.ShapeDtypeStruct((CHUNKS, COLORS, 2, rows, LANES), f32)),
        in_specs=[hbm_spec] * 5 + [vmem_spec] * 3,
        out_specs=(vmem_spec,) * 8 + (hbm_spec,) * 2,
        scratch_shapes=[
            pltpu.VMEM((SLOTS, COLORS, 1, rows * LANES), bf16),
            pltpu.VMEM((CHUNKS, COLORS, rows, LANES), f32),
            pltpu.VMEM((2, 2, rows, LANES), f32),
            pltpu.VMEM((CHUNKS, COLORS, rows, LANES), f32),
            pltpu.VMEM((GROUP, 1, vec_share), bf16),
            pltpu.VMEM((GROUP, 1, LANES), f32),
            pltpu.VMEM((8, LANES), f32),
            dma((SLOTS,)), dma((SLOTS,)), dma((2,)), dma((RING,)),
            dma((IN_FLIGHT,)), dma((2,)), dma((CHUNKS,)),
            dma((COLORS, PIECES)), dma((COLORS, CHUNKS)), dma((COLORS, CHUNKS)), dma((7,)),
            dma((COLORS,)), dma((7, COLORS, PIECES)), dma((COLORS,)), dma((COLORS,)),
        ],
        compiler_params=pltpu.CompilerParams(
            collective_id=0, has_side_effects=True, vmem_limit_bytes=SCRATCH_BYTES),
    )(grad_mat, grad_vec, *states, *vec_states)[:8]


def store_kernel(*refs):
    ins, outs, (vec_weights, sems) = refs[:8], refs[8:16], refs[16:]
    land, vec_land = ins[6:]
    places = [(ins[index], outs[index]) for index in range(3, 6)]
    for index in range(3):
        part = ins[index].shape[0] // STATE_PARTS
        places += [(ins[index].at[pl.ds(at * part, part)], outs[index].at[pl.ds(at * part, part)]) for at in range(STATE_PARTS)]
    for owner in range(GROUP):
        places.append((land.at[owner], outs[6].at[owner]))
    copies = [pltpu.make_async_copy(source, target, sems.at[index]) for index, (source, target) in enumerate(places)]
    for copy in copies:
        copy.start()
    vec_rows = vec_land.shape[1]
    for owner in range(GROUP):
        vec_weights[owner * vec_rows:(owner + 1) * vec_rows, :] = vec_land[owner]
    outs[7][...] = vec_weights[...].astype(jnp.bfloat16)
    for copy in copies:
        copy.wait()


def store_call(results):
    vmem_spec = pl.BlockSpec(memory_space=pltpu.VMEM)
    hbm_spec = pl.BlockSpec(memory_space=pltpu.HBM)
    dma = pltpu.SemaphoreType.DMA
    vec_rows = results[7].size // LANES
    return pl.pallas_call(
        store_kernel,
        name='store_results',
        out_shape=tuple(jax.ShapeDtypeStruct(result.shape, result.dtype) for result in results[:7]) + (
            jax.ShapeDtypeStruct((vec_rows, LANES), jnp.bfloat16),),
        in_specs=[vmem_spec] * 8,
        out_specs=(hbm_spec,) * 7 + (vmem_spec,),
        scratch_shapes=[pltpu.VMEM((vec_rows, LANES), jnp.float32), dma((3 + 3 * STATE_PARTS + GROUP,))],
        compiler_params=pltpu.CompilerParams(vmem_limit_bytes=SCRATCH_BYTES),
    )(*[pltpu.with_memory_space_constraint(result, pltpu.VMEM) for result in results])


def solution(mesh):
    def local_step(grad_mat, grad_vec, master_mat, moment_mat, second_mat, master_vec, moment_vec, second_vec):
        states = [state.reshape(-1, LANES) for state in (master_mat, moment_mat, second_mat)]
        vec_states = [state.reshape(1, -1) for state in (master_vec, moment_vec, second_vec)]
        results = store_call(step_call(grad_mat, grad_vec, states, vec_states))
        return tuple(result.reshape(-1) for result in results)

    row_spec = P(AXIS, None)
    flat_spec = P(AXIS)
    whole_spec = P()
    return jax.shard_map(local_step, mesh=mesh,
                         in_specs=(row_spec, row_spec) + (flat_spec,) * 6,
                         out_specs=(flat_spec,) * 6 + (whole_spec, whole_spec),
                         check_vma=False)
```

```python
import functools

import jax
import jax.numpy as jnp
from jax import lax
from jax.experimental import pallas as pl
from jax.experimental.pallas import tpu as pltpu
from jax.sharding import PartitionSpec as P

STEP = 4
LEARN_RATE = 1e-3
BETA_ONE = 0.9
BETA_TWO = 0.999
ADAM_EPS = 1e-8
DECAY = 0.01
NORM_EPS = 1e-6
FIX_ONE = 1.0 - BETA_ONE ** STEP
FIX_TWO = 1.0 - BETA_TWO ** STEP

AXIS = 'fsdp'
MESH = pl.DeviceIdType.MESH
GROUP = 16
LANES = 128
ORDERS = ((2, 4, 8), (4, 8, 2), (8, 2, 4))
COLORS = len(ORDERS)
CHUNKS = 8
AHEAD = 2
SLOTS = 3
PIECES = 4
IN_FLIGHT = 8
SUB_ROWS = 80
UPDATE_ROWS = 80
RING = 4
STATE_PARTS = 2
ITEMS = 12
SCRATCH_BYTES = 12_800_000


def adam_update(grad_sum, clip_coef, master, moment, second, decay):
    clip_grad = clip_coef * grad_sum
    new_moment = BETA_ONE * moment + (1.0 - BETA_ONE) * clip_grad
    new_second = BETA_TWO * second + (1.0 - BETA_TWO) * clip_grad * clip_grad
    step_dir = (new_moment / FIX_ONE) / (jnp.sqrt(new_second / FIX_TWO) + ADAM_EPS)
    new_master = master - LEARN_RATE * (step_dir + decay * master)
    return new_master, new_moment, new_second


def flip_of(me, bit):
    return bit * (1 - 2 * ((me // bit) % 2))


def step_kernel(rows, share, vec_share, grad_ref, vec_ref, master_ref, moment_ref, second_ref,
                vec_master_ref, vec_moment_ref, vec_second_ref,
                new_master_ref, new_moment_ref, new_second_ref,
                vec_new_master_ref, vec_new_moment_ref, vec_new_second_ref, weights_ref, vec_weights_ref,
                land_ref, recv2,
                pad_in, keep, recv2_in, recv3, vec_land, vec_state, square_land, square_acc,
                pad_sem, part_sem, recv2_in_sem, state_sem,
                send1_sem, send2_sem, send3_sem, recv1_sem, recv2_sem, recv3_sem, small_sem, vec_state_sem,
                send_sem, recv_sem, core_send_sem, core_recv_sem):
    me = lax.axis_index(AXIS)
    core = me % 2
    partner = me + flip_of(me, 1)
    block = rows * LANES
    color_len = share // COLORS
    color_rows = color_len // LANES
    flips = [[flip_of(me, bit) for bit in order] for order in ORDERS]
    piece_rows = CHUNKS * rows // PIECES
    per_owner = share // LANES // piece_rows
    neighbours = [partner] + [me + flip_of(me, bit) + other for bit in ORDERS[0] for other in (0, flip_of(me, 1))]
    others = [me + sum(flip_of(me, bit) for bit in (1, 2, 4, 8) if mask & bit)
              for mask in sorted(range(1, GROUP), key=lambda mask: (-(mask >> 1).bit_count(), mask))]

    def wait_bytes(ref, sem):
        pltpu.make_async_copy(ref, ref, sem).wait()

    def rows_at(color, chunk):
        return pl.ds(pl.multiple_of(color * color_rows + chunk * rows, rows), rows)

    def piece_at(owner, color, chunk):
        start = pl.multiple_of(owner * share + color * color_len + chunk * block, block)
        return grad_ref.at[:, pl.ds(start, block)]

    def packed_at(color, piece, item):
        index = (piece * COLORS + color) * ITEMS + item
        return index // per_owner, pl.multiple_of((index % per_owner) * piece_rows, piece_rows)

    part_owner = COLORS * PIECES * ITEMS // per_owner
    part_rows = 3 * rows

    def route(item, color):
        place, kind = item // 3, (item + 1) % 3
        flip1, flip2, flip3 = flips[color]
        local = (2 - kind) // 2
        target_core = local * (1 - core) + (1 - local) * (kind - 1)
        target = me - core + (1 - local) * flip1 + target_core
        owner = target + (1 - place // 2) * flip2 + (1 - place % 2) * flip3
        source = (1 - local) * (1 + core)
        return owner, target, source, place

    def start_in(piece, step):
        for color in range(COLORS):
            owner = route(step // 2, color)[0]
            pltpu.make_async_copy(piece_at(owner, color, piece * 2 + step % 2), pad_in.at[step % SLOTS, color],
                                  pad_sem.at[step % SLOTS]).start()

    def pack_step(piece, step):
        wait_bytes(pad_in.at[step % SLOTS], pad_sem.at[step % SLOTS])
        for color in range(COLORS):
            place_owner, place_row = packed_at(color, piece, step // 2)

            def pack(sub, inner):
                off = pl.multiple_of(sub * SUB_ROWS * LANES, SUB_ROWS * LANES)
                vals = pad_in[step % SLOTS, color, :, pl.ds(off, SUB_ROWS * LANES)].astype(jnp.float32)
                to = pl.multiple_of(place_row + (step % 2) * rows + sub * SUB_ROWS, SUB_ROWS)
                weights_ref[place_owner, pl.ds(to, SUB_ROWS), :] = (
                    vals.reshape(SUB_ROWS, LANES).astype(jnp.bfloat16))
                return inner

            lax.fori_loop(0, rows // SUB_ROWS, pack, 0, unroll=True)

    def send_item(piece, item, start=0, size=None):
        size = piece_rows if size is None else size
        for color in range(COLORS):
            owner, target, source, place = route(item, color)
            place_owner, place_row = packed_at(color, piece, item)
            from_row = pl.multiple_of(place_row + start, rows)
            to_row = pl.multiple_of(source * piece_rows + start, rows)
            pltpu.make_async_remote_copy(
                weights_ref.at[place_owner, pl.ds(from_row, size)],
                land_ref.at[color, piece, place, pl.ds(to_row, size)],
                send1_sem.at[(piece * ITEMS + item) % IN_FLIGHT], recv1_sem.at[color, piece], device_id=(target,), device_id_type=MESH).start()

    def wait_left(index):
        wait_bytes(weights_ref.at[0, pl.ds(0, COLORS * piece_rows)], send1_sem.at[index])

    def pack_and_send(piece, first):
        def one_step(step, carry):
            @pl.when(step + SLOTS - 1 < 2 * ITEMS)
            def _():
                start_in(piece, step + SLOTS - 1)

            @pl.when(piece * ITEMS + step // 2 - (step % 2) * ITEMS * PIECES >= IN_FLIGHT)
            def _():
                wait_left((piece * ITEMS + step // 2) % IN_FLIGHT)

            pack_step(piece, step)

            @pl.when(step % 2 == 1)
            def _():
                send_item(piece, step // 2)

            return carry

        lax.fori_loop(first, 2 * ITEMS, one_step, 0)

    def start_parts(chunk, place):
        slot = place % SLOTS
        for color in range(COLORS):
            flip1, flip2, flip3 = flips[color]
            owner = me + (1 - place // 2) * flip2 + (1 - place % 2) * flip3
            for source in range(3):
                row = pl.multiple_of(source * piece_rows + (chunk % 2) * rows, rows)
                pltpu.make_async_copy(land_ref.at[color, chunk // 2, place, pl.ds(row, rows)],
                                      weights_ref.at[part_owner + slot, pl.ds(color * part_rows + source * rows, rows)],
                                      part_sem.at[slot]).start()
            pltpu.make_async_copy(piece_at(owner, color, chunk), pad_in.at[slot, color], pad_sem.at[slot]).start()

    def first_sums(chunk):
        for place in range(SLOTS - 1):
            start_parts(chunk, place)
        for place in range(4):
            slot = place % SLOTS
            if place + SLOTS - 1 < 4:
                start_parts(chunk, place + SLOTS - 1)
            wait_bytes(weights_ref.at[part_owner + slot, pl.ds(0, COLORS * part_rows)], part_sem.at[slot])
            wait_bytes(pad_in.at[slot], pad_sem.at[slot])
            for color in range(COLORS):
                at = rows_at(color, chunk)
                total = (new_moment_ref.at[at], new_second_ref.at[at], keep.at[chunk, color], new_master_ref.at[at])[place]

                def add(sub, inner):
                    off = pl.multiple_of(sub * SUB_ROWS * LANES, SUB_ROWS * LANES)
                    to = pl.ds(pl.multiple_of(sub * SUB_ROWS, SUB_ROWS), SUB_ROWS)
                    vals = pad_in[slot, color, :, pl.ds(off, SUB_ROWS * LANES)].astype(jnp.float32)
                    vals = vals.reshape(SUB_ROWS, LANES)
                    for source in range(3):
                        row = pl.multiple_of(color * part_rows + source * rows + sub * SUB_ROWS, SUB_ROWS)
                        vals = vals + weights_ref[part_owner + slot, pl.ds(row, SUB_ROWS), :].astype(jnp.float32)
                    total[to, :] = vals
                    return inner

                lax.fori_loop(0, rows // SUB_ROWS, add, 0, unroll=True)
                if place < 2:
                    pltpu.make_async_remote_copy(
                        total, recv2.at[chunk, color, place], send2_sem.at[place], recv2_sem.at[color, chunk],
                        device_id=(me + flips[color][1],), device_id_type=MESH).start()

    for step in range(SLOTS):
        start_in(0, step)
    barrier = pltpu.get_barrier_semaphore()
    for neighbour in neighbours:
        pl.semaphore_signal(barrier, inc=1, device_id=(neighbour,), device_id_type=MESH)
    pack_step(0, 0)
    pl.semaphore_wait(barrier, len(neighbours))
    send_item(0, 0, 0, rows)
    start_in(0, SLOTS)
    pack_step(0, 1)
    send_item(0, 0, rows, rows)
    pack_and_send(0, 2)

    def pack_ahead(piece, carry):
        for step in range(SLOTS - 1):
            start_in(piece, step)
        pack_and_send(piece, 0)
        return carry

    lax.fori_loop(1, AHEAD, pack_ahead, 0)

    def first_stage(piece, carry):
        for color in range(COLORS):
            wait_bytes(land_ref.at[color, piece], recv1_sem.at[color, piece])

        def one_chunk(chunk, inner):
            first_sums(chunk)
            return inner

        lax.fori_loop(2 * piece, 2 * piece + 2, one_chunk, 0)

        @pl.when(piece + AHEAD < PIECES)
        def _():
            for step in range(SLOTS - 1):
                start_in(piece + AHEAD, step)
            pack_and_send(piece + AHEAD, 0)

        return carry

    lax.fori_loop(0, PIECES, first_stage, 0)

    def second_stage(chunk, carry):
        copies = [pltpu.make_async_copy(recv2.at[chunk, color], recv2_in.at[color % 2], recv2_in_sem.at[color % 2])
                  for color in range(COLORS)]

        def fetch(color):
            wait_bytes(recv2.at[chunk, color], recv2_sem.at[color, chunk])
            copies[color].start()

        fetch(0)
        fetch(1)
        for color in range(COLORS):
            copies[color].wait()
            base = color * color_rows + chunk * rows

            def add(sub, inner):
                to = pl.ds(pl.multiple_of(sub * SUB_ROWS, SUB_ROWS), SUB_ROWS)
                out = pl.ds(pl.multiple_of(base + sub * SUB_ROWS, SUB_ROWS), SUB_ROWS)
                keep[chunk, color, to, :] += recv2_in[color % 2, 0, to, :]
                new_master_ref[out, :] += recv2_in[color % 2, 1, to, :]
                return inner

            lax.fori_loop(0, rows // SUB_ROWS, add, 0)
            pltpu.make_async_remote_copy(
                keep.at[chunk, color], recv3.at[chunk, color], send3_sem.at[chunk], recv3_sem.at[color, chunk],
                device_id=(me + flips[color][2],), device_id_type=MESH).start()
            if color == 0:
                fetch(2)
        return carry

    second_stage(0, 0)
    for other in others:
        pltpu.make_async_remote_copy(
            vec_ref.at[:, pl.ds(pl.multiple_of(other * vec_share, vec_share), vec_share)], vec_land.at[me],
            small_sem.at[0], small_sem.at[1], device_id=(other,), device_id_type=MESH).start()
    vec_own = pltpu.make_async_copy(
        vec_ref.at[:, pl.ds(pl.multiple_of(me * vec_share, vec_share), vec_share)], vec_land.at[me], small_sem.at[2])
    vec_own.start()
    for index, ref in enumerate((vec_master_ref, vec_moment_ref, vec_second_ref)):
        pltpu.make_async_copy(ref, vec_state.at[index], vec_state_sem).start()
    lax.fori_loop(1, CHUNKS, second_stage, 0)

    square_acc[...] = jnp.zeros_like(square_acc)

    def third_stage(chunk, carry):
        for color in range(COLORS):
            wait_bytes(recv3.at[chunk, color], recv3_sem.at[color, chunk])
            base = color * color_rows + chunk * rows

            def add(sub, squares):
                to = pl.ds(pl.multiple_of(sub * SUB_ROWS, SUB_ROWS), SUB_ROWS)
                out = pl.ds(pl.multiple_of(base + sub * SUB_ROWS, SUB_ROWS), SUB_ROWS)
                vals = new_master_ref[out, :] + recv3[chunk, color, to, :]
                new_master_ref[out, :] = vals
                return squares + jnp.sum((vals * vals).reshape(SUB_ROWS // 8, 8, LANES), axis=0)

            squares = lax.fori_loop(0, rows // SUB_ROWS, add, jnp.zeros((8, LANES), jnp.float32), unroll=True)
            square_acc[...] += squares
        return carry

    def state_copies(chunk, color):
        slot = (chunk * COLORS + color) % RING
        at = rows_at(color, chunk)
        return [pltpu.make_async_copy(ref.at[at], keep.at[slot, index], state_sem.at[slot])
                for index, ref in enumerate((master_ref, moment_ref, second_ref))]

    lax.fori_loop(0, CHUNKS - 2, third_stage, 0)
    for chunk in range(RING):
        wait_bytes(keep.at[chunk], send3_sem.at[chunk])
    for item in range(RING):
        for copy in state_copies(item // COLORS, item % COLORS):
            copy.start()
    third_stage(CHUNKS - 2, 0)

    vec_own.wait()
    wait_bytes(vec_land.at[pl.ds(0, GROUP - 1)], small_sem.at[1])
    vec_sum = jnp.sum(vec_land[...].astype(jnp.float32), axis=0)
    vec_square = sum(vec_sum[:, part * LANES:(part + 1) * LANES] ** 2 for part in range(vec_share // LANES))

    for index in range(IN_FLIGHT):
        wait_left(index)
    third_stage(CHUNKS - 1, 0)
    square_land[me] = jnp.sum(square_acc[...], axis=0, keepdims=True) + vec_square

    for other in others:
        pltpu.make_async_remote_copy(
            square_land.at[me], square_land.at[me], small_sem.at[3], small_sem.at[4],
            device_id=(other,), device_id_type=MESH).start()
    wait_bytes(new_moment_ref, send2_sem.at[0])
    wait_bytes(new_second_ref, send2_sem.at[1])
    wait_bytes(square_land.at[pl.ds(0, GROUP - 1)], small_sem.at[4])
    norm = jnp.sqrt(jnp.sum(jnp.sum(square_land[...], axis=0), axis=1, keepdims=True))
    clip_coef = jnp.minimum(1.0, 1.0 / (norm + NORM_EPS))

    def piece_rows_at(color, piece):
        return pl.ds(pl.multiple_of(color * color_rows + piece * piece_rows, piece_rows), piece_rows)

    def link_copy(stage, owner, color, piece, hop, part=None):
        place = weights_ref.at[owner, piece_rows_at(color, piece) if part is None else part]
        return pltpu.make_async_remote_copy(
            place, place, send_sem.at[color], recv_sem.at[stage, color, piece],
            device_id=(me + flips[color][hop],), device_id_type=MESH)

    def core_copy(owner, color, piece):
        place = weights_ref.at[owner, piece_rows_at(color, piece)]
        return pltpu.make_async_remote_copy(
            place, place, core_send_sem.at[color], core_recv_sem.at[color],
            device_id=(partner,), device_id_type=MESH)

    def update_chunk(chunk, form):
        for color in range(COLORS):
            item = chunk * COLORS + color
            slot = item % RING
            wait_bytes(keep.at[slot], state_sem.at[slot])
            base = color * color_rows + chunk * rows

            def update(sub, inner):
                to = pl.ds(pl.multiple_of(sub * UPDATE_ROWS, UPDATE_ROWS), UPDATE_ROWS)
                out = pl.ds(pl.multiple_of(base + sub * UPDATE_ROWS, UPDATE_ROWS), UPDATE_ROWS)
                master, moment, second = adam_update(
                    new_master_ref[out, :], clip_coef, keep[slot, 0, to, :],
                    keep[slot, 1, to, :], keep[slot, 2, to, :], DECAY)
                new_master_ref[out, :] = master
                new_moment_ref[out, :] = moment
                new_second_ref[out, :] = second
                weights_ref[me, out, :] = master.astype(jnp.bfloat16)
                if form == 'parts':
                    for stage, hop in ((0, 0), (1, 1), (3, 2)):
                        link_copy(stage, me, color, 0, hop, out).start()
                return inner

            lax.fori_loop(0, rows // UPDATE_ROWS, update, 0)
            if form == 'chunk':
                for stage, hop in ((0, 0), (1, 1), (3, 2)):
                    link_copy(stage, me, color, 0, hop, rows_at(color, chunk)).start()
            if form == 'piece':
                link_copy(0, me, color, chunk // 2, 0).start()

            @pl.when(item + RING < CHUNKS * COLORS)
            def _():
                for copy in state_copies((item + RING) // COLORS, (item + RING) % COLORS):
                    copy.start()

    def update_later(piece, carry):
        update_chunk(piece * 2, None)
        update_chunk(piece * 2 + 1, 'piece')
        return carry

    update_chunk(0, 'parts')
    update_chunk(1, 'chunk')
    lax.fori_loop(1, PIECES, update_later, 0)

    wait_bytes(vec_state, vec_state_sem)
    vec_new = adam_update(vec_sum, clip_coef, vec_state[0], vec_state[1], vec_state[2], 0.0)
    vec_new_master_ref[...], vec_new_moment_ref[...], vec_new_second_ref[...] = vec_new
    vec_weights_ref[me] = vec_new[0].reshape(vec_share // LANES, LANES)

    def own_sends(piece, carry):
        for color in range(COLORS):
            @pl.when(piece > 0)
            def _():
                link_copy(1, me, color, piece, 1).start()

            core_copy(me, color, piece).start()
        return carry

    lax.fori_loop(0, PIECES, own_sends, 0)

    def own_sends_last(piece, carry):
        for color in range(COLORS):
            link_copy(3, me, color, piece, 2).start()
        return carry

    lax.fori_loop(1, PIECES, own_sends_last, 0)

    for other in others:
        pltpu.make_async_remote_copy(
            vec_weights_ref.at[me], vec_weights_ref.at[me], small_sem.at[5], small_sem.at[6],
            device_id=(other,), device_id_type=MESH).start()

    def arrivals(stage, hops, onward):
        def one_piece(piece, carry):
            for color in range(COLORS):
                owner = me + sum(flips[color][hop] for hop in hops)
                wait_bytes(weights_ref.at[owner, piece_rows_at(color, piece)], recv_sem.at[stage, color, piece])
                for next_stage, hop in onward:
                    link_copy(next_stage, owner, color, piece, hop).start()
                core_copy(owner, color, piece).start()
            return carry

        lax.fori_loop(0, PIECES, one_piece, 0)

    arrivals(0, (0,), ((2, 1), (4, 2)))
    arrivals(1, (1,), ((5, 2),))
    arrivals(3, (2,), ())
    arrivals(2, (0, 1), ((6, 2),))
    arrivals(4, (0, 2), ())
    arrivals(5, (1, 2), ())
    arrivals(6, (0, 1, 2), ())

    for color in range(COLORS):
        eight = weights_ref.at[pl.ds(0, 8), pl.ds(color * color_rows, color_rows)]
        wait_bytes(weights_ref.at[pl.ds(0, 7), pl.ds(color * color_rows, color_rows)], send_sem.at[color])
        wait_bytes(eight, core_send_sem.at[color])
        wait_bytes(eight, core_recv_sem.at[color])
    for index in (5, 6):
        wait_bytes(vec_weights_ref.at[pl.ds(0, GROUP - 1)], small_sem.at[index])
    for chunk in range(RING, CHUNKS):
        wait_bytes(keep.at[chunk], send3_sem.at[chunk])
    wait_bytes(vec_land.at[pl.ds(0, GROUP - 1)], small_sem.at[0])
    wait_bytes(square_land.at[pl.ds(0, GROUP - 1)], small_sem.at[3])


def step_call(grad_mat, grad_vec, states, vec_states):
    share = grad_mat.shape[1] // GROUP
    vec_share = grad_vec.shape[1] // GROUP
    rows = share // COLORS // CHUNKS // LANES
    hbm_spec = pl.BlockSpec(memory_space=pltpu.HBM)
    vmem_spec = pl.BlockSpec(memory_space=pltpu.VMEM)
    f32, bf16 = jnp.float32, jnp.bfloat16
    dma = pltpu.SemaphoreType.DMA
    return pl.pallas_call(
        functools.partial(step_kernel, rows, share, vec_share),
        name='adam_step',
        out_shape=(pltpu.VMEM((share // LANES, LANES), f32),) * 3 + (pltpu.VMEM((1, vec_share), f32),) * 3 + (
            pltpu.VMEM((GROUP, share // LANES, LANES), bf16),
            pltpu.VMEM((GROUP, vec_share // LANES, LANES), f32),
            jax.ShapeDtypeStruct((COLORS, PIECES, 4, 3 * CHUNKS * rows // PIECES, LANES), bf16),
            jax.ShapeDtypeStruct((CHUNKS, COLORS, 2, rows, LANES), f32)),
        in_specs=[hbm_spec] * 8,
        out_specs=(vmem_spec,) * 8 + (hbm_spec,) * 2,
        scratch_shapes=[
            pltpu.VMEM((SLOTS, COLORS, 1, rows * LANES), bf16),
            pltpu.VMEM((CHUNKS, COLORS, rows, LANES), f32),
            pltpu.VMEM((2, 2, rows, LANES), f32),
            pltpu.VMEM((CHUNKS, COLORS, rows, LANES), f32),
            pltpu.VMEM((GROUP, 1, vec_share), bf16),
            pltpu.VMEM((3, 1, vec_share), f32),
            pltpu.VMEM((GROUP, 1, LANES), f32),
            pltpu.VMEM((8, LANES), f32),
            dma((SLOTS,)), dma((SLOTS,)), dma((2,)), dma((RING,)),
            dma((IN_FLIGHT,)), dma((2,)), dma((CHUNKS,)),
            dma((COLORS, PIECES)), dma((COLORS, CHUNKS)), dma((COLORS, CHUNKS)), dma((7,)), dma,
            dma((COLORS,)), dma((7, COLORS, PIECES)), dma((COLORS,)), dma((COLORS,)),
        ],
        compiler_params=pltpu.CompilerParams(
            collective_id=0, has_side_effects=True, vmem_limit_bytes=SCRATCH_BYTES),
    )(grad_mat, grad_vec, *states, *vec_states)[:8]


def store_kernel(*refs):
    ins, outs, (vec_wide, vec_weights, sems, vec_sem) = refs[:8], refs[8:16], refs[16:]
    land, vec_land = ins[6:]
    places = [(ins[index], outs[index]) for index in range(3, 6)]
    for index in range(3):
        part = ins[index].shape[0] // STATE_PARTS
        places += [(ins[index].at[pl.ds(at * part, part)], outs[index].at[pl.ds(at * part, part)]) for at in range(STATE_PARTS)]
    for owner in range(GROUP):
        places.append((land.at[owner], outs[6].at[owner]))
    copies = [pltpu.make_async_copy(source, target, sems.at[index]) for index, (source, target) in enumerate(places)]
    for copy in copies:
        copy.start()
    vec_rows = vec_land.shape[1]
    for owner in range(GROUP):
        vec_wide[owner * vec_rows:(owner + 1) * vec_rows, :] = vec_land[owner]
    vec_weights[...] = vec_wide[...].astype(jnp.bfloat16)
    copies.append(pltpu.make_async_copy(vec_weights, outs[7], vec_sem))
    copies[-1].start()
    for copy in copies:
        copy.wait()


def store_call(results):
    vmem_spec = pl.BlockSpec(memory_space=pltpu.VMEM)
    hbm_spec = pl.BlockSpec(memory_space=pltpu.HBM)
    dma = pltpu.SemaphoreType.DMA
    vec_rows = results[7].size // LANES
    return pl.pallas_call(
        store_kernel,
        name='store_results',
        out_shape=tuple(jax.ShapeDtypeStruct(result.shape, result.dtype) for result in results[:7]) + (
            jax.ShapeDtypeStruct((vec_rows, LANES), jnp.bfloat16),),
        in_specs=[vmem_spec] * 8,
        out_specs=(hbm_spec,) * 8,
        scratch_shapes=[pltpu.VMEM((vec_rows, LANES), jnp.float32), pltpu.VMEM((vec_rows, LANES), jnp.bfloat16), dma((3 + 3 * STATE_PARTS + GROUP,)), dma],
        compiler_params=pltpu.CompilerParams(vmem_limit_bytes=SCRATCH_BYTES),
    )(*[pltpu.with_memory_space_constraint(result, pltpu.VMEM) for result in results])


def solution(mesh):
    def local_step(grad_mat, grad_vec, master_mat, moment_mat, second_mat, master_vec, moment_vec, second_vec):
        states = [state.reshape(-1, LANES) for state in (master_mat, moment_mat, second_mat)]
        vec_states = [state.reshape(1, -1) for state in (master_vec, moment_vec, second_vec)]
        results = store_call(step_call(grad_mat, grad_vec, states, vec_states))
        return tuple(result.reshape(-1) for result in results)

    row_spec = P(AXIS, None)
    flat_spec = P(AXIS)
    whole_spec = P()
    return jax.shard_map(local_step, mesh=mesh,
                         in_specs=(row_spec, row_spec) + (flat_spec,) * 6,
                         out_specs=(flat_spec,) * 6 + (whole_spec, whole_spec),
                         check_vma=False)
```
